128 devices in a mesh: lat: 8 (over z, y_hi), lon: 16 (over x, y_lo, core).
Axes of the slice: x: 4, y: 4 (y_hi: 2, y_lo: 2; y = y_hi * 2 + y_lo), z: 4, core: 2. Of those that a mesh axis runs over, the one named last changes fastest.
Arguments:
- tokens: bfloat16 [96, 384, 512], P('lat', 'lon'), may hold values from -100 to 100
- fine_gain: float32 [512], replicated, may hold values from 0.5 to 1.5
- fine_qkv: bfloat16 [512, 768], replicated, may hold values from -20 to 20
- fine_proj: bfloat16 [256, 512], replicated, may hold values from -0.375 to 0.375
- merge_gain: float32 [2048], replicated, may hold values from 0.5 to 1.5
- merge_weight: bfloat16 [2048, 512], replicated, may hold values from -0.125 to 0.125
- coarse_gain: float32 [512], replicated, may hold values from 0.5 to 1.5
- coarse_qkv: bfloat16 [512, 1536], replicated, may hold values from -20 to 20
- coarse_proj: bfloat16 [512, 512], replicated, may hold values from -0.25 to 0.25
- cotangent: bfloat16 [48, 192, 512], P('lat', 'lon'), may hold values from -6 to 6
Outputs:
- output: bfloat16 [48, 192, 512], P('lat', 'lon')
- grad_tokens: bfloat16 [96, 384, 512], P('lat', 'lon')
- grad_fine_gain: float32 [512], P(('lat', 'lon'))
- grad_fine_qkv: float32 [512, 768], P(('lat', 'lon'))
- grad_fine_proj: float32 [256, 512], P(('lat', 'lon'))
- grad_merge_gain: float32 [2048], P(('lat', 'lon'))
- grad_merge_weight: float32 [2048, 512], P(('lat', 'lon'))
- grad_coarse_gain: float32 [512], P(('lat', 'lon'))
- grad_coarse_qkv: float32 [512, 1536], P(('lat', 'lon'))
- grad_coarse_proj: float32 [512, 512], P(('lat', 'lon'))
The draws below stay inside these ranges and needn't reach their ends.
All inputs are finite; a program needn't handle non-finite values.
Results may differ from the reference program's by a relative error of at most 0.028.
Values may be sent and summed in bfloat16 or wider, within the bound.
No kernel may reach another device: no remote copies, remote signals or barrier semaphores. Data moves between devices by JAX's collectives and lax.ppermute only.
A program may use at most 128 MiB of HBM per device.

```python
import math
import jax
import jax.numpy as jnp
from jax import lax

D = 512
DC = 512
HD = 64
HF = 4
HC = 8
WLAT = 6
WLON = 12
SLAT = 3
SLON = 6
NLAT = 96
NLON = 384


def projection_draw(key, breadth, head_count):
    inner = head_count * HD
    keys_all = jax.random.split(key, 1)
    matrix = jnp.clip(jax.random.normal(keys_all[0], (breadth, 3 * inner), jnp.float32), -6.0, 6.0) * breadth ** (-0.5)
    return jnp.clip(matrix, -20.0, 20.0).astype(jnp.bfloat16)


def draw_tokens(key, part):
    keys_all = jax.random.split(jax.random.fold_in(key, 11), 3)
    row_scale = jnp.exp(jax.random.uniform(keys_all[0], (NLAT, NLON, 1), jnp.float32, 0.0, math.log(10.0)))
    channel_scale = jnp.exp(jax.random.uniform(keys_all[1], (1, 1, D), jnp.float32, -0.7, 0.7))
    base_values = jax.random.normal(keys_all[2], (NLAT, NLON, D), jnp.float32)
    return jnp.clip(base_values * row_scale * channel_scale, -100.0, 100.0).astype(jnp.bfloat16)


def draw_fine_qkv(key, part):
    return projection_draw(jax.random.fold_in(key, 23), D, HF)


def draw_coarse_qkv(key, part):
    return projection_draw(jax.random.fold_in(key, 37), DC, HC)


def level_of(stream_key, extent, shards, least, high):
    factor_of = 1.0
    for position, blocks in shards:
        heights = jax.random.uniform(jax.random.fold_in(jax.random.fold_in(stream_key, 6), position), (blocks,), jnp.float32, least / len(shards), high / len(shards))
        factor_of = factor_of * jnp.repeat(jnp.exp(heights), extent[position] // blocks).reshape((-1,) + (1,) * (len(extent) - 1 - position))
    return factor_of


def centred(own_key, shape, scale, bound, pieces=(), kind=jnp.bfloat16):
    gain = level_of(own_key, shape, pieces, -0.22, 0.18) if pieces else 1.0
    values = jax.random.normal(own_key, shape, jnp.float32) * scale * gain
    return jnp.minimum(jnp.maximum(values, -bound), bound).astype(kind)


def setup_inputs(seed: int = 0) -> dict:
    streams_of = jax.random.split(jax.random.key(seed), 11)
    tokens = draw_tokens(jax.random.fold_in(streams_of[10], 71), 0)
    fine_gain = jnp.clip(1.0 + 0.1 * jax.random.normal(streams_of[1], (D,), jnp.float32), 0.5, 1.5)
    fine_qkv = draw_fine_qkv(jax.random.fold_in(streams_of[10], 71), 0)
    fine_proj = centred(streams_of[3], (HF * HD, D), (HF * HD) ** -0.5, 0.375)
    merge_gain = jnp.clip(1.0 + 0.1 * jax.random.normal(streams_of[4], (4 * D,), jnp.float32), 0.5, 1.5)
    merge_weight = centred(streams_of[5], (4 * D, DC), (4 * D) ** -0.5, 0.125)
    coarse_gain = jnp.clip(1.0 + 0.1 * jax.random.normal(streams_of[6], (DC,), jnp.float32), 0.5, 1.5)
    coarse_qkv = draw_coarse_qkv(jax.random.fold_in(streams_of[10], 71), 0)
    coarse_proj = centred(streams_of[8], (HC * HD, DC), (HC * HD) ** -0.5, 0.25)
    cotangent = centred(streams_of[9], (NLAT // 2, NLON // 2, DC), 1.0, 6.0, ((0, 8), (1, 16)))
    return {"tokens": tokens, "fine_gain": fine_gain, "fine_qkv": fine_qkv, "fine_proj": fine_proj, "merge_gain": merge_gain, "merge_weight": merge_weight, "coarse_gain": coarse_gain, "coarse_qkv": coarse_qkv, "coarse_proj": coarse_proj, "cotangent": cotangent}


EPSILON = 1e-05

def layer_norm(values, gains):
    center = lax.optimization_barrier(jnp.mean(values, axis=-1, keepdims=True))
    shifted = values - center
    spread = lax.optimization_barrier(jnp.mean(shifted * shifted, axis=-1, keepdims=True))
    return shifted * lax.rsqrt(spread + EPSILON) * gains

def window_attention(packed, row_offset, total_rows, head_count):
    row_count, col_count = (packed.shape[0], packed.shape[1])
    head_size = packed.shape[2] // (3 * head_count)
    lat_windows = row_count // WLAT
    lon_windows = col_count // WLON
    grouped = packed.reshape(lat_windows, WLAT, lon_windows, WLON, 3, head_count, head_size)
    grouped = grouped.transpose(4, 0, 2, 5, 1, 3, 6).reshape(3, lat_windows, lon_windows, head_count, WLAT * WLON, head_size)
    queries = grouped[0].astype(jnp.float32)
    keys_all = grouped[1].astype(jnp.float32)
    values_all = grouped[2].astype(jnp.float32)
    scores = jnp.einsum('abhqd,abhkd->abhqk', queries, keys_all) * head_size ** (-0.5)
    row_index = row_offset + jnp.arange(row_count, dtype=jnp.int32)
    region = (row_index >= total_rows - SLAT).reshape(lat_windows, WLAT)
    region = jnp.broadcast_to(region[:, :, None], (lat_windows, WLAT, WLON)).reshape(lat_windows, WLAT * WLON)
    allowed = region[:, None, None, :, None] == region[:, None, None, None, :]
    scores = jnp.where(allowed, scores, -1000000000.0)
    largest = lax.optimization_barrier(jnp.max(scores, axis=-1, keepdims=True))
    exponent = jnp.exp(scores - largest)
    attn_weights = (exponent / lax.optimization_barrier(jnp.sum(exponent, axis=-1, keepdims=True))).astype(jnp.bfloat16)
    mixed_out = jnp.einsum('abhqk,abhkd->abhqd', attn_weights.astype(jnp.float32), values_all).astype(jnp.bfloat16)
    mixed_out = mixed_out.reshape(lat_windows, lon_windows, head_count, WLAT, WLON, head_size)
    return mixed_out.transpose(0, 3, 1, 4, 2, 5).reshape(row_count, col_count, head_count * head_size)

def block_forward(rolled, gains, weight_qkv, weight_proj, row_offset, total_rows, head_count):
    normed = layer_norm(rolled.astype(jnp.float32), gains).astype(jnp.bfloat16)
    packed = jnp.dot(normed, weight_qkv, preferred_element_type=jnp.float32).astype(jnp.bfloat16)
    mixed_out = window_attention(packed, row_offset, total_rows, head_count)
    added = jnp.dot(mixed_out, weight_proj, preferred_element_type=jnp.float32)
    result = (rolled.astype(jnp.float32) + added).astype(jnp.bfloat16)
    return (result, (normed, packed, mixed_out))

def block_backward(grad_out, rolled, gains, weight_qkv, weight_proj, saved, row_offset, total_rows, head_count):
    normed, packed, mixed_out = saved
    grad_mixed = lax.dot_general(grad_out, weight_proj, (((2,), (1,)), ((), ())), preferred_element_type=jnp.float32).astype(jnp.bfloat16)
    grad_proj = lax.dot_general(mixed_out, grad_out, (((0, 1), (0, 1)), ((), ())), preferred_element_type=jnp.float32)

    def attend_only(packed_in):
        return window_attention(packed_in, row_offset, total_rows, head_count)
    _, attend_back = jax.vjp(attend_only, packed)
    grad_packed = attend_back(grad_mixed)[0]
    grad_normed = lax.dot_general(grad_packed, weight_qkv, (((2,), (1,)), ((), ())), preferred_element_type=jnp.float32).astype(jnp.bfloat16)
    grad_qkv = lax.dot_general(normed, grad_packed, (((0, 1), (0, 1)), ((), ())), preferred_element_type=jnp.float32)
    _, norm_back = jax.vjp(layer_norm, rolled.astype(jnp.float32), gains)
    grad_input, grad_gain = norm_back(grad_normed.astype(jnp.float32))
    grad_rolled = (grad_out.astype(jnp.float32) + grad_input).astype(jnp.bfloat16)
    return (grad_rolled, grad_gain, grad_qkv, grad_proj)

def merge_tokens(patch_grid):
    row_count, col_count, breadth = patch_grid.shape
    reshaped = patch_grid.reshape(row_count // 2, 2, col_count // 2, 2, breadth)
    return reshaped.transpose(0, 2, 3, 1, 4).reshape(row_count // 2, col_count // 2, 4 * breadth)

def split_tokens(merged_grid):
    row_count, col_count, breadth = merged_grid.shape
    narrow = breadth // 4
    reshaped = merged_grid.reshape(row_count, col_count, 2, 2, narrow)
    return reshaped.transpose(0, 3, 1, 2, 4).reshape(2 * row_count, 2 * col_count, narrow)

def merge_forward(fine_grid, gains, weight):
    packed_grid = merge_tokens(fine_grid)
    normed = layer_norm(packed_grid.astype(jnp.float32), gains).astype(jnp.bfloat16)
    merged = jnp.dot(normed, weight, preferred_element_type=jnp.float32).astype(jnp.bfloat16)
    return (merged, (packed_grid, normed))

def merge_backward(grad_merged, saved, gains, weight):
    packed_grid, normed = saved
    grad_normed = lax.dot_general(grad_merged, weight, (((2,), (1,)), ((), ())), preferred_element_type=jnp.float32).astype(jnp.bfloat16)
    grad_weight = lax.dot_general(normed, grad_merged, (((0, 1), (0, 1)), ((), ())), preferred_element_type=jnp.float32)
    _, norm_back = jax.vjp(layer_norm, packed_grid.astype(jnp.float32), gains)
    grad_packed, grad_gain = norm_back(grad_normed.astype(jnp.float32))
    return (split_tokens(grad_packed.astype(jnp.bfloat16)), grad_gain, grad_weight)

def reference(tokens, fine_gain, fine_qkv, fine_proj, merge_gain, merge_weight, coarse_gain, coarse_qkv, coarse_proj, cotangent):
    fine_total = tokens.shape[0]
    coarse_total = fine_total // 2
    grad_scale = (tokens.shape[0] * tokens.shape[1] // 4) ** (-0.5)
    start = jnp.int32(0)
    rolled_fine = jnp.roll(tokens, (-SLAT, -SLON), axis=(0, 1))
    fine_result, fine_saved = block_forward(rolled_fine, fine_gain, fine_qkv, fine_proj, start, fine_total, HF)
    fine_grid = jnp.roll(fine_result, (SLAT, SLON), axis=(0, 1))
    merged, merge_saved = merge_forward(fine_grid, merge_gain, merge_weight)
    rolled_coarse = jnp.roll(merged, (-SLAT, -SLON), axis=(0, 1))
    coarse_result, coarse_saved = block_forward(rolled_coarse, coarse_gain, coarse_qkv, coarse_proj, start, coarse_total, HC)
    output = jnp.roll(coarse_result, (SLAT, SLON), axis=(0, 1))
    grad_coarse_out = jnp.roll(cotangent, (-SLAT, -SLON), axis=(0, 1))
    grad_rolled_coarse, coarse_gain_sum, coarse_qkv_sum, coarse_proj_sum = block_backward(grad_coarse_out, rolled_coarse, coarse_gain, coarse_qkv, coarse_proj, coarse_saved, start, coarse_total, HC)
    grad_merged = jnp.roll(grad_rolled_coarse, (SLAT, SLON), axis=(0, 1))
    grad_fine_grid, merge_gain_sum, merge_weight_sum = merge_backward(grad_merged, merge_saved, merge_gain, merge_weight)
    grad_fine_out = jnp.roll(grad_fine_grid, (-SLAT, -SLON), axis=(0, 1))
    grad_rolled_fine, fine_gain_sum, fine_qkv_sum, fine_proj_sum = block_backward(grad_fine_out, rolled_fine, fine_gain, fine_qkv, fine_proj, fine_saved, start, fine_total, HF)
    grad_tokens = jnp.roll(grad_rolled_fine, (SLAT, SLON), axis=(0, 1))
    return (output, grad_tokens, fine_gain_sum * grad_scale, fine_qkv_sum * grad_scale, fine_proj_sum * grad_scale, merge_gain_sum * grad_scale, merge_weight_sum * grad_scale, coarse_gain_sum * grad_scale, coarse_qkv_sum * grad_scale, coarse_proj_sum * grad_scale)
```

```python
import jax
import jax.numpy as jnp
from jax import lax
from jax.sharding import PartitionSpec as P

HF = 4
HC = 8
WLAT = 6
WLON = 12
SLAT = 3
SLON = 6


EPSILON = 1e-05


def from_behind(value, axis, steps):
    count = lax.axis_size(axis)
    pairs = [(source, (source + steps) % count) for source in range(count)]
    return lax.ppermute(value, axis, pairs)


def in_blocks(shard, dim, peers):
    dims = shard.shape
    tiles = shard.reshape(*dims[:dim], peers, dims[dim] // peers, *dims[dim + 1 :])
    return jnp.moveaxis(tiles, dim, 0)


def sum_together(arrays, axes, dims):
    peers = lax.axis_size(axes)
    tiles = [in_blocks(a, dim, peers) for a, dim in zip(arrays, dims)]
    lines = jnp.concatenate([b.reshape(peers, -1).astype(jnp.bfloat16) for b in tiles], axis=1)
    span = -(-lines.shape[1] // 2048) * 16
    lines = jnp.pad(lines, ((0, 0), (0, span * 128 - lines.shape[1]))).reshape(peers, span, 128)
    arrived = lax.all_to_all(lines, axes, 0, 0)
    flat = jnp.sum(arrived.astype(jnp.float32), axis=0).reshape(-1)
    at, finished = 0, []
    for b in tiles:
        part = b[0]
        finished.append(flat[at : at + part.size].reshape(part.shape))
        at += part.size
    return tuple(finished)


def layer_norm(values, gains):
    center = jnp.mean(values, axis=-1, keepdims=True)
    shifted = values - center
    spread = jnp.mean(shifted * shifted, axis=-1, keepdims=True)
    return shifted * lax.rsqrt(spread + EPSILON) * gains


def window_attention(packed, row_offset, total_rows, head_count):
    row_count, col_count = (packed.shape[0], packed.shape[1])
    head_size = packed.shape[2] // (3 * head_count)
    lat_windows = row_count // WLAT
    lon_windows = col_count // WLON
    grouped = packed.reshape(lat_windows, WLAT, lon_windows, WLON, 3, head_count, head_size)
    grouped = grouped.transpose(4, 0, 2, 5, 1, 3, 6).reshape(
        3, lat_windows, lon_windows, head_count, WLAT * WLON, head_size
    )
    queries = grouped[0].astype(jnp.float32)
    keys_all = grouped[1].astype(jnp.float32)
    values_all = grouped[2].astype(jnp.float32)
    scores = jnp.einsum("abhqd,abhkd->abhqk", queries, keys_all) * head_size ** (-0.5)
    row_index = row_offset + jnp.arange(row_count, dtype=jnp.int32)
    region = (row_index >= total_rows - SLAT).reshape(lat_windows, WLAT)
    region = jnp.broadcast_to(region[:, :, None], (lat_windows, WLAT, WLON)).reshape(
        lat_windows, WLAT * WLON
    )
    allowed = region[:, None, None, :, None] == region[:, None, None, None, :]
    scores = jnp.where(allowed, scores, -1000000000.0)
    largest = jnp.max(scores, axis=-1, keepdims=True)
    exponent = jnp.exp(scores - largest)
    attn_weights = (exponent / jnp.sum(exponent, axis=-1, keepdims=True)).astype(jnp.bfloat16)
    mixed_out = jnp.einsum(
        "abhqk,abhkd->abhqd", attn_weights.astype(jnp.float32), values_all
    ).astype(jnp.bfloat16)
    mixed_out = mixed_out.reshape(lat_windows, lon_windows, head_count, WLAT, WLON, head_size)
    return mixed_out.transpose(0, 3, 1, 4, 2, 5).reshape(
        row_count, col_count, head_count * head_size
    )


def block_forward(rolled, gains, weight_qkv, weight_proj, row_offset, total_rows, head_count):
    normed = layer_norm(rolled.astype(jnp.float32), gains).astype(jnp.bfloat16)
    packed = jnp.dot(normed, weight_qkv, preferred_element_type=jnp.float32).astype(jnp.bfloat16)
    mixed_out = window_attention(packed, row_offset, total_rows, head_count)
    added = jnp.dot(mixed_out, weight_proj, preferred_element_type=jnp.float32)
    result = (rolled.astype(jnp.float32) + added).astype(jnp.bfloat16)
    return (result, (normed, packed, mixed_out))


def block_backward(
    grad_out, rolled, gains, weight_qkv, weight_proj, saved, row_offset, total_rows, head_count
):
    normed, packed, mixed_out = saved
    grad_mixed = lax.dot_general(
        grad_out, weight_proj, (((2,), (1,)), ((), ())), preferred_element_type=jnp.float32
    ).astype(jnp.bfloat16)
    grad_proj = lax.dot_general(
        mixed_out, grad_out, (((0, 1), (0, 1)), ((), ())), preferred_element_type=jnp.float32
    )

    def attend_only(packed_in):
        return window_attention(packed_in, row_offset, total_rows, head_count)

    _, attend_back = jax.vjp(attend_only, packed)
    grad_packed = attend_back(grad_mixed)[0]
    grad_normed = lax.dot_general(
        grad_packed, weight_qkv, (((2,), (1,)), ((), ())), preferred_element_type=jnp.float32
    ).astype(jnp.bfloat16)
    grad_qkv = lax.dot_general(
        normed, grad_packed, (((0, 1), (0, 1)), ((), ())), preferred_element_type=jnp.float32
    )
    _, norm_back = jax.vjp(layer_norm, rolled.astype(jnp.float32), gains)
    grad_input, grad_gain = norm_back(grad_normed.astype(jnp.float32))
    grad_rolled = (grad_out.astype(jnp.float32) + grad_input).astype(jnp.bfloat16)
    return (grad_rolled, grad_gain, grad_qkv, grad_proj)


def merge_tokens(patch_grid):
    row_count, col_count, breadth = patch_grid.shape
    reshaped = patch_grid.reshape(row_count // 2, 2, col_count // 2, 2, breadth)
    return reshaped.transpose(0, 2, 3, 1, 4).reshape(row_count // 2, col_count // 2, 4 * breadth)


def split_tokens(merged_grid):
    row_count, col_count, breadth = merged_grid.shape
    narrow = breadth // 4
    reshaped = merged_grid.reshape(row_count, col_count, 2, 2, narrow)
    return reshaped.transpose(0, 3, 1, 2, 4).reshape(2 * row_count, 2 * col_count, narrow)


def merge_forward(fine_grid, gains, weight):
    packed_grid = merge_tokens(fine_grid)
    normed = layer_norm(packed_grid.astype(jnp.float32), gains).astype(jnp.bfloat16)
    merged = jnp.dot(normed, weight, preferred_element_type=jnp.float32).astype(jnp.bfloat16)
    return (merged, (packed_grid, normed))


def merge_backward(grad_merged, saved, gains, weight):
    packed_grid, normed = saved
    grad_normed = lax.dot_general(
        grad_merged, weight, (((2,), (1,)), ((), ())), preferred_element_type=jnp.float32
    ).astype(jnp.bfloat16)
    grad_weight = lax.dot_general(
        normed, grad_merged, (((0, 1), (0, 1)), ((), ())), preferred_element_type=jnp.float32
    )
    _, norm_back = jax.vjp(layer_norm, packed_grid.astype(jnp.float32), gains)
    grad_packed, grad_gain = norm_back(grad_normed.astype(jnp.float32))
    return (split_tokens(grad_packed.astype(jnp.bfloat16)), grad_gain, grad_weight)


def rotate_ahead(patch_grid):
    arrived = from_behind(patch_grid[:SLAT], "lat", -1)
    patch_grid = jnp.concatenate([patch_grid[SLAT:], arrived], axis=0)
    arrived = from_behind(patch_grid[:, :SLON], "lon", -1)
    return jnp.concatenate([patch_grid[:, SLON:], arrived], axis=1)


def rotate_back(patch_grid):
    arrived = from_behind(patch_grid[-SLAT:], "lat", 1)
    patch_grid = jnp.concatenate([arrived, patch_grid[:-SLAT]], axis=0)
    arrived = from_behind(patch_grid[:, -SLON:], "lon", 1)
    return jnp.concatenate([arrived, patch_grid[:, :-SLON]], axis=1)


def local(
    tokens,
    fine_gain,
    fine_qkv,
    fine_proj,
    merge_gain,
    merge_weight,
    coarse_gain,
    coarse_qkv,
    coarse_proj,
    cotangent,
):
    fine_rows = tokens.shape[0]
    coarse_rows = fine_rows // 2
    lat_count = lax.axis_size("lat")
    lat_place = lax.axis_index("lat")
    fine_total = fine_rows * lat_count
    coarse_total = coarse_rows * lat_count
    fine_offset = lat_place * fine_rows
    coarse_offset = lat_place * coarse_rows
    grad_scale = (fine_total * tokens.shape[1] * lax.axis_size("lon") // 4) ** (-0.5)
    rolled_fine = rotate_ahead(tokens)
    fine_result, fine_saved = block_forward(
        rolled_fine, fine_gain, fine_qkv, fine_proj, fine_offset, fine_total, HF
    )
    fine_grid = rotate_back(fine_result)
    merged, merge_saved = merge_forward(fine_grid, merge_gain, merge_weight)
    rolled_coarse = rotate_ahead(merged)
    coarse_result, coarse_saved = block_forward(
        rolled_coarse, coarse_gain, coarse_qkv, coarse_proj, coarse_offset, coarse_total, HC
    )
    output = rotate_back(coarse_result)
    grad_coarse_out = rotate_ahead(cotangent)
    grad_rolled_coarse, coarse_gain_sum, coarse_qkv_sum, coarse_proj_sum = block_backward(
        grad_coarse_out,
        rolled_coarse,
        coarse_gain,
        coarse_qkv,
        coarse_proj,
        coarse_saved,
        coarse_offset,
        coarse_total,
        HC,
    )
    grad_merged = rotate_back(grad_rolled_coarse)
    grad_fine_grid, merge_gain_sum, merge_weight_sum = merge_backward(
        grad_merged, merge_saved, merge_gain, merge_weight
    )
    grad_fine_out = rotate_ahead(grad_fine_grid)
    grad_rolled_fine, fine_gain_sum, fine_qkv_sum, fine_proj_sum = block_backward(
        grad_fine_out,
        rolled_fine,
        fine_gain,
        fine_qkv,
        fine_proj,
        fine_saved,
        fine_offset,
        fine_total,
        HF,
    )
    grad_tokens = rotate_back(grad_rolled_fine)
    summed = sum_together(
        (
            fine_gain_sum,
            fine_qkv_sum,
            fine_proj_sum,
            merge_gain_sum,
            merge_weight_sum,
            coarse_gain_sum,
            coarse_qkv_sum,
            coarse_proj_sum,
        ),
        ("lat", "lon"),
        (0, 0, 0, 0, 0, 0, 0, 0),
    )
    fine_gain_sum, fine_qkv_sum, fine_proj_sum = (summed[0], summed[1], summed[2])
    merge_gain_sum, merge_weight_sum = (summed[3], summed[4])
    coarse_gain_sum, coarse_qkv_sum, coarse_proj_sum = (summed[5], summed[6], summed[7])
    return (
        output,
        grad_tokens,
        fine_gain_sum * grad_scale,
        fine_qkv_sum * grad_scale,
        fine_proj_sum * grad_scale,
        merge_gain_sum * grad_scale,
        merge_weight_sum * grad_scale,
        coarse_gain_sum * grad_scale,
        coarse_qkv_sum * grad_scale,
        coarse_proj_sum * grad_scale,
    )


def solution(mesh):
    return jax.shard_map(
        local,
        mesh=mesh,
        in_specs=(
            P("lat", "lon", None),
            P(),
            P(),
            P(),
            P(),
            P(),
            P(),
            P(),
            P(),
            P("lat", "lon", None),
        ),
        out_specs=(
            P("lat", "lon", None),
            P("lat", "lon", None),
            P(("lat", "lon")),
            P(("lat", "lon"), None),
            P(("lat", "lon"), None),
            P(("lat", "lon")),
            P(("lat", "lon"), None),
            P(("lat", "lon")),
            P(("lat", "lon"), None),
            P(("lat", "lon"), None),
        ),
        check_vma=False,
    )
```

```python
import jax
import jax.numpy as jnp
import numpy as np
from jax import lax
from jax.experimental import pallas as pl
from jax.experimental.pallas import tpu as pltpu
from jax.sharding import Mesh, PartitionSpec as P

D = 512
HF = 4
HC = 8
CELLS = 72
WINDOWS = 4
ROWS = 12
COLS = 24
EPSILON = 1e-05
NEGATIVE = -1000000000.0
LOWEST = -3.0e38
INTERPRET = False

F32 = jnp.float32
BF16 = jnp.bfloat16


def window_order():
    return [
        (6 * a + r, 12 * b + c) for a in range(2) for b in range(2) for r in range(6) for c in range(12)
    ]


def patch_order():
    return [
        (2 * r + dr, 2 * c + dc) for dc in range(2) for dr in range(2) for r in range(6) for c in range(12)
    ]


def plain_order(rows, cols):
    return [(r, c) for r in range(rows) for c in range(cols)]


def leading(rows, cols):
    half_r, half_c = (3, 6)
    side = [(r, c) for r in range(half_r, rows) for c in range(half_c)]
    edge = [(r, c) for r in range(half_r) for c in range(half_c, cols)]
    corner = [(r, c) for r in range(half_r) for c in range(half_c)]
    return (side, edge, corner)


def trailing(rows, cols):
    half_r, half_c = (3, 6)
    side = [(r, c) for r in range(rows - half_r) for c in range(cols - half_c, cols)]
    edge = [(r, c) for r in range(rows - half_r, rows) for c in range(cols - half_c)]
    corner = [(r, c) for r in range(rows - half_r, rows) for c in range(cols - half_c, cols)]
    return (side, edge, corner)


SLOTS = (80, 80, 48)
COARSE_AT = (56, 56, 24)
STACK = sum(SLOTS)


def pick(order, cells, places, total):
    where = {cell: i for i, cell in enumerate(order)}
    matrix = np.zeros((total, len(order)), np.float32)
    for place, cell in zip(places, cells):
        matrix[place, where[cell]] = 1.0
    return matrix


def send_matrix(order, pieces, starts):
    cells, places, at = [], [], 0
    for piece, start, slot in zip(pieces, starts, SLOTS):
        cells += piece
        places += [at + start + i for i in range(len(piece))]
        at += slot
    return pick(order, cells, places, STACK)


def take_matrices(own_order, out_cells, pieces, starts, shift, rows, cols):
    own = {cell: i for i, cell in enumerate(own_order)}
    stack, at = {}, 0
    for piece, start, slot in zip(pieces, starts, SLOTS):
        for i, cell in enumerate(piece):
            stack[cell] = at + start + i
        at += slot
    main = np.zeros((len(out_cells), len(own_order)), np.float32)
    halo = np.zeros((len(out_cells), STACK), np.float32)
    for i, cell in enumerate(out_cells):
        if cell is None:
            continue
        r, c = (cell[0] + shift[0], cell[1] + shift[1])
        if 0 <= r < rows and 0 <= c < cols:
            main[i, own[r, c]] = 1.0
        else:
            halo[i, stack[r % rows, c % cols]] = 1.0
    return main, halo


def padded_rows(rows, cols, height):
    return [(r, c) if c < cols else None for r in range(rows) for c in range(height)]


ZERO3 = (0, 0, 0)
PLAIN_F = plain_order(ROWS, COLS)
PLAIN_C = plain_order(6, 12)
TABLES = dict(
    tok_send=send_matrix(PLAIN_F, leading(ROWS, COLS), ZERO3),
    cot_send=send_matrix(PLAIN_C, leading(6, 12), COARSE_AT),
)
TABLES["tok_main"], TABLES["tok_halo"] = take_matrices(
    PLAIN_F, window_order(), leading(ROWS, COLS), ZERO3, (3, 6), ROWS, COLS
)
TABLES["cot_main"], TABLES["cot_halo"] = take_matrices(
    PLAIN_C, PLAIN_C, leading(6, 12), COARSE_AT, (3, 6), 6, 12
)
TABLES["y_send"] = send_matrix(window_order(), leading(ROWS, COLS), ZERO3)
TABLES["y_main"], TABLES["y_halo"] = take_matrices(
    window_order(), patch_order(), leading(ROWS, COLS), ZERO3, (3, 6), ROWS, COLS
)
TABLES["df_send"] = send_matrix(patch_order(), trailing(ROWS, COLS), ZERO3)
TABLES["df_main"], TABLES["df_halo"] = take_matrices(
    patch_order(), window_order(), trailing(ROWS, COLS), ZERO3, (-3, -6), ROWS, COLS
)
TABLES["out_send"] = send_matrix(PLAIN_C, trailing(6, 12), COARSE_AT)
TABLES["out_main"], TABLES["out_halo"] = take_matrices(
    PLAIN_C, padded_rows(6, 12, 16), trailing(6, 12), COARSE_AT, (-3, -6), 6, 12
)
TABLES["dx_send"] = send_matrix(window_order(), trailing(ROWS, COLS), ZERO3)
TABLES["dx_main"], TABLES["dx_halo"] = take_matrices(
    window_order(), PLAIN_F, trailing(ROWS, COLS), ZERO3, (-3, -6), ROWS, COLS
)


def table(name):
    return jnp.asarray(TABLES[name], BF16)


def mm(a, b):
    return lax.dot_general(a, b, (((1,), (0,)), ((), ())), preferred_element_type=F32)


def mm_nt(a, b):
    return lax.dot_general(a, b, (((1,), (1,)), ((), ())), preferred_element_type=F32)


def mm_tn(a, b):
    return lax.dot_general(a, b, (((0,), (0,)), ((), ())), preferred_element_type=F32)


def rounded(x):
    return x.astype(BF16).astype(F32)


def call(kernel, outs, *args, scratch=()):
    return pl.pallas_call(
        kernel,
        out_shape=[jax.ShapeDtypeStruct(s, d) for s, d in outs],
        scratch_shapes=list(scratch),
        interpret=INTERPRET,
    )(*args)


def normalize(x):
    shifted = x - jnp.mean(x, axis=-1, keepdims=True)
    inverse = lax.rsqrt(jnp.mean(shifted * shifted, axis=-1, keepdims=True) + EPSILON)
    return shifted * inverse, inverse


def normalize_back(d, xhat, inverse):
    return inverse * (
        d - jnp.mean(d, axis=-1, keepdims=True) - xhat * jnp.mean(d * xhat, axis=-1, keepdims=True)
    )


def lane_half():
    lane = lax.broadcasted_iota(jnp.int32, (1, 128), 1)
    low = (lane < 64).astype(F32)
    return low, 1.0 - low


def stacked(x):
    low, high = lane_half()
    pad = jnp.zeros((128 - CELLS, 128), F32)
    return jnp.concatenate([x * low, pad, x * high, pad], axis=0).astype(BF16)


def unstacked(x):
    low, high = lane_half()
    return x[:CELLS] * low + x[128 : 128 + CELLS] * high


def key_lanes():
    lane = lax.broadcasted_iota(jnp.int32, (CELLS, 256), 1)
    return jnp.where(lane >= 128, lane - 128, lane)


def apart(split):
    row = lax.broadcasted_iota(jnp.int32, (CELLS, 256), 0)
    key = key_lanes()
    differ = (row >= CELLS // 2) != (key >= CELLS // 2)
    return jnp.logical_and(differ, split)


def halves(fn, x):
    return jnp.concatenate(
        [jnp.broadcast_to(fn(x[:, :128]), (CELLS, 128)), jnp.broadcast_to(fn(x[:, 128:]), (CELLS, 128))],
        axis=1,
    )


def attend(q, k2, v2, differ):
    scores = mm_nt(q.astype(BF16), k2) * 0.125
    scores = jnp.where(differ, NEGATIVE, scores)
    scores = jnp.where(key_lanes() < CELLS, scores, LOWEST)
    exponent = jnp.exp(scores - halves(lambda s: jnp.max(s, axis=1, keepdims=True), scores))
    weights = exponent / halves(lambda s: jnp.sum(s, axis=1, keepdims=True), exponent)
    return weights, mm(weights.astype(BF16), v2)


def attend_back(q, k2, v2, weights, differ, d):
    d = d.astype(BF16)
    dv = unstacked(mm_tn(weights.astype(BF16), d))
    dw = rounded(mm_nt(d, v2))
    ds = weights * (dw - halves(lambda s: jnp.sum(s, axis=1, keepdims=True), dw * weights))
    ds = jnp.where(differ, 0.0, ds * 0.125).astype(BF16)
    dq = mm(ds, k2)
    dk = unstacked(mm_tn(ds, q.astype(BF16)))
    return dq, dk, dv


def first_kernel(tok, cot, tok_send, cot_send, tok2d, side, edge, corner, cot2d):
    x = tok[...].astype(F32).reshape(ROWS * COLS, D).astype(BF16)
    tok2d[...] = x
    for r in range(6):
        cot2d[pl.ds(12 * r, 12), :] = cot[r].astype(F32)
    y = cot2d[...].astype(BF16)
    stack = (mm(tok_send[...], x) + mm(cot_send[...], y)).astype(BF16)
    side[...] = stack[:80]
    edge[...] = stack[80:160]
    corner[...] = stack[160:]


def fine_forward_kernel(
    seam, x_in, side, edge, corner, gain, wqkv, wproj, t_main, t_halo, y_send,
    x_out, n_out, p_out, w_out, m_out, y_out, side_out, edge_out, corner_out, mixed,
):
    halo = jnp.concatenate([side[...], edge[...], corner[...]], axis=0)
    x = mm(t_main[...], x_in[...]) + mm(t_halo[...], halo)
    x_out[...] = x.astype(BF16)
    xhat, _ = normalize(x)
    n = (xhat * gain[...]).astype(BF16)
    n_out[...] = n
    p_out[...] = rounded(mm(n, wqkv[...]))
    for w in range(WINDOWS):
        differ = apart((seam[0] == 1) if w >= 2 else False)
        for p in range(HF // 2):
            rows = pl.ds(CELLS * w, CELLS)
            q, k, v = (p_out[rows, pl.ds(256 * part + 128 * p, 128)] for part in range(3))
            weights, out = attend(q, stacked(k), stacked(v), differ)
            w_out[2 * w + p] = weights
            mixed[rows, pl.ds(128 * p, 128)] = out
    m = mixed[...].astype(BF16)
    m_out[...] = m
    y = (x + mm(m, wproj[...])).astype(BF16)
    y_out[...] = y
    stack = mm(y_send[...], y).astype(BF16)
    side_out[...] = stack[:80]
    edge_out[...] = stack[80:160]
    corner_out[...] = stack[160:]


def coarse_kernel(
    seam, y_in, side, edge, corner, cot_in, cside, cedge, ccorner,
    mgain, mweight, gain, wqkv, wproj, y_main, y_halo, c_main, c_halo, df_send, out_send,
    y2_out, df_out, side_out, edge_out, corner_out, fac_out, gains_out, packed, mixed, dpacked, wsave,
):
    halo = jnp.concatenate([side[...], edge[...], corner[...]], axis=0)
    patches = mm(y_main[...], y_in[...]) + mm(y_halo[...], halo)
    g = jnp.concatenate([patches[CELLS * i : CELLS * (i + 1)] for i in range(4)], axis=1)
    ghat, ginv = normalize(g)
    mn = (ghat * mgain[...]).astype(BF16)
    z = rounded(mm(mn, mweight[...]))
    zhat, zinv = normalize(z)
    n = (zhat * gain[...]).astype(BF16)
    packed[...] = rounded(mm(n, wqkv[...]))
    differ = apart(seam[0] == 1)
    for p in range(HC // 2):
        lanes = pl.ds(128 * p, 128)
        q, k, v = (packed[:, pl.ds(512 * part + 128 * p, 128)] for part in range(3))
        weights, out = attend(q, stacked(k), stacked(v), differ)
        wsave[p] = weights
        mixed[:, lanes] = out
    m = mixed[...].astype(BF16)
    y2 = (z + mm(m, wproj[...])).astype(BF16)
    y2_out[...] = y2

    chalo = jnp.concatenate([cside[...], cedge[...], ccorner[...]], axis=0)
    dy = mm(c_main[...], cot_in[...].astype(BF16)) + mm(c_halo[...], chalo)
    mixed[...] = rounded(mm_nt(dy.astype(BF16), wproj[...]))
    for p in range(HC // 2):
        q, k, v = (packed[:, pl.ds(512 * part + 128 * p, 128)] for part in range(3))
        grads = attend_back(q, stacked(k), stacked(v), wsave[p], differ, mixed[:, pl.ds(128 * p, 128)])
        for part in range(3):
            dpacked[:, pl.ds(512 * part + 128 * p, 128)] = grads[part]
    dp = dpacked[...].astype(BF16)
    dn = rounded(mm_nt(dp, wqkv[...]))
    gain_sum = jnp.sum(dn * zhat, axis=0, keepdims=True)
    dz = (dy + normalize_back(dn * gain[...], zhat, zinv)).astype(BF16)
    dmn = rounded(mm_nt(dz, mweight[...]))
    mgain_sum = jnp.sum(dmn * ghat, axis=0, keepdims=True)
    dg = normalize_back(dmn * mgain[...], ghat, ginv)
    df = jnp.concatenate([dg[:, D * i : D * (i + 1)] for i in range(4)], axis=0).astype(BF16)
    df_out[...] = df
    stack = (mm(df_send[...], df) + mm(out_send[...], y2)).astype(BF16)
    side_out[...] = stack[:80]
    edge_out[...] = stack[80:160]
    corner_out[...] = stack[160:]
    at = 0
    for piece in (mn, n, m, dz, dp, dy.astype(BF16)):
        fac_out[:, pl.ds(at, piece.shape[1])] = piece
        at += piece.shape[1]
    for i in range(4):
        gains_out[pl.ds(1 + i, 1), :] = mgain_sum[:, D * i : D * (i + 1)]
    gains_out[pl.ds(0, 1), :] = gain_sum
    gains_out[pl.ds(5, 3), :] = jnp.zeros((3, D), F32)


def fine_backward_kernel(
    seam, df_in, side, edge, corner, x_in, p_in, w_in, gain, wqkv, wproj, d_main, d_halo, dx_send, gains_in,
    dx_out, side_out, edge_out, corner_out, fac_out, gains_out, dmixed, dpacked,
):
    halo = jnp.concatenate([side[...], edge[...], corner[...]], axis=0)
    dy = mm(d_main[...], df_in[...]) + mm(d_halo[...], halo)
    dmixed[...] = rounded(mm_nt(dy.astype(BF16), wproj[...]))
    for w in range(WINDOWS):
        differ = apart((seam[0] == 1) if w >= 2 else False)
        for p in range(HF // 2):
            rows = pl.ds(CELLS * w, CELLS)
            q, k, v = (p_in[rows, pl.ds(256 * part + 128 * p, 128)] for part in range(3))
            d = dmixed[rows, pl.ds(128 * p, 128)]
            grads = attend_back(q, stacked(k), stacked(v), w_in[2 * w + p], differ, d)
            for part in range(3):
                dpacked[rows, pl.ds(256 * part + 128 * p, 128)] = grads[part]
    dp = dpacked[...].astype(BF16)
    dn = rounded(mm_nt(dp, wqkv[...]))
    xhat, inverse = normalize(x_in[...].astype(F32))
    gains_out[...] = gains_in[...]
    gains_out[pl.ds(5, 1), :] = jnp.sum(dn * xhat, axis=0, keepdims=True)
    dx = (dy + normalize_back(dn * gain[...], xhat, inverse)).astype(BF16)
    dx_out[...] = dx
    stack = mm(dx_send[...], dx).astype(BF16)
    side_out[...] = stack[:80]
    edge_out[...] = stack[80:160]
    corner_out[...] = stack[160:]
    fac_out[:, pl.ds(0, 768)] = dp
    fac_out[:, pl.ds(768, D)] = dy.astype(BF16)


def spread(width, place, block, wide, stride, offset, core):
    source = lax.broadcasted_iota(jnp.int32, (width, wide), 0)
    target = lax.broadcasted_iota(jnp.int32, (width, wide), 1)
    group = target // stride
    i = target - group * stride - offset
    inside = jnp.logical_and(i >= 0, i < block)
    match = source == (2 * group + core) * block + i
    return jnp.where(jnp.logical_and(inside, match), 1.0, 0.0).astype(BF16)


def both(own, other, lanes):
    return jnp.concatenate([own[:, lanes].astype(F32), other[:, lanes].astype(F32)], axis=0).astype(BF16)


def coarse_weights_kernel(place, own, other, out):
    core = place[0]
    groups = out.shape[0]
    rows = out.shape[1] // 2
    share = D // (2 * groups)
    at = lambda start, size: both(own, other, pl.ds(start, size))
    dz = at(2048 + 1024, D)
    block = spread(D, core, rows, D // 2, rows, 0, core)
    for b in range(4):
        left = mm(at(D * b, D), block).astype(BF16)
        g = D // 2 // rows
        out[pl.ds(g * b, g), pl.ds(0, rows), :] = mm_tn(left, dz).reshape(g, rows, D).astype(BF16)
    n = at(2048, D)
    m = at(2048 + D, D)
    total = None
    for j in range(4):
        right = at(2048 + 1536 + D * j, D)
        sel = spread(D, core, share, groups * rows, rows, share * j, core)
        left = mm(n if j < 3 else m, sel).astype(BF16)
        term = mm_tn(left, right)
        total = term if total is None else total + term
    out[:, pl.ds(rows, rows), :] = total.reshape(groups, rows, D).astype(BF16)


def fine_weights_kernel(place, n_own, n_other, m_own, m_other, own, other, gains, gains_other, out, chunks):
    core = place[0]
    groups = out.shape[0]
    rows = out.shape[1]
    share = D // (2 * groups)
    n = both(n_own, n_other, pl.ds(0, D))
    m = both(m_own, m_other, pl.ds(0, 256))
    total = None
    for j in range(3):
        right = both(own, other, pl.ds(256 * j, 256))
        left = mm(n, spread(D, core, share, groups * rows, rows, share * j, core)).astype(BF16)
        term = mm_tn(left, right)
        total = term if total is None else total + term
    for h in range(2):
        right = both(own, other, pl.ds(768 + 256 * h, 256))
        offset = 3 * share + (share // 2) * h
        left = mm(m, spread(256, core, share // 2, groups * rows, rows, offset, core)).astype(BF16)
        total = total + mm_tn(left, right)
    out[:, :, pl.ds(0, 256)] = total.reshape(groups, rows, 256).astype(BF16)
    both_gains = gains[...] + gains_other[...]
    for r in range(6):
        for q in range(4):
            chunks[pl.ds(4 * r + q, 1), :] = both_gains[r : r + 1, 128 * q : 128 * (q + 1)]
    chunks[pl.ds(24, 8), :] = jnp.zeros((8, 128), F32)
    target = lax.broadcasted_iota(jnp.int32, (groups * rows, 32), 0)
    source = lax.broadcasted_iota(jnp.int32, (groups * rows, 32), 1)
    g = target // rows
    r = target - g * rows
    device = 2 * g + core
    want = jnp.where(
        r == 0,
        device * share // 128,
        jnp.where(r == 1, 4 + device * 4 * share // 128, jnp.where(r == 2, 20 + device * share // 128, -1)),
    )
    choose = jnp.where(source == want, 1.0, 0.0).astype(BF16)
    out[:, :, pl.ds(256, 128)] = (
        mm(choose, chunks[...].astype(BF16)).reshape(groups, rows, 128).astype(BF16)
    )


def total_of(ref):
    def step(i, acc):
        return acc + ref[i].astype(F32)

    return lax.fori_loop(1, ref.shape[0], step, ref[0].astype(F32))


def last_kernel(
    scale, coarse, fine, y2, side, edge, corner, dx, dside, dedge, dcorner, out_main, out_halo, dx_main, dx_halo,
    out, grad, fqkv, fproj, merge, cqkv, cproj, gains,
):
    factor = scale[0]
    rows = coarse.shape[1] // 2
    share = rows // 4
    total = total_of(coarse) * factor
    merge[...] = total[:rows]
    for j in range(3):
        cqkv[:, pl.ds(D * j, D)] = total[rows + share * j : rows + share * (j + 1)]
    cproj[...] = total[rows + 3 * share :]
    total = total_of(fine) * factor
    for j in range(3):
        fqkv[:, pl.ds(256 * j, 256)] = total[share * j : share * (j + 1), :256]
    for h in range(2):
        start = 3 * share + share // 2 * h
        fproj[:, pl.ds(256 * h, 256)] = total[start : start + share // 2, :256]
    gains[...] = total[:8, 256:]
    halo = jnp.concatenate([side[...], edge[...], corner[...]], axis=0)
    y = mm(out_main[...], y2[...]) + mm(out_halo[...], halo)
    for r in range(6):
        out[r] = y[16 * r : 16 * r + 12].astype(BF16)
    halo = jnp.concatenate([dside[...], dedge[...], dcorner[...]], axis=0)
    d = mm(dx_main[...], dx[...]) + mm(dx_halo[...], halo)
    grad[...] = d.reshape(ROWS, COLS, D).astype(BF16)


SEAM = pl.BlockSpec(memory_space=pltpu.SMEM)


def scalar_call(kernel, outs, scalar, *args, scratch=()):
    vmem = pl.BlockSpec(memory_space=pltpu.VMEM)
    return pl.pallas_call(
        kernel,
        out_shape=[jax.ShapeDtypeStruct(s, d) for s, d in outs],
        in_specs=[SEAM] + [vmem] * len(args),
        out_specs=[vmem] * len(outs),
        scratch_shapes=list(scratch),
        interpret=INTERPRET,
    )(scalar, *args)


PIECES = [((s, D), BF16) for s in SLOTS]


def exchange(pieces, step):
    lat = lax.axis_size("lat")
    pair = lax.axis_size("pair")
    lon = 2 * pair
    arrived = []
    for piece, (dr, dc) in zip(pieces, ((0, 1), (1, 0), (1, 1))):
        pairs = []
        for r in range(lat):
            for c in range(lon):
                to = ((r + step * dr) % lat) * lon + (c + step * dc) % lon
                pairs.append((r * lon + c, to))
        arrived.append(lax.ppermute(piece, ("lat", "pair", "core"), pairs))
    return arrived


def partner(value):
    return lax.ppermute(value, "core", [(0, 1), (1, 0)])


def local(
    tokens, fine_gain, fine_qkv, fine_proj, merge_gain, merge_weight, coarse_gain, coarse_qkv, coarse_proj, cotangent
):
    lat_count = lax.axis_size("lat")
    groups = lat_count * lax.axis_size("pair")
    share = D // (2 * groups)
    rows = 4 * share
    seam = (lax.axis_index("lat") == lat_count - 1).astype(jnp.int32).reshape(1)
    core = lax.axis_index("core").astype(jnp.int32).reshape(1)
    grad_scale = (ROWS * COLS * 2 * groups // 4) ** (-0.5)
    fgain, mgain, cgain = (v.reshape(1, -1) for v in (fine_gain, merge_gain, coarse_gain))
    cells = WINDOWS * CELLS

    tok, *pieces, cot = call(
        first_kernel,
        [((cells, D), BF16)] + PIECES + [((CELLS, D), F32)],
        tokens, cotangent, table("tok_send"), table("cot_send"),
    )
    ahead = exchange(pieces, -1)
    x, n, p, w, m, y, *pieces = scalar_call(
        fine_forward_kernel,
        [
            ((cells, D), BF16), ((cells, D), BF16), ((cells, 768), F32), ((8, CELLS, 256), F32),
            ((cells, 256), BF16), ((cells, D), BF16),
        ]
        + PIECES,
        seam, tok, *ahead, fgain, fine_qkv, fine_proj, table("tok_main"), table("tok_halo"), table("y_send"),
        scratch=[pltpu.VMEM((cells, 256), F32)],
    )
    merged = exchange(pieces, -1)
    n_other, m_other = (partner(n), partner(m))
    y2, df, *rest = scalar_call(
        coarse_kernel,
        [((CELLS, D), BF16), ((cells, D), BF16)] + PIECES + [((CELLS, 5632), BF16), ((8, D), F32)],
        seam, y, *merged, cot, *ahead, mgain, merge_weight, cgain, coarse_qkv, coarse_proj,
        table("y_main"), table("y_halo"), table("cot_main"), table("cot_halo"), table("df_send"), table("out_send"),
        scratch=[
            pltpu.VMEM((CELLS, 1536), F32), pltpu.VMEM((CELLS, D), F32), pltpu.VMEM((CELLS, 1536), F32),
            pltpu.VMEM((4, CELLS, 256), F32),
        ],
    )
    pieces, fac, gains = (rest[:3], rest[3], rest[4])
    back = exchange(pieces, 1)
    fac_other = partner(fac)
    (coarse_part,) = scalar_call(
        coarse_weights_kernel, [((groups, 2 * rows, D), BF16)], core, fac, fac_other
    )
    dx, *rest = scalar_call(
        fine_backward_kernel,
        [((cells, D), BF16)] + PIECES + [((cells, 1280), BF16), ((8, D), F32)],
        seam, df, *back, x, p, w, fgain, fine_qkv, fine_proj, table("df_main"), table("df_halo"), table("dx_send"),
        gains,
        scratch=[pltpu.VMEM((cells, 256), F32), pltpu.VMEM((cells, 768), F32)],
    )
    pieces, fac, gains = (rest[:3], rest[3], rest[4])
    ended = exchange(pieces, 1)
    fac_other, gains_other = (partner(fac), partner(gains))
    (fine_part,) = scalar_call(
        fine_weights_kernel, [((groups, rows, 384), BF16)],
        core, n, n_other, m, m_other, fac, fac_other, gains, gains_other,
        scratch=[pltpu.VMEM((32, 128), F32)],
    )
    coarse_sum = lax.all_to_all(coarse_part, ("lat", "pair"), 0, 0)
    fine_sum = lax.all_to_all(fine_part, ("lat", "pair"), 0, 0)
    output, grad, fqkv, fproj, merge, cqkv, cproj, gain_sums = scalar_call(
        last_kernel,
        [
            ((6, 12, D), BF16), ((ROWS, COLS, D), BF16), ((share, 768), F32), ((share // 2, D), F32),
            ((rows, D), F32), ((share, 1536), F32), ((share, D), F32), ((8, 128), F32),
        ],
        jnp.full((1,), grad_scale, F32), coarse_sum, fine_sum, y2, *back, dx, *ended,
        table("out_main"), table("out_halo"), table("dx_main"), table("dx_halo"),
    )
    device = (lax.axis_index("lat") * lax.axis_size("pair") + lax.axis_index("pair")) * 2 + lax.axis_index("core")
    cg = lax.dynamic_slice(gain_sums[0], (device * share % 128,), (share,))
    mg = lax.dynamic_slice(gain_sums[1], (device * rows % 128,), (rows,))
    fg = lax.dynamic_slice(gain_sums[2], (device * share % 128,), (share,))
    return (output, grad, fg, fqkv, fproj, mg, merge, cg, cqkv, cproj)


def solution(mesh):
    lat, lon = (mesh.shape["lat"], mesh.shape["lon"])
    split = Mesh(mesh.devices.reshape(lat, lon // 2, 2), ("lat", "pair", "core"))
    lon = ("pair", "core")
    grid = P("lat", lon, None)
    whole = ("lat", "pair", "core")
    return jax.shard_map(
        local,
        mesh=split,
        in_specs=(grid, P(), P(), P(), P(), P(), P(), P(), P(), grid),
        out_specs=(
            grid, grid, P(whole), P(whole, None), P(whole, None), P(whole), P(whole, None), P(whole),
            P(whole, None), P(whole, None),
        ),
        check_vma=False,
    )
```

```python
import jax
import jax.numpy as jnp
import numpy as np
from jax import lax
from jax.experimental import pallas as pl
from jax.experimental.pallas import tpu as pltpu
from jax.sharding import Mesh, PartitionSpec as P

D = 512
HF = 4
HC = 8
CELLS = 72
TALL = 80
WINDOWS = 4
ROWS = 12
COLS = 24
EPSILON = 1e-05
NEGATIVE = -1000000000.0
LOWEST = -3.0e38
INTERPRET = False
VMEM_LIMIT = 12 * 1024 * 1024
FLOPS = 5_000_000_000
BYTES = 4_000_000


F32 = jnp.float32
BF16 = jnp.bfloat16


def window_order():
    return [
        (6 * a + r, 12 * b + c) for a in range(2) for b in range(2) for r in range(6) for c in range(12)
    ]


def patch_order():
    return [
        (2 * r + dr, 2 * c + dc) for dc in range(2) for dr in range(2) for r in range(6) for c in range(12)
    ]


def plain_order(rows, cols):
    return [(r, c) for r in range(rows) for c in range(cols)]


def leading(rows, cols):
    half_r, half_c = (3, 6)
    side = [(r, c) for r in range(half_r, rows) for c in range(half_c)]
    edge = [(r, c) for r in range(half_r) for c in range(half_c, cols)]
    corner = [(r, c) for r in range(half_r) for c in range(half_c)]
    return (side, edge, corner)


def trailing(rows, cols):
    half_r, half_c = (3, 6)
    side = [(r, c) for r in range(rows - half_r) for c in range(cols - half_c, cols)]
    edge = [(r, c) for r in range(rows - half_r, rows) for c in range(cols - half_c)]
    corner = [(r, c) for r in range(rows - half_r, rows) for c in range(cols - half_c, cols)]
    return (side, edge, corner)


SLOTS = (80, 80, 48)
NARROW = (64, 64, 32)
COARSE_AT = (56, 56, 24)


def pick(order, cells, places, total):
    where = {cell: i for i, cell in enumerate(order)}
    matrix = np.zeros((total, len(order)), np.float32)
    for place, cell in zip(places, cells):
        matrix[place, where[cell]] = 1.0
    return matrix


def send_matrix(order, pieces, starts, slots=SLOTS):
    cells, places, at = [], [], 0
    for piece, start, slot in zip(pieces, starts, slots):
        cells += piece
        places += [at + start + i for i in range(len(piece))]
        at += slot
    return pick(order, cells, places, at)


def take_matrices(own_order, out_cells, pieces, starts, shift, rows, cols, slots=SLOTS):
    own = {cell: i for i, cell in enumerate(own_order)}
    stack, at = {}, 0
    for piece, start, slot in zip(pieces, starts, slots):
        for i, cell in enumerate(piece):
            stack[cell] = at + start + i
        at += slot
    main = np.zeros((len(out_cells), len(own_order)), np.float32)
    halo = np.zeros((len(out_cells), at), np.float32)
    for i, cell in enumerate(out_cells):
        if cell is None:
            continue
        r, c = (cell[0] + shift[0], cell[1] + shift[1])
        if 0 <= r < rows and 0 <= c < cols:
            main[i, own[r, c]] = 1.0
        else:
            halo[i, stack[r % rows, c % cols]] = 1.0
    return main, halo


def padded_rows(rows, cols, height):
    return [(r, c) if c < cols else None for r in range(rows) for c in range(height)]


ZERO3 = (0, 0, 0)
PLAIN_F = plain_order(ROWS, COLS)
PLAIN_C = plain_order(6, 12)
TABLES = dict(
    tok_send=send_matrix(PLAIN_F, leading(ROWS, COLS), ZERO3),
    cot_send=send_matrix(PLAIN_C, leading(6, 12), COARSE_AT),
)
TABLES["tok_main"], TABLES["tok_halo"] = take_matrices(
    PLAIN_F, window_order(), leading(ROWS, COLS), ZERO3, (3, 6), ROWS, COLS
)
TABLES["cot_main"], TABLES["cot_halo"] = take_matrices(
    PLAIN_C, PLAIN_C, leading(6, 12), COARSE_AT, (3, 6), 6, 12
)
TABLES["y_send"] = send_matrix(window_order(), leading(ROWS, COLS), ZERO3, NARROW)
TABLES["y_main"], TABLES["y_halo"] = take_matrices(
    window_order(), patch_order(), leading(ROWS, COLS), ZERO3, (3, 6), ROWS, COLS, NARROW
)
TABLES["df_send"] = send_matrix(patch_order(), trailing(ROWS, COLS), ZERO3)
TABLES["df_main"], TABLES["df_halo"] = take_matrices(
    patch_order(), window_order(), trailing(ROWS, COLS), ZERO3, (-3, -6), ROWS, COLS
)
TABLES["out_send"] = send_matrix(PLAIN_C, trailing(6, 12), COARSE_AT)
TABLES["out_main"], TABLES["out_halo"] = take_matrices(
    PLAIN_C, padded_rows(6, 12, 16), trailing(6, 12), COARSE_AT, (-3, -6), 6, 12
)
TABLES["dx_send"] = send_matrix(window_order(), trailing(ROWS, COLS), ZERO3, NARROW)
TABLES["dx_main"], TABLES["dx_halo"] = take_matrices(
    window_order(), PLAIN_F, trailing(ROWS, COLS), ZERO3, (-3, -6), ROWS, COLS, NARROW
)


def table(name):
    return jnp.asarray(TABLES[name], BF16)


def mm(a, b):
    return lax.dot_general(a, b, (((1,), (0,)), ((), ())), preferred_element_type=F32)


def mm_nt(a, b):
    return lax.dot_general(a, b, (((1,), (1,)), ((), ())), preferred_element_type=F32)


def mm_tn(a, b):
    return lax.dot_general(a, b, (((0,), (0,)), ((), ())), preferred_element_type=F32)


def rounded(x):
    return x.astype(BF16).astype(F32)


def call(kernel, outs, *args, scratch=()):
    return pl.pallas_call(
        kernel,
        out_shape=[jax.ShapeDtypeStruct(s, d) for s, d in outs],
        scratch_shapes=list(scratch),
        compiler_params=pltpu.CompilerParams(vmem_limit_bytes=VMEM_LIMIT),
        cost_estimate=pl.CostEstimate(flops=FLOPS, bytes_accessed=BYTES, transcendentals=0),
        interpret=INTERPRET,
    )(*args)


def cut(stack, *refs):
    at = 0
    for ref in refs:
        ref[...] = stack[at : at + ref.shape[0]]
        at += ref.shape[0]


def normalize(x):
    shifted = x - jnp.mean(x, axis=-1, keepdims=True)
    inverse = lax.rsqrt(jnp.mean(shifted * shifted, axis=-1, keepdims=True) + EPSILON)
    return shifted * inverse, inverse


def normalize_back(d, xhat, inverse):
    return inverse * (
        d - jnp.mean(d, axis=-1, keepdims=True) - xhat * jnp.mean(d * xhat, axis=-1, keepdims=True)
    )


def lane_half():
    lane = lax.broadcasted_iota(jnp.int32, (1, 128), 1)
    low = (lane < 64).astype(F32)
    return low, 1.0 - low


def stacked(x):
    low, high = lane_half()
    pad = jnp.zeros((128 - CELLS, 128), F32)
    return jnp.concatenate([x * low, pad, x * high, pad], axis=0).astype(BF16)


def unstacked(x):
    low, high = lane_half()
    return x[:CELLS] * low + x[128 : 128 + CELLS] * high


def key_lanes():
    lane = lax.broadcasted_iota(jnp.int32, (CELLS, 256), 1)
    return jnp.where(lane >= 128, lane - 128, lane)


def apart(split):
    row = lax.broadcasted_iota(jnp.int32, (CELLS, 256), 0)
    key = key_lanes()
    differ = (row >= CELLS // 2) != (key >= CELLS // 2)
    return jnp.logical_and(differ, split)


def halves(fn, x):
    return jnp.concatenate(
        [jnp.broadcast_to(fn(x[:, :128]), (CELLS, 128)), jnp.broadcast_to(fn(x[:, 128:]), (CELLS, 128))],
        axis=1,
    )


def attend(q, k2, v2, differ):
    scores = mm_nt(q.astype(BF16), k2) * 0.125
    scores = jnp.where(differ, NEGATIVE, scores)
    scores = jnp.where(key_lanes() < CELLS, scores, LOWEST)
    exponent = jnp.exp(scores - halves(lambda s: jnp.max(s, axis=1, keepdims=True), scores))
    weights = exponent / halves(lambda s: jnp.sum(s, axis=1, keepdims=True), exponent)
    return weights, mm(weights.astype(BF16), v2)


def attend_back(q, k2, v2, weights, differ, d):
    d = d.astype(BF16)
    dv = unstacked(mm_tn(weights.astype(BF16), d))
    dw = rounded(mm_nt(d, v2))
    ds = weights * (dw - halves(lambda s: jnp.sum(s, axis=1, keepdims=True), dw * weights))
    ds = jnp.where(differ, 0.0, ds * 0.125).astype(BF16)
    dq = mm(ds, k2)
    dk = unstacked(mm_tn(ds, q.astype(BF16)))
    return dq, dk, dv


def first_kernel(tok, cot, tok_send, cot_send, tok2d, side, edge, corner, cot2d):
    x = tok[...].astype(F32).reshape(ROWS * COLS, D).astype(BF16)
    tok2d[...] = x
    for r in range(6):
        cot2d[pl.ds(12 * r, 12), :] = cot[r].astype(F32)
    y = cot2d[...].astype(BF16)
    stack = (mm(tok_send[...], x) + mm(cot_send[...], y)).astype(BF16)
    cut(stack, side, edge, corner)


def fine_forward_kernel(
    seam, x_in, side, edge, corner, gain, wqkv, wproj, t_main, t_halo, y_send,
    x_out, n_out, p_out, w_out, m_out, y_out, side_out, edge_out, corner_out, mixed,
):
    halo = jnp.concatenate([side[...], edge[...], corner[...]], axis=0)
    x = mm(t_main[...], x_in[...]) + mm(t_halo[...], halo)
    x_out[...] = x.astype(BF16)
    xhat, _ = normalize(x)
    n = (xhat * gain[...]).astype(BF16)
    n_out[...] = n
    p_out[...] = rounded(mm(n, wqkv[...]))
    for w in range(WINDOWS):
        differ = apart((seam[0] == 1) if w >= 2 else False)
        for p in range(HF // 2):
            rows = pl.ds(CELLS * w, CELLS)
            q, k, v = (p_out[rows, pl.ds(256 * part + 128 * p, 128)] for part in range(3))
            weights, out = attend(q, stacked(k), stacked(v), differ)
            w_out[2 * w + p] = weights
            mixed[rows, pl.ds(128 * p, 128)] = out
    m = mixed[...].astype(BF16)
    m_out[...] = m
    y = (x + mm(m, wproj[...])).astype(BF16)
    y_out[...] = y
    stack = mm(y_send[...], y).astype(BF16)
    cut(stack, side_out, edge_out, corner_out)


def coarse_kernel(
    seam, y_in, side, edge, corner, cot_in, cside, cedge, ccorner,
    mgain, mweight, gain, wqkv, wproj, y_main, y_halo, c_main, c_halo, df_send, out_send,
    y2_out, df_out, side_out, edge_out, corner_out, fac_out, gains_out, packed, mixed, dpacked, wsave,
):
    halo = jnp.concatenate([side[...], edge[...], corner[...]], axis=0)
    patches = mm(y_main[...], y_in[...]) + mm(y_halo[...], halo)
    g = jnp.concatenate([patches[CELLS * i : CELLS * (i + 1)] for i in range(4)], axis=1)
    ghat, ginv = normalize(g)
    mn = (ghat * mgain[...]).astype(BF16)
    z = rounded(mm(mn, mweight[...]))
    zhat, zinv = normalize(z)
    n = (zhat * gain[...]).astype(BF16)
    packed[...] = rounded(mm(n, wqkv[...]))
    differ = apart(seam[0] == 1)
    for p in range(HC // 2):
        lanes = pl.ds(128 * p, 128)
        q, k, v = (packed[:, pl.ds(512 * part + 128 * p, 128)] for part in range(3))
        weights, out = attend(q, stacked(k), stacked(v), differ)
        wsave[p] = weights
        mixed[:, lanes] = out
    m = mixed[...].astype(BF16)
    y2 = (z + mm(m, wproj[...])).astype(BF16)
    y2_out[...] = y2

    chalo = jnp.concatenate([cside[...], cedge[...], ccorner[...]], axis=0)
    dy = mm(c_main[...], cot_in[...].astype(BF16)) + mm(c_halo[...], chalo)
    mixed[...] = rounded(mm_nt(dy.astype(BF16), wproj[...]))
    for p in range(HC // 2):
        q, k, v = (packed[:, pl.ds(512 * part + 128 * p, 128)] for part in range(3))
        grads = attend_back(q, stacked(k), stacked(v), wsave[p], differ, mixed[:, pl.ds(128 * p, 128)])
        for part in range(3):
            dpacked[:, pl.ds(512 * part + 128 * p, 128)] = grads[part]
    dp = dpacked[...].astype(BF16)
    dn = rounded(mm_nt(dp, wqkv[...]))
    gain_sum = jnp.sum(dn * zhat, axis=0, keepdims=True)
    dz = (dy + normalize_back(dn * gain[...], zhat, zinv)).astype(BF16)
    dmn = rounded(mm_nt(dz, mweight[...]))
    mgain_sum = jnp.sum(dmn * ghat, axis=0, keepdims=True)
    dg = normalize_back(dmn * mgain[...], ghat, ginv)
    df = jnp.concatenate([dg[:, D * i : D * (i + 1)] for i in range(4)], axis=0).astype(BF16)
    df_out[...] = df
    stack = (mm(df_send[...], df) + mm(out_send[...], y2)).astype(BF16)
    cut(stack, side_out, edge_out, corner_out)
    at = 0
    for piece in (mn, n, m, dz, dp, dy.astype(BF16)):
        fac_out[pl.ds(0, CELLS), pl.ds(at, piece.shape[1])] = piece
        at += piece.shape[1]
    fac_out[pl.ds(CELLS, TALL - CELLS), :] = jnp.zeros((TALL - CELLS, at), BF16)
    for i in range(4):
        gains_out[pl.ds(1 + i, 1), :] = mgain_sum[:, D * i : D * (i + 1)]
    gains_out[pl.ds(0, 1), :] = gain_sum
    gains_out[pl.ds(5, 3), :] = jnp.zeros((3, D), F32)


def fine_backward_kernel(
    seam, df_in, side, edge, corner, x_in, p_in, w_in, gain, wqkv, wproj, d_main, d_halo, dx_send, gains_in,
    dx_out, side_out, edge_out, corner_out, fac_out, gains_out, dmixed, dpacked,
):
    halo = jnp.concatenate([side[...], edge[...], corner[...]], axis=0)
    dy = mm(d_main[...], df_in[...]) + mm(d_halo[...], halo)
    dmixed[...] = rounded(mm_nt(dy.astype(BF16), wproj[...]))
    for w in range(WINDOWS):
        differ = apart((seam[0] == 1) if w >= 2 else False)
        for p in range(HF // 2):
            rows = pl.ds(CELLS * w, CELLS)
            q, k, v = (p_in[rows, pl.ds(256 * part + 128 * p, 128)] for part in range(3))
            d = dmixed[rows, pl.ds(128 * p, 128)]
            grads = attend_back(q, stacked(k), stacked(v), w_in[2 * w + p], differ, d)
            for part in range(3):
                dpacked[rows, pl.ds(256 * part + 128 * p, 128)] = grads[part]
    dp = dpacked[...].astype(BF16)
    dn = rounded(mm_nt(dp, wqkv[...]))
    xhat, inverse = normalize(x_in[...].astype(F32))
    gains_out[...] = gains_in[...]
    gains_out[pl.ds(5, 1), :] = jnp.sum(dn * xhat, axis=0, keepdims=True)
    dx = (dy + normalize_back(dn * gain[...], xhat, inverse)).astype(BF16)
    dx_out[...] = dx
    stack = mm(dx_send[...], dx).astype(BF16)
    cut(stack, side_out, edge_out, corner_out)
    fac_out[:, pl.ds(0, 768)] = dp
    fac_out[:, pl.ds(768, D)] = dy.astype(BF16)


def one_hot(want, width):
    lane = lax.broadcasted_iota(jnp.int32, (want.shape[0], width), 1)
    return jnp.where(lane == want, 1.0, 0.0).astype(BF16)


def own_rows(share, width, core, by_group):
    count = width // 2
    groups = count // share
    row = lax.broadcasted_iota(jnp.int32, (count, 1), 0)
    low = share if by_group else groups
    high_part = lax.shift_right_logical(row, low.bit_length() - 1)
    low_part = lax.bitwise_and(row, low - 1)
    group, i = (high_part, low_part) if by_group else (low_part, high_part)
    return one_hot((2 * group + core) * share + i, width)


def coarse_weights_kernel(place, own, other, merge_out, out, lines):
    core = place[0]
    groups, rows = out.shape[:2]
    share = D // (2 * groups)

    def at(start, size):
        return jnp.concatenate([own[:, pl.ds(start, size)], other[:, pl.ds(start, size)]], axis=0)

    dz = at(2048 + 1024, D)
    select = own_rows(rows, D, core, True)
    g = D // 2 // rows
    for b in range(4):
        left = mm_nt(select, at(D * b, D)).astype(BF16)
        merge_out[pl.ds(g * b, g), :, :] = mm(left, dz).reshape(g, rows, D).astype(BF16)
    select = own_rows(share, D, core, False)
    n = mm_nt(select, at(2048, D)).astype(BF16)
    m = mm_nt(select, at(2048 + D, D)).astype(BF16)
    for j in range(4):
        part = mm(n if j < 3 else m, at(2048 + 1536 + D * j, D))
        for i in range(share):
            for h in range(4):
                lines[pl.ds(groups * rows * h + share * j + i, groups, rows), :] = part[groups * i : groups * (i + 1), 128 * h : 128 * h + 128]
    for h in range(4):
        out[:, :, pl.ds(128 * h, 128)] = lines[pl.ds(groups * rows * h, groups * rows), :].reshape(groups, rows, 128).astype(BF16)


def fine_weights_kernel(
    place, coarse, n_own, n_other, m_own, m_other, own, other, gains, gains_other, out, chunks, lines
):
    core = place[0]
    groups = out.shape[0]
    rows = 8
    share = D // (2 * groups)
    top = coarse.shape[1]
    out[:, pl.ds(0, top), pl.ds(0, D)] = coarse[...]
    out[:, pl.ds(0, top), pl.ds(D, 128)] = jnp.zeros((groups, top, 128), BF16)
    select = own_rows(share, D, core, False)
    dp = lambda ref: ref[:, pl.ds(0, 768)]
    dy = lambda ref: ref[:, pl.ds(768, D)]
    n = [mm_nt(select, ref[...]).astype(BF16) for ref in (n_own, n_other)]
    part = mm(n[0], dp(own)) + mm(n[1], dp(other))
    half = share // 2
    for i in range(share):
        line = part[groups * i : groups * (i + 1)]
        for h in range(4):
            lines[pl.ds(groups * rows * h + i, groups, rows), :] = line[:, 128 * h : 128 * h + 128]
        for h in range(2):
            lines[pl.ds(groups * rows * (2 * (i // half) + h) + share + i % half, groups, rows), :] = line[:, 512 + 128 * h : 640 + 128 * h]
    select = own_rows(half, 256, core, False)
    m = [mm_nt(select, ref[...]).astype(BF16) for ref in (m_own, m_other)]
    part = mm(m[0], dy(own)) + mm(m[1], dy(other))
    for i in range(half):
        line = part[groups * i : groups * (i + 1)]
        for h in range(4):
            lines[pl.ds(groups * rows * h + share + half + i, groups, rows), :] = line[:, 128 * h : 128 * h + 128]
    for h in range(4):
        out[:, pl.ds(top, rows), pl.ds(128 * h, 128)] = lines[pl.ds(groups * rows * h, groups * rows), :].reshape(groups, rows, 128).astype(BF16)
    both_gains = gains[...] + gains_other[...]
    for r in range(6):
        for q in range(4):
            chunks[pl.ds(4 * r + q, 1), :] = both_gains[r : r + 1, 128 * q : 128 * (q + 1)]
    chunks[pl.ds(24, 8), :] = jnp.zeros((8, 128), F32)
    row = lax.broadcasted_iota(jnp.int32, (groups * rows, 1), 0)
    device = 2 * lax.shift_right_logical(row, 3) + core
    r = lax.bitwise_and(row, 7)
    small = lax.shift_right_logical(device * share, 7)
    want = jnp.where(
        r == 0,
        small,
        jnp.where(r == 1, 4 + lax.shift_right_logical(device * share * 4, 7), jnp.where(r == 2, 20 + small, -1)),
    )
    out[:, pl.ds(top, rows), pl.ds(512, 128)] = (
        mm(one_hot(want, 32), chunks[...].astype(BF16)).reshape(groups, rows, 128).astype(BF16)
    )


def total_of(ref):
    def step(i, acc):
        return acc + ref[i].astype(F32)

    return lax.fori_loop(1, ref.shape[0], step, ref[0].astype(F32))


def last_kernel(
    place, merge_in, rest, y2, side, edge, corner, dx, dside, dedge, dcorner, out_main, out_halo, dx_main, dx_halo,
    out, grad, fgain, fqkv, fproj, mgain, merge, cgain, cqkv, cproj,
):
    rows = merge_in.shape[1]
    share = rows // 4
    half = share // 2
    factor = (ROWS * COLS * D // share // 4) ** (-0.5)
    merge[...] = total_of(merge_in) * factor
    total = total_of(rest) * factor
    for j in range(3):
        cqkv[:, pl.ds(D * j, D)] = total[share * j : share * (j + 1), :D]
    cproj[...] = total[3 * share : rows, :D]
    total = total[rows:]
    fqkv[:, pl.ds(0, D)] = total[:share, :D]
    for h in range(2):
        fqkv[pl.ds(half * h, half), pl.ds(D, 256)] = total[share : share + half, 256 * h : 256 * h + 256]
    fproj[...] = total[share + half :, :D]
    for r, (ref, size) in enumerate(((cgain, share), (mgain, rows), (fgain, share))):
        first = lax.rem(place[0] * size, 128)
        turned = pltpu.roll(total[:, D:], lax.rem(128 - first, 128), 1)
        ref[...] = turned[r : r + 1, :size]
    halo = jnp.concatenate([side[...], edge[...], corner[...]], axis=0)
    y = mm(out_main[...], y2[...]) + mm(out_halo[...], halo)
    for r in range(6):
        out[r] = y[16 * r : 16 * r + 12].astype(BF16)
    halo = jnp.concatenate([dside[...], dedge[...], dcorner[...]], axis=0)
    d = mm(dx_main[...], dx[...]) + mm(dx_halo[...], halo)
    grad[...] = d.reshape(ROWS, COLS, D).astype(BF16)


SEAM = pl.BlockSpec(memory_space=pltpu.SMEM)


def scalar_call(kernel, outs, scalar, *args, scratch=()):
    vmem = pl.BlockSpec(memory_space=pltpu.VMEM)
    return pl.pallas_call(
        kernel,
        out_shape=[jax.ShapeDtypeStruct(s, d) for s, d in outs],
        in_specs=[SEAM] + [vmem] * len(args),
        out_specs=[vmem] * len(outs),
        scratch_shapes=list(scratch),
        compiler_params=pltpu.CompilerParams(vmem_limit_bytes=VMEM_LIMIT),
        cost_estimate=pl.CostEstimate(flops=FLOPS, bytes_accessed=BYTES, transcendentals=0),
        interpret=INTERPRET,
    )(scalar, *args)


def exchange(pieces, step):
    lat = lax.axis_size("lat")
    pair = lax.axis_size("pair")
    lon = 2 * pair
    arrived = []
    for piece, (dr, dc) in zip(pieces, ((0, 1), (1, 0), (1, 1))):
        pairs = []
        for r in range(lat):
            for c in range(lon):
                to = ((r + step * dr) % lat) * lon + (c + step * dc) % lon
                pairs.append((r * lon + c, to))
        arrived.append(lax.ppermute(piece, ("lat", "pair", "core"), pairs))
    return arrived


def partner(value):
    return lax.ppermute(value, "core", [(0, 1), (1, 0)])


def deal(value):
    return lax.all_to_all(value, ("lat", "pair"), 0, 0)


def local(
    tokens, fine_gain, fine_qkv, fine_proj, merge_gain, merge_weight, coarse_gain, coarse_qkv, coarse_proj, cotangent
):
    lat_count = lax.axis_size("lat")
    groups = lat_count * lax.axis_size("pair")
    share = D // (2 * groups)
    rows = 4 * share
    seam = (lax.axis_index("lat") == lat_count - 1).astype(jnp.int32).reshape(1)
    core = lax.axis_index("core").astype(jnp.int32).reshape(1)
    fgain, mgain, cgain = (v.reshape(1, -1) for v in (fine_gain, merge_gain, coarse_gain))
    cells = WINDOWS * CELLS

    pieces = [((size, D), BF16) for size in SLOTS]
    narrow = [((size, D), BF16) for size in NARROW]
    tok, *sent, cot = call(
        first_kernel,
        [((cells, D), BF16)] + pieces + [((CELLS, D), F32)],
        tokens, cotangent, table("tok_send"), table("cot_send"),
    )
    ahead = exchange(sent, -1)
    x, n, p, w, m, y, *sent = scalar_call(
        fine_forward_kernel,
        [
            ((cells, D), BF16), ((cells, D), BF16), ((cells, 768), F32), ((8, CELLS, 256), F32),
            ((cells, 256), BF16), ((cells, D), BF16),
        ]
        + narrow,
        seam, tok, *ahead, fgain, fine_qkv, fine_proj, table("tok_main"), table("tok_halo"), table("y_send"),
        scratch=[pltpu.VMEM((cells, 256), F32)],
    )
    merged = exchange(sent, -1)
    n_other, m_other = (partner(n), partner(m))
    y2, df, *sent, fac, gains = scalar_call(
        coarse_kernel,
        [((CELLS, D), BF16), ((cells, D), BF16)] + pieces + [((TALL, 5632), BF16), ((8, D), F32)],
        seam, y, *merged, cot, *ahead, mgain, merge_weight, cgain, coarse_qkv, coarse_proj,
        table("y_main"), table("y_halo"), table("cot_main"), table("cot_halo"), table("df_send"), table("out_send"),
        scratch=[
            pltpu.VMEM((CELLS, 1536), F32), pltpu.VMEM((CELLS, D), F32), pltpu.VMEM((CELLS, 1536), F32),
            pltpu.VMEM((4, CELLS, 256), F32),
        ],
    )
    back = exchange(sent, 1)
    merge_part, coarse_part = scalar_call(
        coarse_weights_kernel,
        [((groups, rows, D), BF16)] * 2,
        core, fac, partner(fac),
        scratch=[pltpu.VMEM((4 * groups * rows, 128), F32)],
    )
    merge_sum = deal(merge_part)
    dx, *sent, fac, gains = scalar_call(
        fine_backward_kernel,
        [((cells, D), BF16)] + narrow + [((cells, 1280), BF16), ((8, D), F32)],
        seam, df, *back, x, p, w, fgain, fine_qkv, fine_proj, table("df_main"), table("df_halo"), table("dx_send"),
        gains,
        scratch=[pltpu.VMEM((cells, 256), F32), pltpu.VMEM((cells, 768), F32)],
    )
    ended = exchange(sent, 1)
    (rest,) = scalar_call(
        fine_weights_kernel,
        [((groups, rows + 8, 640), BF16)],
        core, coarse_part, n, n_other, m, m_other, fac, partner(fac), gains, partner(gains),
        scratch=[pltpu.VMEM((32, 128), F32), pltpu.VMEM((4 * groups * 8, 128), F32)],
    )
    rest_sum = deal(rest)
    device = (lax.axis_index("lat") * lax.axis_size("pair") + lax.axis_index("pair")) * 2 + lax.axis_index("core")
    output, grad, fg, fqkv, fproj, mg, merge, cg, cqkv, cproj = scalar_call(
        last_kernel,
        [
            ((6, 12, D), BF16), ((ROWS, COLS, D), BF16), ((1, share), F32), ((share, 768), F32),
            ((share // 2, D), F32), ((1, rows), F32), ((rows, D), F32), ((1, share), F32), ((share, 1536), F32),
            ((share, D), F32),
        ],
        device.astype(jnp.int32).reshape(1), merge_sum, rest_sum, y2, *back, dx, *ended,
        table("out_main"), table("out_halo"), table("dx_main"), table("dx_halo"),
    )
    fg, mg, cg = (v.reshape(-1) for v in (fg, mg, cg))
    return (output, grad, fg, fqkv, fproj, mg, merge, cg, cqkv, cproj)


def solution(mesh):
    lat, lon = (mesh.shape["lat"], mesh.shape["lon"])
    split = Mesh(mesh.devices.reshape(lat, lon // 2, 2), ("lat", "pair", "core"))
    lon = ("pair", "core")
    grid = P("lat", lon, None)
    whole = ("lat", "pair", "core")
    return jax.shard_map(
        local,
        mesh=split,
        in_specs=(grid, P(), P(), P(), P(), P(), P(), P(), P(), grid),
        out_specs=(
            grid, grid, P(whole), P(whole, None), P(whole, None), P(whole), P(whole, None), P(whole),
            P(whole, None), P(whole, None),
        ),
        check_vma=False,
    )
```

```python
import jax
import jax.numpy as jnp
import numpy as np
from jax import lax
from jax.experimental import pallas as pl
from jax.experimental.pallas import tpu as pltpu
from jax.sharding import Mesh, PartitionSpec as P

D = 512
HF = 4
HC = 8
CELLS = 72
TALL = 80
WINDOWS = 4
ROWS = 12
COLS = 24
EPSILON = 1e-05
NEGATIVE = -1000000000.0
LOWEST = -3.0e38
INTERPRET = False
VMEM_SPEC = pl.BlockSpec(memory_space=pltpu.VMEM)
SMEM_SPEC = pl.BlockSpec(memory_space=pltpu.SMEM)
VMEM_LIMIT = 12 * 1024 * 1024
FLOPS = 5_000_000_000
BYTES = 4_000_000


F32 = jnp.float32
BF16 = jnp.bfloat16


def window_order():
    return [
        (6 * a + r, 12 * b + c) for a in range(2) for b in range(2) for r in range(6) for c in range(12)
    ]


def patch_order():
    return [
        (2 * r + dr, 2 * c + dc) for dc in range(2) for dr in range(2) for r in range(6) for c in range(12)
    ]


def plain_order(rows, cols):
    return [(r, c) for r in range(rows) for c in range(cols)]


def leading(rows, cols):
    half_r, half_c = (3, 6)
    side = [(r, c) for r in range(half_r, rows) for c in range(half_c)]
    edge = [(r, c) for r in range(half_r) for c in range(half_c, cols)]
    corner = [(r, c) for r in range(half_r) for c in range(half_c)]
    return (side, edge, corner)


def trailing(rows, cols):
    half_r, half_c = (3, 6)
    side = [(r, c) for r in range(rows - half_r) for c in range(cols - half_c, cols)]
    edge = [(r, c) for r in range(rows - half_r, rows) for c in range(cols - half_c)]
    corner = [(r, c) for r in range(rows - half_r, rows) for c in range(cols - half_c, cols)]
    return (side, edge, corner)


SLOTS = (80, 80, 48)
NARROW = (64, 64, 32)
COARSE_AT = (56, 56, 24)


def pick(order, cells, places, total):
    where = {cell: i for i, cell in enumerate(order)}
    matrix = np.zeros((total, len(order)), np.float32)
    for place, cell in zip(places, cells):
        matrix[place, where[cell]] = 1.0
    return matrix


def send_matrix(order, pieces, starts, slots=SLOTS):
    cells, places, at = [], [], 0
    for piece, start, slot in zip(pieces, starts, slots):
        cells += piece
        places += [at + start + i for i in range(len(piece))]
        at += slot
    return pick(order, cells, places, at)


def take_matrices(own_order, out_cells, pieces, starts, shift, rows, cols, slots=SLOTS):
    own = {cell: i for i, cell in enumerate(own_order)}
    stack, at = {}, 0
    for piece, start, slot in zip(pieces, starts, slots):
        for i, cell in enumerate(piece):
            stack[cell] = at + start + i
        at += slot
    main = np.zeros((len(out_cells), len(own_order)), np.float32)
    halo = np.zeros((len(out_cells), at), np.float32)
    for i, cell in enumerate(out_cells):
        if cell is None:
            continue
        r, c = (cell[0] + shift[0], cell[1] + shift[1])
        if 0 <= r < rows and 0 <= c < cols:
            main[i, own[r, c]] = 1.0
        else:
            halo[i, stack[r % rows, c % cols]] = 1.0
    return main, halo


def padded_rows(rows, cols, height):
    return [(r, c) if c < cols else None for r in range(rows) for c in range(height)]


ZERO3 = (0, 0, 0)
PLAIN_F = plain_order(ROWS, COLS)
PLAIN_C = plain_order(6, 12)
TABLES = dict(
    tok_send=send_matrix(PLAIN_F, leading(ROWS, COLS), ZERO3),
    cot_send=send_matrix(PLAIN_C, leading(6, 12), COARSE_AT),
)
TABLES["tok_main"], TABLES["tok_halo"] = take_matrices(
    PLAIN_F, window_order(), leading(ROWS, COLS), ZERO3, (3, 6), ROWS, COLS
)
TABLES["cot_main"], TABLES["cot_halo"] = take_matrices(
    PLAIN_C, PLAIN_C, leading(6, 12), COARSE_AT, (3, 6), 6, 12
)
TABLES["y_send"] = send_matrix(window_order(), leading(ROWS, COLS), ZERO3, NARROW)
TABLES["y_main"], TABLES["y_halo"] = take_matrices(
    window_order(), patch_order(), leading(ROWS, COLS), ZERO3, (3, 6), ROWS, COLS, NARROW
)
TABLES["df_send"] = send_matrix(patch_order(), trailing(ROWS, COLS), ZERO3)
TABLES["df_main"], TABLES["df_halo"] = take_matrices(
    patch_order(), window_order(), trailing(ROWS, COLS), ZERO3, (-3, -6), ROWS, COLS
)
TABLES["out_send"] = send_matrix(PLAIN_C, trailing(6, 12), COARSE_AT)
TABLES["out_main"], TABLES["out_halo"] = take_matrices(
    PLAIN_C, padded_rows(6, 12, 16), trailing(6, 12), COARSE_AT, (-3, -6), 6, 12
)
TABLES["dx_send"] = send_matrix(window_order(), trailing(ROWS, COLS), ZERO3, NARROW)
TABLES["dx_main"], TABLES["dx_halo"] = take_matrices(
    window_order(), PLAIN_F, trailing(ROWS, COLS), ZERO3, (-3, -6), ROWS, COLS, NARROW
)


def table(name):
    return jnp.asarray(TABLES[name], BF16)


def mm(a, b):
    return lax.dot_general(a, b, (((1,), (0,)), ((), ())), preferred_element_type=F32)


def mm_nt(a, b):
    return lax.dot_general(a, b, (((1,), (1,)), ((), ())), preferred_element_type=F32)


def mm_tn(a, b):
    return lax.dot_general(a, b, (((0,), (0,)), ((), ())), preferred_element_type=F32)


def rounded(x):
    return x.astype(BF16).astype(F32)


def call(kernel, outs, *args, scratch=(), specs=None, limit=None):
    return pl.pallas_call(
        kernel,
        out_shape=[jax.ShapeDtypeStruct(s, d) for s, d in outs],
        in_specs=specs or [VMEM_SPEC] * len(args),
        out_specs=[VMEM_SPEC] * len(outs),
        scratch_shapes=list(scratch),
        compiler_params=pltpu.CompilerParams(vmem_limit_bytes=limit or VMEM_LIMIT),
        cost_estimate=pl.CostEstimate(flops=FLOPS, bytes_accessed=BYTES, transcendentals=0),
        interpret=INTERPRET,
    )(*args)


def scalar_call(kernel, outs, scalar, *args, scratch=()):
    return call(kernel, outs, scalar, *args, scratch=scratch, specs=[SMEM_SPEC] + [VMEM_SPEC] * len(args))


def cut(stack, *refs):
    at = 0
    for ref in refs:
        ref[...] = stack[at : at + ref.shape[0]]
        at += ref.shape[0]


def normalize(x):
    shifted = x - jnp.mean(x, axis=-1, keepdims=True)
    inverse = lax.rsqrt(jnp.mean(shifted * shifted, axis=-1, keepdims=True) + EPSILON)
    return shifted * inverse, inverse


def normalize_back(d, xhat, inverse):
    return inverse * (
        d - jnp.mean(d, axis=-1, keepdims=True) - xhat * jnp.mean(d * xhat, axis=-1, keepdims=True)
    )


def lane_half():
    lane = lax.broadcasted_iota(jnp.int32, (1, 128), 1)
    low = (lane < 64).astype(F32)
    return low, 1.0 - low


def stacked(x):
    low, high = lane_half()
    pad = jnp.zeros((128 - CELLS, 128), F32)
    return jnp.concatenate([x * low, pad, x * high, pad], axis=0).astype(BF16)


def unstacked(x):
    low, high = lane_half()
    return x[:CELLS] * low + x[128 : 128 + CELLS] * high


def key_lanes():
    lane = lax.broadcasted_iota(jnp.int32, (CELLS, 256), 1)
    return jnp.where(lane >= 128, lane - 128, lane)


def apart(split):
    row = lax.broadcasted_iota(jnp.int32, (CELLS, 256), 0)
    key = key_lanes()
    differ = (row >= CELLS // 2) != (key >= CELLS // 2)
    return jnp.logical_and(differ, split)


def halves(fn, x):
    return jnp.concatenate(
        [jnp.broadcast_to(fn(x[:, :128]), (CELLS, 128)), jnp.broadcast_to(fn(x[:, 128:]), (CELLS, 128))],
        axis=1,
    )


def attend(q, k2, v2, differ):
    scores = mm_nt(q.astype(BF16), k2) * 0.125
    scores = jnp.where(differ, NEGATIVE, scores)
    scores = jnp.where(key_lanes() < CELLS, scores, LOWEST)
    exponent = jnp.exp(scores - halves(lambda s: jnp.max(s, axis=1, keepdims=True), scores))
    weights = exponent / halves(lambda s: jnp.sum(s, axis=1, keepdims=True), exponent)
    return weights, mm(weights.astype(BF16), v2)


def attend_back(q, k2, v2, weights, differ, d):
    d = d.astype(BF16)
    dv = unstacked(mm_tn(weights.astype(BF16), d))
    dw = rounded(mm_nt(d, v2))
    ds = weights * (dw - halves(lambda s: jnp.sum(s, axis=1, keepdims=True), dw * weights))
    ds = jnp.where(differ, 0.0, ds * 0.125).astype(BF16)
    dq = mm(ds, k2)
    dk = unstacked(mm_tn(ds, q.astype(BF16)))
    return dq, dk, dv


def first_kernel(
    tok_in, cot_in, tok_send_in, cot_send_in, tok2d, side, edge, corner, cot2d,
    tok, cot, tok_send, cot_send, arrived,
):
    loads = [
        pltpu.make_async_copy(source, target, arrived.at[i])
        for i, (source, target) in enumerate(
            ((tok_in, tok), (cot_in, cot), (tok_send_in, tok_send), (cot_send_in, cot_send))
        )
    ]
    for load in loads:
        load.start()
    for load in loads:
        load.wait()
    x = tok[...].astype(F32).reshape(ROWS * COLS, D).astype(BF16)
    tok2d[...] = x
    for r in range(6):
        cot2d[pl.ds(12 * r, 12), :] = cot[r].astype(F32)
    y = cot2d[...].astype(BF16)
    stack = (mm(tok_send[...], x) + mm(cot_send[...], y)).astype(BF16)
    cut(stack, side, edge, corner)


def fine_forward_kernel(
    place, x_in, side, edge, corner, gain, wqkv, wproj, t_main, t_halo, y_send,
    x_out, n_out, p_out, w_out, m_out, y_out, side_out, edge_out, corner_out, mixed,
):
    halo = jnp.concatenate([side[...], edge[...], corner[...]], axis=0)
    x = mm(t_main[...], x_in[...]) + mm(t_halo[...], halo)
    x_out[...] = x.astype(BF16)
    xhat, _ = normalize(x)
    n = (xhat * gain[...]).astype(BF16)
    n_out[...] = n
    p_out[...] = rounded(mm(n, wqkv[...]))
    for w in range(WINDOWS):
        differ = apart(decode(place)[2] == 1 if w >= 2 else False)
        for p in range(HF // 2):
            rows = pl.ds(CELLS * w, CELLS)
            q, k, v = (p_out[rows, pl.ds(256 * part + 128 * p, 128)] for part in range(3))
            weights, out = attend(q, stacked(k), stacked(v), differ)
            w_out[2 * w + p] = weights
            mixed[rows, pl.ds(128 * p, 128)] = out
    m = mixed[...].astype(BF16)
    m_out[...] = m
    y = (x + mm(m, wproj[...])).astype(BF16)
    y_out[...] = y
    stack = mm(y_send[...], y).astype(BF16)
    cut(stack, side_out, edge_out, corner_out)


def coarse_kernel(
    place, y_in, side, edge, corner, cot_in, cside, cedge, ccorner,
    mgain, mweight, gain, wqkv, wproj, y_main, y_halo, c_main, c_halo, df_send, out_send,
    y2_out, df_out, side_out, edge_out, corner_out, fac_out, gains_out, packed, mixed, dpacked, wsave,
):
    halo = jnp.concatenate([side[...], edge[...], corner[...]], axis=0)
    patches = mm(y_main[...], y_in[...]) + mm(y_halo[...], halo)
    g = jnp.concatenate([patches[CELLS * i : CELLS * (i + 1)] for i in range(4)], axis=1)
    ghat, ginv = normalize(g)
    mn = (ghat * mgain[...]).astype(BF16)
    z = rounded(mm(mn, mweight[...]))
    zhat, zinv = normalize(z)
    n = (zhat * gain[...]).astype(BF16)
    packed[...] = rounded(mm(n, wqkv[...]))
    differ = apart(decode(place)[2] == 1)
    for p in range(HC // 2):
        lanes = pl.ds(128 * p, 128)
        q, k, v = (packed[:, pl.ds(512 * part + 128 * p, 128)] for part in range(3))
        weights, out = attend(q, stacked(k), stacked(v), differ)
        wsave[p] = weights
        mixed[:, lanes] = out
    m = mixed[...].astype(BF16)
    y2 = (z + mm(m, wproj[...])).astype(BF16)
    y2_out[...] = y2

    chalo = jnp.concatenate([cside[...], cedge[...], ccorner[...]], axis=0)
    dy = mm(c_main[...], cot_in[...].astype(BF16)) + mm(c_halo[...], chalo)
    mixed[...] = rounded(mm_nt(dy.astype(BF16), wproj[...]))
    for p in range(HC // 2):
        q, k, v = (packed[:, pl.ds(512 * part + 128 * p, 128)] for part in range(3))
        grads = attend_back(q, stacked(k), stacked(v), wsave[p], differ, mixed[:, pl.ds(128 * p, 128)])
        for part in range(3):
            dpacked[:, pl.ds(512 * part + 128 * p, 128)] = grads[part]
    dp = dpacked[...].astype(BF16)
    dn = rounded(mm_nt(dp, wqkv[...]))
    gain_sum = jnp.sum(dn * zhat, axis=0, keepdims=True)
    dz = (dy + normalize_back(dn * gain[...], zhat, zinv)).astype(BF16)
    dmn = rounded(mm_nt(dz, mweight[...]))
    mgain_sum = jnp.sum(dmn * ghat, axis=0, keepdims=True)
    dg = normalize_back(dmn * mgain[...], ghat, ginv)
    df = jnp.concatenate([dg[:, D * i : D * (i + 1)] for i in range(4)], axis=0).astype(BF16)
    df_out[...] = df
    stack = (mm(df_send[...], df) + mm(out_send[...], y2)).astype(BF16)
    cut(stack, side_out, edge_out, corner_out)
    at = 0
    for piece in (mn, n, m, dz, dp, dy.astype(BF16)):
        fac_out[pl.ds(0, CELLS), pl.ds(at, piece.shape[1])] = piece
        at += piece.shape[1]
    fac_out[pl.ds(CELLS, TALL - CELLS), :] = jnp.zeros((TALL - CELLS, at), BF16)
    for i in range(4):
        gains_out[pl.ds(1 + i, 1), :] = mgain_sum[:, D * i : D * (i + 1)]
    gains_out[pl.ds(0, 1), :] = gain_sum
    gains_out[pl.ds(5, 3), :] = jnp.zeros((3, D), F32)


def fine_backward_kernel(
    place, df_in, side, edge, corner, x_in, p_in, w_in, gain, wqkv, wproj, d_main, d_halo, dx_send, gains_in,
    dx_out, side_out, edge_out, corner_out, fac_out, gains_out, dmixed, dpacked,
):
    halo = jnp.concatenate([side[...], edge[...], corner[...]], axis=0)
    dy = mm(d_main[...], df_in[...]) + mm(d_halo[...], halo)
    dmixed[...] = rounded(mm_nt(dy.astype(BF16), wproj[...]))
    for w in range(WINDOWS):
        differ = apart(decode(place)[2] == 1 if w >= 2 else False)
        for p in range(HF // 2):
            rows = pl.ds(CELLS * w, CELLS)
            q, k, v = (p_in[rows, pl.ds(256 * part + 128 * p, 128)] for part in range(3))
            d = dmixed[rows, pl.ds(128 * p, 128)]
            grads = attend_back(q, stacked(k), stacked(v), w_in[2 * w + p], differ, d)
            for part in range(3):
                dpacked[rows, pl.ds(256 * part + 128 * p, 128)] = grads[part]
    dp = dpacked[...].astype(BF16)
    dn = rounded(mm_nt(dp, wqkv[...]))
    xhat, inverse = normalize(x_in[...].astype(F32))
    gains_out[...] = gains_in[...]
    gains_out[pl.ds(5, 1), :] = jnp.sum(dn * xhat, axis=0, keepdims=True)
    dx = (dy + normalize_back(dn * gain[...], xhat, inverse)).astype(BF16)
    dx_out[...] = dx
    stack = mm(dx_send[...], dx).astype(BF16)
    cut(stack, side_out, edge_out, corner_out)
    fac_out[:, pl.ds(0, 768)] = dp
    fac_out[:, pl.ds(768, D)] = dy.astype(BF16)


def decode(place):
    code = place[0]
    shifted = [code] + [lax.shift_right_logical(code, i) for i in (1, 2, 3)]
    return tuple(lax.bitwise_and(v, 1) for v in shifted[:3]) + (shifted[3],)


def one_hot(want, width):
    lane = lax.broadcasted_iota(jnp.int32, (want.shape[0], width), 1)
    return jnp.where(lane == want, 1.0, 0.0).astype(BF16)


def own_rows(share, width, core, by_group):
    count = width // 2
    groups = count // share
    row = lax.broadcasted_iota(jnp.int32, (count, 1), 0)
    low = share if by_group else groups
    high_part = lax.shift_right_logical(row, low.bit_length() - 1)
    low_part = lax.bitwise_and(row, low - 1)
    group, i = (high_part, low_part) if by_group else (low_part, high_part)
    return one_hot((2 * group + core) * share + i, width)


def coarse_weights_kernel(place, own, other, merge_keep, merge_send, coarse_keep, coarse_send, lines):
    core, parity, _, _ = decode(place)
    block, tall = (merge_keep.shape[0] // 2, merge_keep.shape[1])
    rows = tall // 4
    groups = 4 * block
    share = rows // 4

    def at(start, size):
        return jnp.concatenate([own[:, pl.ds(start, size)], other[:, pl.ds(start, size)]], axis=0)

    def put(b, h, value, same, differs):
        place_of = (pl.ds(block * (b // 2), block), pl.ds(rows * h, rows), slice(None))

        @pl.when(parity == b % 2)
        def _():
            same[place_of] = value

        @pl.when(parity != b % 2)
        def _():
            differs[place_of] = value

    dz = at(2048 + 1024, D)
    select = own_rows(rows, D, core, True)
    for b in range(4):
        left = mm_nt(select, at(D * b, D)).astype(BF16)
        part = mm(left, dz).reshape(block, rows, D).astype(BF16)
        for h in range(4):
            put(b, h, part[:, :, 128 * h : 128 * h + 128], merge_keep, merge_send)
    select = own_rows(share, D, core, False)
    n = mm_nt(select, at(2048, D)).astype(BF16)
    m = mm_nt(select, at(2048 + D, D)).astype(BF16)
    for j in range(4):
        part = mm(n if j < 3 else m, at(2048 + 1536 + D * j, D))
        for i in range(share):
            line = part[groups * i : groups * (i + 1)]
            for h in range(4):
                lines[pl.ds(groups * rows * h + share * j + i, groups, rows), :] = line[:, 128 * h : 128 * h + 128]
    for h in range(4):
        for b in range(4):
            chunk = lines[pl.ds(groups * rows * h + block * rows * b, block * rows), :]
            put(b, h, chunk.reshape(block, rows, 128).astype(BF16), coarse_send, coarse_keep)


def fine_weights_kernel(
    place, merge_keep, merge_came, coarse_keep, coarse_came, n_own, n_other, m_own, m_other, own, other,
    gains, gains_other, out, chunks, lines,
):
    core, parity, _, _ = decode(place)
    groups = out.shape[0]
    block, top = (merge_keep.shape[0] // 2, merge_keep.shape[1])
    rows = 8
    share = D // (2 * groups)
    for k in range(2):
        part = pl.ds(block * k, block)
        merge = merge_keep[part].astype(F32) + merge_came[part].astype(F32)
        coarse = coarse_keep[part].astype(F32) + coarse_came[part].astype(F32)
        out[pl.ds(block * (2 * k + parity), block), pl.ds(0, top), :] = merge.astype(BF16)
        out[pl.ds(block * (2 * k + 1 - parity), block), pl.ds(0, top), :] = coarse.astype(BF16)
    select = own_rows(share, D, core, False)
    dp = lambda ref: ref[:, pl.ds(0, 768)]
    dy = lambda ref: ref[:, pl.ds(768, D)]
    n = [mm_nt(select, ref[...]).astype(BF16) for ref in (n_own, n_other)]
    part = mm(n[0], dp(own)) + mm(n[1], dp(other))
    half = share // 2
    for i in range(share):
        line = part[groups * i : groups * (i + 1)]
        for h in range(4):
            lines[pl.ds(groups * rows * h + i, groups, rows), :] = line[:, 128 * h : 128 * h + 128]
        for h in range(2):
            lines[pl.ds(groups * rows * (2 * (i // half) + h) + share + i % half, groups, rows), :] = line[:, 512 + 128 * h : 640 + 128 * h]
    select = own_rows(half, 256, core, False)
    m = [mm_nt(select, ref[...]).astype(BF16) for ref in (m_own, m_other)]
    part = mm(m[0], dy(own)) + mm(m[1], dy(other))
    for i in range(half):
        line = part[groups * i : groups * (i + 1)]
        for h in range(4):
            lines[pl.ds(groups * rows * h + share + half + i, groups, rows), :] = line[:, 128 * h : 128 * h + 128]
    for h in range(4):
        chunk = lines[pl.ds(groups * rows * h, groups * rows), :]
        out[:, pl.ds(top + rows * h, rows), :] = chunk.reshape(groups, rows, 128).astype(BF16)
    both_gains = gains[...] + gains_other[...]
    for r in range(6):
        for q in range(4):
            chunks[pl.ds(4 * r + q, 1), :] = both_gains[r : r + 1, 128 * q : 128 * (q + 1)]
    chunks[pl.ds(24, 8), :] = jnp.zeros((8, 128), F32)
    row = lax.broadcasted_iota(jnp.int32, (groups * rows, 1), 0)
    device = 2 * lax.shift_right_logical(row, 3) + core
    r = lax.bitwise_and(row, 7)
    small = lax.shift_right_logical(device * share, 7)
    want = jnp.where(
        r == 0,
        small,
        jnp.where(r == 1, 4 + lax.shift_right_logical(device * share * 4, 7), jnp.where(r == 2, 20 + small, -1)),
    )
    out[:, pl.ds(top + 4 * rows, rows), :] = (
        mm(one_hot(want, 32), chunks[...].astype(BF16)).reshape(groups, rows, 128).astype(BF16)
    )


def assemble_kernel(
    y2, side, edge, corner, dx, dside, dedge, dcorner, out_main, out_halo, dx_main, dx_halo, out, grad
):
    halo = jnp.concatenate([side[...], edge[...], corner[...]], axis=0)
    y = mm(out_main[...], y2[...]) + mm(out_halo[...], halo)
    for r in range(6):
        out[r] = y[16 * r : 16 * r + 12].astype(BF16)
    halo = jnp.concatenate([dside[...], dedge[...], dcorner[...]], axis=0)
    d = mm(dx_main[...], dx[...]) + mm(dx_halo[...], halo)
    grad[...] = d.reshape(ROWS, COLS, D).astype(BF16)


def sum_kernel(place, parts, fgain, fqkv, fproj, mgain, merge, cgain, cqkv, cproj):
    _, parity, _, device = decode(place)
    groups = parts.shape[0]
    block = groups // 4
    rows, share = (merge.shape[0], cqkv.shape[0])
    half = share // 2
    top = 4 * rows
    factor = (ROWS * COLS * 2 * groups // 4) ** (-0.5)
    sums = []
    for first in range(2):
        total = None
        for k in range(2):
            for i in range(block):
                term = parts[block * (2 * k + first) + i].astype(F32)
                total = term if total is None else total + term
        sums.append(total * factor)
    same = (jnp.full((top, 128), parity, jnp.int32) == 0)
    first, second = (sums[0][:top], sums[1][:top])
    merged = jnp.where(same, first, second)
    coarse = jnp.where(same, second, first)
    total = sums[0][top:] + sums[1][top:]
    for h in range(4):
        lanes = pl.ds(128 * h, 128)
        merge[:, lanes] = merged[rows * h : rows * (h + 1)]
        for j in range(3):
            cqkv[:, pl.ds(D * j + 128 * h, 128)] = coarse[rows * h + share * j : rows * h + share * (j + 1)]
        cproj[:, lanes] = coarse[rows * h + 3 * share : rows * (h + 1)]
        line = total[8 * h : 8 * h + 8]
        fqkv[:, lanes] = line[:share]
        fqkv[pl.ds(half * (h // 2), half), pl.ds(D + 128 * (h % 2), 128)] = line[share : share + half]
        fproj[:, lanes] = line[share + half : 2 * share]
    for r, (ref, size) in enumerate(((cgain, share), (mgain, rows), (fgain, share))):
        first = lax.rem(device * size, 128)
        turned = pltpu.roll(total[32:40], lax.rem(128 - first, 128), 1)
        ref[...] = turned[r : r + 1, :size]


def exchange(pieces, step):
    lat = lax.axis_size("lat")
    pair = lax.axis_size("pair")
    lon = 2 * pair
    arrived = []
    for piece, (dr, dc) in zip(pieces, ((0, 1), (1, 0), (1, 1))):
        pairs = []
        for r in range(lat):
            for c in range(lon):
                to = ((r + step * dr) % lat) * lon + (c + step * dc) % lon
                pairs.append((r * lon + c, to))
        arrived.append(lax.ppermute(piece, ("lat", "pair", "core"), pairs))
    return arrived


def partner(value):
    return lax.ppermute(value, "core", [(0, 1), (1, 0)])


def fold(value, second):
    ring = lax.axis_size("lat") // 2
    pairs = []
    for z in range(ring):
        step = 1 if z % 2 == (1 if second else 0) else -1
        pairs += [(2 * z + y, 2 * ((z + step) % ring) + y) for y in range(2)]
    return lax.ppermute(value, "lat", pairs)


def deal(value):
    return lax.all_to_all(value, ("lat", "pair"), 0, 0)


def local(
    tokens, fine_gain, fine_qkv, fine_proj, merge_gain, merge_weight, coarse_gain, coarse_qkv, coarse_proj, cotangent
):
    lat_count = lax.axis_size("lat")
    groups = lat_count * lax.axis_size("pair")
    share = D // (2 * groups)
    rows = 4 * share
    lat, core = (lax.axis_index("lat"), lax.axis_index("core"))
    device = (lat * lax.axis_size("pair") + lax.axis_index("pair")) * 2 + core
    parity = lax.bitwise_and(lax.shift_right_logical(lat, 1), 1)
    seam = (lat == lat_count - 1).astype(jnp.int32)
    place = (device * 8 + seam * 4 + parity * 2 + core).astype(jnp.int32).reshape(1)
    fgain, mgain, cgain = (v.reshape(1, -1) for v in (fine_gain, merge_gain, coarse_gain))
    cells = WINDOWS * CELLS

    pieces = [((size, D), BF16) for size in SLOTS]
    narrow = [((size, D), BF16) for size in NARROW]
    tok, *sent, cot = call(
        first_kernel,
        [((cells, D), BF16)] + pieces + [((CELLS, D), F32)],
        *(
            pltpu.with_memory_space_constraint(v, pltpu.HBM)
            for v in (tokens, cotangent, table("tok_send"), table("cot_send"))
        ),
        specs=[pl.BlockSpec(memory_space=pltpu.HBM)] * 4,
        scratch=[
            pltpu.VMEM((ROWS, COLS, D), BF16), pltpu.VMEM((6, 12, D), BF16), pltpu.VMEM((sum(SLOTS), cells), BF16),
            pltpu.VMEM((sum(SLOTS), CELLS), BF16), pltpu.SemaphoreType.DMA((4,)),
        ],
    )
    ahead = exchange(sent, -1)
    x, n, p, w, m, y, *sent = scalar_call(
        fine_forward_kernel,
        [
            ((cells, D), BF16), ((cells, D), BF16), ((cells, 768), F32), ((8, CELLS, 256), F32),
            ((cells, 256), BF16), ((cells, D), BF16),
        ]
        + narrow,
        place, tok, *ahead, fgain, fine_qkv, fine_proj, table("tok_main"), table("tok_halo"), table("y_send"),
        scratch=[pltpu.VMEM((cells, 256), F32)],
    )
    merged = exchange(sent, -1)
    n_other, m_other = (partner(n), partner(m))
    y2, df, *sent, fac, gains = scalar_call(
        coarse_kernel,
        [((CELLS, D), BF16), ((cells, D), BF16)] + pieces + [((TALL, 5632), BF16), ((8, D), F32)],
        place, y, *merged, cot, *ahead, mgain, merge_weight, cgain, coarse_qkv, coarse_proj,
        table("y_main"), table("y_halo"), table("cot_main"), table("cot_halo"), table("df_send"), table("out_send"),
        scratch=[
            pltpu.VMEM((CELLS, 1536), F32), pltpu.VMEM((CELLS, D), F32), pltpu.VMEM((CELLS, 1536), F32),
            pltpu.VMEM((4, CELLS, 256), F32),
        ],
    )
    back = exchange(sent, 1)
    chunk = ((groups // 2, 4 * rows, 128), BF16)
    merge_keep, merge_send, coarse_keep, coarse_send = scalar_call(
        coarse_weights_kernel,
        [chunk] * 4,
        place, fac, partner(fac),
        scratch=[pltpu.VMEM((4 * groups * rows, 128), F32)],
    )
    merge_came = fold(merge_send, False)
    coarse_came = fold(coarse_send, True)
    dx, *sent, fac, gains = scalar_call(
        fine_backward_kernel,
        [((cells, D), BF16)] + narrow + [((cells, 1280), BF16), ((8, D), F32)],
        place, df, *back, x, p, w, fgain, fine_qkv, fine_proj, table("df_main"), table("df_halo"), table("dx_send"),
        gains,
        scratch=[pltpu.VMEM((cells, 256), F32), pltpu.VMEM((cells, 768), F32)],
    )
    ended = exchange(sent, 1)
    (rest,) = scalar_call(
        fine_weights_kernel,
        [((groups, 4 * rows + 40, 128), BF16)],
        place, merge_keep, merge_came, coarse_keep, coarse_came, n, n_other, m, m_other,
        fac, partner(fac), gains, partner(gains),
        scratch=[pltpu.VMEM((32, 128), F32), pltpu.VMEM((4 * groups * 8, 128), F32)],
    )
    parts = deal(rest)
    output, grad = call(
        assemble_kernel,
        [((6, 12, D), BF16), ((ROWS, COLS, D), BF16)],
        y2, *back, dx, *ended, table("out_main"), table("out_halo"), table("dx_main"), table("dx_halo"),
    )
    fg, fqkv, fproj, mg, merge, cg, cqkv, cproj = scalar_call(
        sum_kernel,
        [
            ((1, share), F32), ((share, 768), F32), ((share // 2, D), F32), ((1, rows), F32), ((rows, D), F32),
            ((1, share), F32), ((share, 1536), F32), ((share, D), F32),
        ],
        place, parts,
    )
    fg, mg, cg = (v.reshape(-1) for v in (fg, mg, cg))
    return (output, grad, fg, fqkv, fproj, mg, merge, cg, cqkv, cproj)


def solution(mesh):
    lat, lon = (mesh.shape["lat"], mesh.shape["lon"])
    split = Mesh(mesh.devices.reshape(lat, lon // 2, 2), ("lat", "pair", "core"))
    lon = ("pair", "core")
    grid = P("lat", lon, None)
    whole = ("lat", "pair", "core")
    return jax.shard_map(
        local,
        mesh=split,
        in_specs=(grid, P(), P(), P(), P(), P(), P(), P(), P(), grid),
        out_specs=(
            grid, grid, P(whole), P(whole, None), P(whole, None), P(whole), P(whole, None), P(whole),
            P(whole, None), P(whole, None),
        ),
        check_vma=False,
    )
```

```python
import jax
import jax.numpy as jnp
import numpy as np
from jax import lax
from jax.experimental import pallas as pl
from jax.experimental.pallas import tpu as pltpu
from jax.sharding import Mesh, PartitionSpec as P

D = 512
HF = 4
HC = 8
CELLS = 72
TALL = 80
WINDOWS = 4
ROWS = 12
COLS = 24
EPSILON = 1e-05
NEGATIVE = -1000000000.0
LOWEST = -3.0e38
INTERPRET = False
VMEM_SPEC = pl.BlockSpec(memory_space=pltpu.VMEM)
SMEM_SPEC = pl.BlockSpec(memory_space=pltpu.SMEM)
VMEM_LIMIT = 12 * 1024 * 1024
FLOPS = 5_000_000_000
BYTES = 4_000_000


F32 = jnp.float32
BF16 = jnp.bfloat16


def window_order():
    return [
        (6 * a + r, 12 * b + c) for a in range(2) for b in range(2) for r in range(6) for c in range(12)
    ]


def patch_order():
    return [
        (2 * r + dr, 2 * c + dc) for dc in range(2) for dr in range(2) for r in range(6) for c in range(12)
    ]


def plain_order(rows, cols):
    return [(r, c) for r in range(rows) for c in range(cols)]


def leading(rows, cols):
    half_r, half_c = (3, 6)
    side = [(r, c) for r in range(half_r, rows) for c in range(half_c)]
    edge = [(r, c) for r in range(half_r) for c in range(half_c, cols)]
    corner = [(r, c) for r in range(half_r) for c in range(half_c)]
    return (side, edge, corner)


def trailing(rows, cols):
    half_r, half_c = (3, 6)
    side = [(r, c) for r in range(rows - half_r) for c in range(cols - half_c, cols)]
    edge = [(r, c) for r in range(rows - half_r, rows) for c in range(cols - half_c)]
    corner = [(r, c) for r in range(rows - half_r, rows) for c in range(cols - half_c, cols)]
    return (side, edge, corner)


SLOTS = (80, 80, 48)
NARROW = (64, 64, 32)
COARSE_AT = (56, 56, 24)


def pick(order, cells, places, total):
    where = {cell: i for i, cell in enumerate(order)}
    matrix = np.zeros((total, len(order)), np.float32)
    for place, cell in zip(places, cells):
        matrix[place, where[cell]] = 1.0
    return matrix


def send_matrix(order, pieces, starts, slots=SLOTS):
    cells, places, at = [], [], 0
    for piece, start, slot in zip(pieces, starts, slots):
        cells += piece
        places += [at + start + i for i in range(len(piece))]
        at += slot
    return pick(order, cells, places, at)


def take_matrices(own_order, out_cells, pieces, starts, shift, rows, cols, slots=SLOTS):
    own = {cell: i for i, cell in enumerate(own_order)}
    stack, at = {}, 0
    for piece, start, slot in zip(pieces, starts, slots):
        for i, cell in enumerate(piece):
            stack[cell] = at + start + i
        at += slot
    main = np.zeros((len(out_cells), len(own_order)), np.float32)
    halo = np.zeros((len(out_cells), at), np.float32)
    for i, cell in enumerate(out_cells):
        if cell is None:
            continue
        r, c = (cell[0] + shift[0], cell[1] + shift[1])
        if 0 <= r < rows and 0 <= c < cols:
            main[i, own[r, c]] = 1.0
        else:
            halo[i, stack[r % rows, c % cols]] = 1.0
    return main, halo


def padded_rows(rows, cols, height):
    return [(r, c) if c < cols else None for r in range(rows) for c in range(height)]


ZERO3 = (0, 0, 0)
PLAIN_F = plain_order(ROWS, COLS)
PLAIN_C = plain_order(6, 12)
TABLES = dict(
    tok_send=send_matrix(PLAIN_F, leading(ROWS, COLS), ZERO3),
    cot_send=send_matrix(PLAIN_C, leading(6, 12), COARSE_AT),
)
TABLES["tok_main"], TABLES["tok_halo"] = take_matrices(
    PLAIN_F, window_order(), leading(ROWS, COLS), ZERO3, (3, 6), ROWS, COLS
)
TABLES["cot_main"], TABLES["cot_halo"] = take_matrices(
    PLAIN_C, PLAIN_C, leading(6, 12), COARSE_AT, (3, 6), 6, 12
)
TABLES["y_send"] = send_matrix(window_order(), leading(ROWS, COLS), ZERO3, NARROW)
TABLES["y_main"], TABLES["y_halo"] = take_matrices(
    window_order(), patch_order(), leading(ROWS, COLS), ZERO3, (3, 6), ROWS, COLS, NARROW
)
TABLES["df_send"] = send_matrix(patch_order(), trailing(ROWS, COLS), ZERO3)
TABLES["df_main"], TABLES["df_halo"] = take_matrices(
    patch_order(), window_order(), trailing(ROWS, COLS), ZERO3, (-3, -6), ROWS, COLS
)
TABLES["out_send"] = send_matrix(PLAIN_C, trailing(6, 12), COARSE_AT)
TABLES["out_main"], TABLES["out_halo"] = take_matrices(
    PLAIN_C, padded_rows(6, 12, 16), trailing(6, 12), COARSE_AT, (-3, -6), 6, 12
)
TABLES["dx_send"] = send_matrix(window_order(), trailing(ROWS, COLS), ZERO3, NARROW)
TABLES["dx_main"], TABLES["dx_halo"] = take_matrices(
    window_order(), PLAIN_F, trailing(ROWS, COLS), ZERO3, (-3, -6), ROWS, COLS, NARROW
)


def table(name):
    return jnp.asarray(TABLES[name], BF16)


def mm(a, b):
    return lax.dot_general(a, b, (((1,), (0,)), ((), ())), preferred_element_type=F32)


def mm_nt(a, b):
    return lax.dot_general(a, b, (((1,), (1,)), ((), ())), preferred_element_type=F32)


def mm_tn(a, b):
    return lax.dot_general(a, b, (((0,), (0,)), ((), ())), preferred_element_type=F32)


def rounded(x):
    return x.astype(BF16).astype(F32)


def call(kernel, outs, *args, scratch=(), specs=None, limit=None):
    return pl.pallas_call(
        kernel,
        out_shape=[jax.ShapeDtypeStruct(s, d) for s, d in outs],
        in_specs=specs or [VMEM_SPEC] * len(args),
        out_specs=[VMEM_SPEC] * len(outs),
        scratch_shapes=list(scratch),
        compiler_params=pltpu.CompilerParams(vmem_limit_bytes=limit or VMEM_LIMIT),
        cost_estimate=pl.CostEstimate(flops=FLOPS, bytes_accessed=BYTES, transcendentals=0),
        interpret=INTERPRET,
    )(*args)


def scalar_call(kernel, outs, scalar, *args, scratch=()):
    return call(kernel, outs, scalar, *args, scratch=scratch, specs=[SMEM_SPEC] + [VMEM_SPEC] * len(args))


def cut(stack, *refs):
    at = 0
    for ref in refs:
        ref[...] = stack[at : at + ref.shape[0]]
        at += ref.shape[0]


def normalize(x):
    shifted = x - jnp.mean(x, axis=-1, keepdims=True)
    inverse = lax.rsqrt(jnp.mean(shifted * shifted, axis=-1, keepdims=True) + EPSILON)
    return shifted * inverse, inverse


def normalize_back(d, xhat, inverse):
    return inverse * (
        d - jnp.mean(d, axis=-1, keepdims=True) - xhat * jnp.mean(d * xhat, axis=-1, keepdims=True)
    )


def lane_half():
    lane = lax.broadcasted_iota(jnp.int32, (1, 128), 1)
    low = (lane < 64).astype(F32)
    return low, 1.0 - low


def stacked(x):
    low, high = lane_half()
    pad = jnp.zeros((128 - CELLS, 128), F32)
    return jnp.concatenate([x * low, pad, x * high, pad], axis=0).astype(BF16)


def unstacked(x):
    low, high = lane_half()
    return x[:CELLS] * low + x[128 : 128 + CELLS] * high


def key_lanes():
    lane = lax.broadcasted_iota(jnp.int32, (CELLS, 256), 1)
    return jnp.where(lane >= 128, lane - 128, lane)


def apart(split):
    row = lax.broadcasted_iota(jnp.int32, (CELLS, 256), 0)
    key = key_lanes()
    differ = (row >= CELLS // 2) != (key >= CELLS // 2)
    return jnp.logical_and(differ, split)


def halves(fn, x):
    return jnp.concatenate(
        [jnp.broadcast_to(fn(x[:, :128]), (CELLS, 128)), jnp.broadcast_to(fn(x[:, 128:]), (CELLS, 128))],
        axis=1,
    )


def attend(q, k2, v2, differ):
    scores = mm_nt(q.astype(BF16), k2) * 0.125
    scores = jnp.where(differ, NEGATIVE, scores)
    scores = jnp.where(key_lanes() < CELLS, scores, LOWEST)
    exponent = jnp.exp(scores - halves(lambda s: jnp.max(s, axis=1, keepdims=True), scores))
    weights = exponent / halves(lambda s: jnp.sum(s, axis=1, keepdims=True), exponent)
    return weights, mm(weights.astype(BF16), v2)


def attend_back(q, k2, v2, weights, differ, d):
    d = d.astype(BF16)
    dv = unstacked(mm_tn(weights.astype(BF16), d))
    dw = rounded(mm_nt(d, v2))
    ds = weights * (dw - halves(lambda s: jnp.sum(s, axis=1, keepdims=True), dw * weights))
    ds = jnp.where(differ, 0.0, ds * 0.125).astype(BF16)
    dq = mm(ds, k2)
    dk = unstacked(mm_tn(ds, q.astype(BF16)))
    return dq, dk, dv


def first_kernel(
    tok_in, cot_in, tok_send_in, cot_send_in, tok2d, side, edge, corner, cot2d,
    tok, cot, tok_send, cot_send, arrived,
):
    loads = [
        pltpu.make_async_copy(source, target, arrived.at[i])
        for i, (source, target) in enumerate(
            ((tok_in, tok), (cot_in, cot), (tok_send_in, tok_send), (cot_send_in, cot_send))
        )
    ]
    for load in loads:
        load.start()
    for load in loads:
        load.wait()
    x = tok[...].astype(F32).reshape(ROWS * COLS, D).astype(BF16)
    tok2d[...] = x
    for r in range(6):
        cot2d[pl.ds(12 * r, 12), :] = cot[r].astype(F32)
    y = cot2d[...].astype(BF16)
    stack = (mm(tok_send[...], x) + mm(cot_send[...], y)).astype(BF16)
    cut(stack, side, edge, corner)


def fine_forward_kernel(
    place, x_in, side, edge, corner, gain, wqkv, wproj, t_main, t_halo, y_send,
    x_out, n_out, p_out, w_out, m_out, y_out, side_out, edge_out, corner_out, mixed,
):
    halo = jnp.concatenate([side[...], edge[...], corner[...]], axis=0)
    x = mm(t_main[...], x_in[...]) + mm(t_halo[...], halo)
    x_out[...] = x.astype(BF16)
    xhat, _ = normalize(x)
    n = (xhat * gain[...]).astype(BF16)
    n_out[...] = n
    p_out[...] = rounded(mm(n, wqkv[...]))
    for w in range(WINDOWS):
        differ = apart(decode(place)[3] == 1 if w >= 2 else False)
        for p in range(HF // 2):
            rows = pl.ds(CELLS * w, CELLS)
            q, k, v = (p_out[rows, pl.ds(256 * part + 128 * p, 128)] for part in range(3))
            weights, out = attend(q, stacked(k), stacked(v), differ)
            w_out[2 * w + p] = weights
            mixed[rows, pl.ds(128 * p, 128)] = out
    m = mixed[...].astype(BF16)
    m_out[...] = m
    y = (x + mm(m, wproj[...])).astype(BF16)
    y_out[...] = y
    stack = mm(y_send[...], y).astype(BF16)
    cut(stack, side_out, edge_out, corner_out)


def coarse_kernel(
    place, y_in, side, edge, corner, cot_in, cside, cedge, ccorner,
    mgain, mweight, gain, wqkv, wproj, y_main, y_halo, c_main, c_halo, df_send, out_send,
    y2_out, df_out, side_out, edge_out, corner_out, fac_out, packed, mixed, dpacked, wsave,
):
    halo = jnp.concatenate([side[...], edge[...], corner[...]], axis=0)
    patches = mm(y_main[...], y_in[...]) + mm(y_halo[...], halo)
    g = jnp.concatenate([patches[CELLS * i : CELLS * (i + 1)] for i in range(4)], axis=1)
    ghat, ginv = normalize(g)
    mn = (ghat * mgain[...]).astype(BF16)
    z = rounded(mm(mn, mweight[...]))
    zhat, zinv = normalize(z)
    n = (zhat * gain[...]).astype(BF16)
    packed[...] = rounded(mm(n, wqkv[...]))
    differ = apart(decode(place)[3] == 1)
    for p in range(HC // 2):
        lanes = pl.ds(128 * p, 128)
        q, k, v = (packed[:, pl.ds(512 * part + 128 * p, 128)] for part in range(3))
        weights, out = attend(q, stacked(k), stacked(v), differ)
        wsave[p] = weights
        mixed[:, lanes] = out
    m = mixed[...].astype(BF16)
    y2 = (z + mm(m, wproj[...])).astype(BF16)
    y2_out[...] = y2

    chalo = jnp.concatenate([cside[...], cedge[...], ccorner[...]], axis=0)
    dy = mm(c_main[...], cot_in[...].astype(BF16)) + mm(c_halo[...], chalo)
    mixed[...] = rounded(mm_nt(dy.astype(BF16), wproj[...]))
    for p in range(HC // 2):
        q, k, v = (packed[:, pl.ds(512 * part + 128 * p, 128)] for part in range(3))
        grads = attend_back(q, stacked(k), stacked(v), wsave[p], differ, mixed[:, pl.ds(128 * p, 128)])
        for part in range(3):
            dpacked[:, pl.ds(512 * part + 128 * p, 128)] = grads[part]
    dp = dpacked[...].astype(BF16)
    dn = rounded(mm_nt(dp, wqkv[...]))
    dz = (dy + normalize_back(dn * gain[...], zhat, zinv)).astype(BF16)
    dmn = rounded(mm_nt(dz, mweight[...]))
    dg = normalize_back(dmn * mgain[...], ghat, ginv)
    df = jnp.concatenate([dg[:, D * i : D * (i + 1)] for i in range(4)], axis=0).astype(BF16)
    df_out[...] = df
    stack = (mm(df_send[...], df) + mm(out_send[...], y2)).astype(BF16)
    cut(stack, side_out, edge_out, corner_out)
    at = 0
    for piece in (mn, n, m, dz, dp, dy.astype(BF16)):
        fac_out[pl.ds(0, CELLS), pl.ds(at, piece.shape[1])] = piece
        at += piece.shape[1]
    fac_out[pl.ds(CELLS, TALL - CELLS), :] = jnp.zeros((TALL - CELLS, at), BF16)


def fine_backward_kernel(
    place, df_in, side, edge, corner, x_in, p_in, w_in, gain, wqkv, wproj, d_main, d_halo, dx_send,
    dx_out, side_out, edge_out, corner_out, fac_out, dmixed, dpacked,
):
    halo = jnp.concatenate([side[...], edge[...], corner[...]], axis=0)
    dy = mm(d_main[...], df_in[...]) + mm(d_halo[...], halo)
    dmixed[...] = rounded(mm_nt(dy.astype(BF16), wproj[...]))
    for w in range(WINDOWS):
        differ = apart(decode(place)[3] == 1 if w >= 2 else False)
        for p in range(HF // 2):
            rows = pl.ds(CELLS * w, CELLS)
            q, k, v = (p_in[rows, pl.ds(256 * part + 128 * p, 128)] for part in range(3))
            d = dmixed[rows, pl.ds(128 * p, 128)]
            grads = attend_back(q, stacked(k), stacked(v), w_in[2 * w + p], differ, d)
            for part in range(3):
                dpacked[rows, pl.ds(256 * part + 128 * p, 128)] = grads[part]
    dp = dpacked[...].astype(BF16)
    dn = rounded(mm_nt(dp, wqkv[...]))
    xhat, inverse = normalize(x_in[...].astype(F32))
    dx = (dy + normalize_back(dn * gain[...], xhat, inverse)).astype(BF16)
    dx_out[...] = dx
    stack = mm(dx_send[...], dx).astype(BF16)
    cut(stack, side_out, edge_out, corner_out)
    fac_out[:, pl.ds(0, 768)] = dp
    fac_out[:, pl.ds(768, D)] = dy.astype(BF16)


def decode(place):
    code = place[0]
    bits = tuple(lax.bitwise_and(lax.shift_right_logical(code, i), 1) for i in range(4))
    return bits + (lax.shift_right_logical(code, 4),)


def one_hot(want, width):
    lane = lax.broadcasted_iota(jnp.int32, (want.shape[0], width), 1)
    return jnp.where(lane == want, 1.0, 0.0).astype(BF16)


def row_index(count):
    return lax.broadcasted_iota(jnp.int32, (count, 1), 0)


def field(x, low, bits):
    return lax.bitwise_and(lax.shift_right_logical(x, low), (1 << bits) - 1)


def coarse_weights_kernel(
    place, own, other, m0k, m0s, m1k, m1s, c0k, c0s, c1k, c1s, lines
):
    core, zp, yp, _, _ = decode(place)

    def at(start, size):
        return jnp.concatenate([own[:, pl.ds(start, size)], other[:, pl.ds(start, size)]], axis=0)

    dz = at(2048 + 1024, D)
    row = row_index(256)
    group = field(row, 4, 3) * 2 + lax.bitwise_xor(field(row, 7, 1), yp)
    select = one_hot((2 * group + core) * 16 + field(row, 0, 4), D)
    for zh in range(2):
        pair = [at(D * (2 * zh + k), D) for k in range(2)]
        plain = jnp.full(pair[0].shape, zp, jnp.int32) == 0
        ordered = (
            jnp.where(plain, pair[0].astype(F32), pair[1].astype(F32)).astype(BF16),
            jnp.where(plain, pair[1].astype(F32), pair[0].astype(F32)).astype(BF16),
        )
        for zd in range(2):
            left = mm_nt(select, ordered[zd]).astype(BF16)
            part = mm(left, dz).reshape(16, 16, D)
            for yd in range(2):
                for h in range(4):
                    piece = part[8 * yd : 8 * yd + 8, :, 128 * h : 128 * h + 128]
                    (m0s if zd else m0k)[pl.ds(16 * yd + 8 * zh, 8), pl.ds(8 * h, 8), :] = piece[:, :8].astype(BF16)
                    (m1s if yd else m1k)[pl.ds(16 * zd + 8 * zh, 8), pl.ds(8 * h, 8), :] = piece[:, 8:].astype(BF16)
    row = row_index(256)
    z = field(row, 3, 1) * 2 + lax.bitwise_xor(field(row, 5, 1), zp)
    group = z * 16 + field(row, 0, 3) * 2 + lax.bitwise_xor(field(row, 4, 1), yp)
    select = one_hot((2 * group + core) * 4 + field(row, 6, 2), D)
    n = mm_nt(select, at(2048, D)).astype(BF16)
    m = mm_nt(select, at(2048 + D, D)).astype(BF16)
    for j in range(4):
        part = mm(n if j < 3 else m, at(2048 + 1536 + D * j, D))
        for i in range(4):
            line = part[64 * i : 64 * (i + 1)]
            for h in range(4):
                lines[pl.ds(512 * (4 * (j // 2) + h) + 4 * (j % 2) + i, 64, 8), :] = line[:, 128 * h : 128 * h + 128]
    for h in range(4):
        first = lines[pl.ds(512 * h, 512), :].reshape(64, 8, 128).astype(BF16)
        c0s[:, pl.ds(8 * h, 8), :] = first[:32]
        c0k[:, pl.ds(8 * h, 8), :] = first[32:]
        second = lines[pl.ds(512 * (4 + h), 512), :].reshape(64, 8, 128).astype(BF16)
        for zd in range(2):
            c1s[pl.ds(16 * zd, 16), pl.ds(8 * h, 8), :] = second[32 * zd : 32 * zd + 16]
            c1k[pl.ds(16 * zd, 16), pl.ds(8 * h, 8), :] = second[32 * zd + 16 : 32 * zd + 32]


def middle_kernel(m0k, m0c, m1k, m1c, c0k, c0c, c1k, c1c, m0, m0s, m1, m1s, c0, c0s, c1, c1s):
    for keep, came, first, second in (
        (m0k, m0c, m0, m0s), (m1k, m1c, m1s, m1), (c0k, c0c, c0s, c0), (c1k, c1c, c1, c1s)
    ):
        total = (keep[...].astype(F32) + came[...].astype(F32)).astype(BF16)
        first[...] = total[:16]
        second[...] = total[16:]


def fine_weights_kernel(place, n_own, n_other, m_own, m_other, own, other, out, lines):
    core = decode(place)[0]
    row = row_index(256)
    select = one_hot((2 * field(row, 0, 6) + core) * 4 + field(row, 6, 2), D)
    dp = lambda ref: ref[:, pl.ds(0, 768)]
    dy = lambda ref: ref[:, pl.ds(768, D)]
    n = [mm_nt(select, ref[...]).astype(BF16) for ref in (n_own, n_other)]
    part = mm(n[0], dp(own)) + mm(n[1], dp(other))
    for i in range(4):
        line = part[64 * i : 64 * (i + 1)]
        for h in range(4):
            lines[pl.ds(512 * h + i, 64, 8), :] = line[:, 128 * h : 128 * h + 128]
        for h in range(2):
            lines[pl.ds(512 * (2 * (i // 2) + h) + 4 + i % 2, 64, 8), :] = line[:, 512 + 128 * h : 640 + 128 * h]
    row = row_index(128)
    select = one_hot((2 * field(row, 0, 6) + core) * 2 + field(row, 6, 1), 256)
    m = [mm_nt(select, ref[...]).astype(BF16) for ref in (m_own, m_other)]
    part = mm(m[0], dy(own)) + mm(m[1], dy(other))
    for i in range(2):
        line = part[64 * i : 64 * (i + 1)]
        for h in range(4):
            lines[pl.ds(512 * h + 6 + i, 64, 8), :] = line[:, 128 * h : 128 * h + 128]
    for h in range(4):
        out[:, pl.ds(8 * h, 8), :] = lines[pl.ds(512 * h, 512), :].reshape(64, 8, 128).astype(BF16)


def join_kernel(place, m0, m0c, m1, m1c, c0, c0c, c1, c1c, fine, out):
    _, zp, yp, _, _ = decode(place)
    for keep, came, zd, yd in ((m0, m0c, 0, 0), (m1, m1c, 1, 0), (c0, c0c, 1, 1), (c1, c1c, 0, 1)):
        total = (keep[...].astype(F32) + came[...].astype(F32)).astype(BF16)
        for zh in range(2):
            out[zh, lax.bitwise_xor(zp, zd), :, lax.bitwise_xor(yp, yd), pl.ds(0, 32), :] = total[8 * zh : 8 * zh + 8]
    out[:, :, :, :, pl.ds(32, 32), :] = fine[...].reshape(2, 2, 8, 2, 32, 128)


def gain_rows(weight, gain, device, share):
    count = max(8, share)
    pick_rows = one_hot(device * share + row_index(count), gain.shape[1])
    over = jnp.sum(pick_rows.astype(F32) * gain, axis=1, keepdims=True)
    return mm(pick_rows, weight)[:share] / over[:share]


def assemble_kernel(
    place, y2, side, edge, corner, dx, dside, dedge, dcorner, out_main, out_halo, dx_main, dx_halo,
    fgain, fqkv, mgain, mweight, cgain, cqkv, out, grad, fcoef, mcoef, ccoef,
):
    device = decode(place)[4]
    fcoef[...] = gain_rows(fqkv[...], fgain[...], device, 4)
    mcoef[...] = gain_rows(mweight[...], mgain[...], device, 16)
    ccoef[...] = gain_rows(cqkv[...], cgain[...], device, 4)
    halo = jnp.concatenate([side[...], edge[...], corner[...]], axis=0)
    y = mm(out_main[...], y2[...]) + mm(out_halo[...], halo)
    for r in range(6):
        out[r] = y[16 * r : 16 * r + 12].astype(BF16)
    halo = jnp.concatenate([dside[...], dedge[...], dcorner[...]], axis=0)
    d = mm(dx_main[...], dx[...]) + mm(dx_halo[...], halo)
    grad[...] = d.reshape(ROWS, COLS, D).astype(BF16)


def as_row(column):
    size = column.shape[0]
    row = lax.broadcasted_iota(jnp.int32, (size, size), 0)
    lane = lax.broadcasted_iota(jnp.int32, (size, size), 1)
    return jnp.sum(jnp.where(row == lane, column, 0.0), axis=0, keepdims=True)


def sum_kernel(place, parts, fcoef, mcoef, ccoef, fgain, fqkv, fproj, mgain, merge, cgain, cqkv, cproj):
    _, zp, yp, _, _ = decode(place)
    factor = (ROWS * COLS * 128 // 4) ** (-0.5)
    sums = []
    for z in range(2):
        for y in range(2):
            total = None
            for zh in range(2):
                for k in range(8):
                    term = parts[zh, z, k, y].astype(F32)
                    total = term if total is None else total + term
            sums.append(total * factor)
    fine = (sums[0] + sums[1] + sums[2] + sums[3])[32:]
    tops = [v[:32] for v in sums]
    z_same = jnp.full((32, 128), zp, jnp.int32) == 0
    y_same = jnp.full((32, 128), yp, jnp.int32) == 0

    def related(zd, yd):
        low = [jnp.where(z_same, tops[2 * zd + y], tops[2 * (1 - zd) + y]) for y in range(2)]
        return jnp.where(y_same, low[yd], low[1 - yd])

    m0, m1, c0, c1 = (related(0, 0), related(1, 0), related(1, 1), related(0, 1))
    for h in range(4):
        lanes = pl.ds(128 * h, 128)
        rows = slice(8 * h, 8 * h + 8)
        merge[pl.ds(0, 8), lanes] = m0[rows]
        merge[pl.ds(8, 8), lanes] = m1[rows]
        cqkv[:, lanes] = c0[8 * h : 8 * h + 4]
        cqkv[:, pl.ds(D + 128 * h, 128)] = c0[8 * h + 4 : 8 * h + 8]
        cqkv[:, pl.ds(2 * D + 128 * h, 128)] = c1[8 * h : 8 * h + 4]
        cproj[:, lanes] = c1[8 * h + 4 : 8 * h + 8]
        fqkv[:, lanes] = fine[8 * h : 8 * h + 4]
        fqkv[pl.ds(2 * (h // 2), 2), pl.ds(D + 128 * (h % 2), 128)] = fine[8 * h + 4 : 8 * h + 6]
        fproj[:, lanes] = fine[8 * h + 6 : 8 * h + 8]
    for ref, coef, grad in ((fgain, fcoef, fqkv), (mgain, mcoef, merge), (cgain, ccoef, cqkv)):
        ref[...] = as_row(jnp.sum(coef[...] * grad[...], axis=1, keepdims=True))


def exchange(pieces, step):
    lat = lax.axis_size("lat")
    pair = lax.axis_size("pair")
    lon = 2 * pair
    arrived = []
    for piece, (dr, dc) in zip(pieces, ((0, 1), (1, 0), (1, 1))):
        pairs = []
        for r in range(lat):
            for c in range(lon):
                to = ((r + step * dr) % lat) * lon + (c + step * dc) % lon
                pairs.append((r * lon + c, to))
        arrived.append(lax.ppermute(piece, ("lat", "pair", "core"), pairs))
    return arrived


def partner(value):
    return lax.ppermute(value, "core", [(0, 1), (1, 0)])


def fold(value, axis, second):
    lat, pair = (lax.axis_size("lat"), lax.axis_size("pair"))
    pairs = []
    for r in range(lat):
        for p in range(pair):
            z, y = (r // 2, (r % 2) * 2 + p % 2)
            at = z if axis == "z" else y
            at = (at + (1 if at % 2 == (1 if second else 0) else -1)) % 4
            z, y = (at, y) if axis == "z" else (z, at)
            pairs.append((r * pair + p, (2 * z + y // 2) * pair + (p // 2) * 2 + y % 2))
    return lax.ppermute(value, ("lat", "pair"), pairs)


def deal(value):
    return lax.all_to_all(value, ("lat", "pair"), 0, 0)


def local(
    tokens, fine_gain, fine_qkv, fine_proj, merge_gain, merge_weight, coarse_gain, coarse_qkv, coarse_proj, cotangent
):
    lat_count = lax.axis_size("lat")
    lat, core = (lax.axis_index("lat"), lax.axis_index("core"))
    device = (lat * lax.axis_size("pair") + lax.axis_index("pair")) * 2 + core
    parity = lax.bitwise_and(lax.shift_right_logical(lat, 1), 1)
    seam = (lat == lat_count - 1).astype(jnp.int32)
    flip = lax.bitwise_and(lax.axis_index("pair"), 1)
    place = (device * 16 + seam * 8 + flip * 4 + parity * 2 + core).astype(jnp.int32).reshape(1)
    fgain, mgain, cgain = (v.reshape(1, -1) for v in (fine_gain, merge_gain, coarse_gain))
    cells = WINDOWS * CELLS

    pieces = [((size, D), BF16) for size in SLOTS]
    narrow = [((size, D), BF16) for size in NARROW]
    tok, *sent, cot = call(
        first_kernel,
        [((cells, D), BF16)] + pieces + [((CELLS, D), F32)],
        *(
            pltpu.with_memory_space_constraint(v, pltpu.HBM)
            for v in (tokens, cotangent, table("tok_send"), table("cot_send"))
        ),
        specs=[pl.BlockSpec(memory_space=pltpu.HBM)] * 4,
        scratch=[
            pltpu.VMEM((ROWS, COLS, D), BF16), pltpu.VMEM((6, 12, D), BF16), pltpu.VMEM((sum(SLOTS), cells), BF16),
            pltpu.VMEM((sum(SLOTS), CELLS), BF16), pltpu.SemaphoreType.DMA((4,)),
        ],
    )
    ahead = exchange(sent, -1)
    x, n, p, w, m, y, *sent = scalar_call(
        fine_forward_kernel,
        [
            ((cells, D), BF16), ((cells, D), BF16), ((cells, 768), F32), ((8, CELLS, 256), F32),
            ((cells, 256), BF16), ((cells, D), BF16),
        ]
        + narrow,
        place, tok, *ahead, fgain, fine_qkv, fine_proj, table("tok_main"), table("tok_halo"), table("y_send"),
        scratch=[pltpu.VMEM((cells, 256), F32)],
    )
    merged = exchange(sent, -1)
    n_other, m_other = (partner(n), partner(m))
    y2, df, *sent, fac = scalar_call(
        coarse_kernel,
        [((CELLS, D), BF16), ((cells, D), BF16)] + pieces + [((TALL, 5632), BF16)],
        place, y, *merged, cot, *ahead, mgain, merge_weight, cgain, coarse_qkv, coarse_proj,
        table("y_main"), table("y_halo"), table("cot_main"), table("cot_halo"), table("df_send"), table("out_send"),
        scratch=[
            pltpu.VMEM((CELLS, 1536), F32), pltpu.VMEM((CELLS, D), F32), pltpu.VMEM((CELLS, 1536), F32),
            pltpu.VMEM((4, CELLS, 256), F32),
        ],
    )
    back = exchange(sent, 1)
    m0k, m0s, m1k, m1s, c0k, c0s, c1k, c1s = scalar_call(
        coarse_weights_kernel,
        [((32, 32, 128), BF16)] * 8,
        place, fac, partner(fac),
        scratch=[pltpu.VMEM((4096, 128), F32)],
    )
    first = [
        fold(v, axis, second)
        for v, axis, second in ((m0s, "z", False), (m1s, "y", False), (c0s, "z", True), (c1s, "y", True))
    ]
    dx, *sent, fac = scalar_call(
        fine_backward_kernel,
        [((cells, D), BF16)] + narrow + [((cells, 1280), BF16)],
        place, df, *back, x, p, w, fgain, fine_qkv, fine_proj, table("df_main"), table("df_halo"), table("dx_send"),
        scratch=[pltpu.VMEM((cells, 256), F32), pltpu.VMEM((cells, 768), F32)],
    )
    ended = exchange(sent, 1)
    m0, m0s, m1, m1s, c0, c0s, c1, c1s = call(
        middle_kernel,
        [((16, 32, 128), BF16)] * 8,
        m0k, first[0], m1k, first[1], c0k, first[2], c1k, first[3],
    )
    again = [
        fold(v, axis, second)
        for v, axis, second in ((m0s, "y", False), (m1s, "z", False), (c0s, "y", True), (c1s, "z", True))
    ]
    (fine_part,) = scalar_call(
        fine_weights_kernel,
        [((64, 32, 128), BF16)],
        place, n, n_other, m, m_other, fac, partner(fac),
        scratch=[pltpu.VMEM((2048, 128), F32)],
    )
    (joined,) = scalar_call(
        join_kernel,
        [((2, 2, 8, 2, 64, 128), BF16)],
        place, m0, again[0], m1, again[1], c0, again[2], c1, again[3], fine_part,
    )
    parts = deal(joined.reshape(64, 64, 128)).reshape(2, 2, 8, 2, 64, 128)
    output, grad, fcoef, mcoef, ccoef = scalar_call(
        assemble_kernel,
        [((6, 12, D), BF16), ((ROWS, COLS, D), BF16), ((4, 768), F32), ((16, D), F32), ((4, 1536), F32)],
        place, y2, *back, dx, *ended, table("out_main"), table("out_halo"), table("dx_main"), table("dx_halo"),
        fgain, fine_qkv, mgain, merge_weight, cgain, coarse_qkv,
    )
    fg, fqkv, fproj, mg, merge, cg, cqkv, cproj = scalar_call(
        sum_kernel,
        [
            ((1, 4), F32), ((4, 768), F32), ((2, D), F32), ((1, 16), F32), ((16, D), F32), ((1, 4), F32),
            ((4, 1536), F32), ((4, D), F32),
        ],
        place, parts, fcoef, mcoef, ccoef,
    )
    fg, mg, cg = (v.reshape(-1) for v in (fg, mg, cg))
    return (output, grad, fg, fqkv, fproj, mg, merge, cg, cqkv, cproj)


def solution(mesh):
    lat, lon = (mesh.shape["lat"], mesh.shape["lon"])
    split = Mesh(mesh.devices.reshape(lat, lon // 2, 2), ("lat", "pair", "core"))
    lon = ("pair", "core")
    grid = P("lat", lon, None)
    whole = ("lat", "pair", "core")
    return jax.shard_map(
        local,
        mesh=split,
        in_specs=(grid, P(), P(), P(), P(), P(), P(), P(), P(), grid),
        out_specs=(
            grid, grid, P(whole), P(whole, None), P(whole, None), P(whole), P(whole, None), P(whole),
            P(whole, None), P(whole, None),
        ),
        check_vma=False,
    )
```

```python
import jax
import jax.numpy as jnp
import numpy as np
from jax import lax
from jax.experimental import pallas as pl
from jax.experimental.pallas import tpu as pltpu
from jax.sharding import Mesh, PartitionSpec as P

D = 512
HF = 4
HC = 8
CELLS = 72
TALL = 80
WINDOWS = 4
ROWS = 12
COLS = 24
EPSILON = 1e-05
NEGATIVE = -1000000000.0
LOWEST = -3.0e38
INTERPRET = False
VMEM_SPEC = pl.BlockSpec(memory_space=pltpu.VMEM)
SMEM_SPEC = pl.BlockSpec(memory_space=pltpu.SMEM)
VMEM_LIMIT = 12 * 1024 * 1024
FLOPS = 5_000_000_000
BYTES = 4_000_000


F32 = jnp.float32
BF16 = jnp.bfloat16


def window_order():
    return [
        (6 * a + r, 12 * b + c) for a in range(2) for b in range(2) for r in range(6) for c in range(12)
    ]


def patch_order():
    return [
        (2 * r + dr, 2 * c + dc) for dc in range(2) for dr in range(2) for r in range(6) for c in range(12)
    ]


def plain_order(rows, cols):
    return [(r, c) for r in range(rows) for c in range(cols)]


def leading(rows, cols):
    half_r, half_c = (3, 6)
    side = [(r, c) for r in range(half_r, rows) for c in range(half_c)]
    edge = [(r, c) for r in range(half_r) for c in range(half_c, cols)]
    corner = [(r, c) for r in range(half_r) for c in range(half_c)]
    return (side, edge, corner)


def trailing(rows, cols):
    half_r, half_c = (3, 6)
    side = [(r, c) for r in range(rows - half_r) for c in range(cols - half_c, cols)]
    edge = [(r, c) for r in range(rows - half_r, rows) for c in range(cols - half_c)]
    corner = [(r, c) for r in range(rows - half_r, rows) for c in range(cols - half_c, cols)]
    return (side, edge, corner)


SLOTS = (80, 80, 48)
NARROW = (64, 64, 32)
COARSE_AT = (56, 56, 24)


def pick(order, cells, places, total):
    where = {cell: i for i, cell in enumerate(order)}
    matrix = np.zeros((total, len(order)), np.float32)
    for place, cell in zip(places, cells):
        matrix[place, where[cell]] = 1.0
    return matrix


def send_matrix(order, pieces, starts, slots=SLOTS):
    cells, places, at = [], [], 0
    for piece, start, slot in zip(pieces, starts, slots):
        cells += piece
        places += [at + start + i for i in range(len(piece))]
        at += slot
    return pick(order, cells, places, at)


def take_matrices(own_order, out_cells, pieces, starts, shift, rows, cols, slots=SLOTS):
    own = {cell: i for i, cell in enumerate(own_order)}
    stack, at = {}, 0
    for piece, start, slot in zip(pieces, starts, slots):
        for i, cell in enumerate(piece):
            stack[cell] = at + start + i
        at += slot
    main = np.zeros((len(out_cells), len(own_order)), np.float32)
    halo = np.zeros((len(out_cells), at), np.float32)
    for i, cell in enumerate(out_cells):
        if cell is None:
            continue
        r, c = (cell[0] + shift[0], cell[1] + shift[1])
        if 0 <= r < rows and 0 <= c < cols:
            main[i, own[r, c]] = 1.0
        else:
            halo[i, stack[r % rows, c % cols]] = 1.0
    return main, halo


def padded_rows(rows, cols, height):
    return [(r, c) if c < cols else None for r in range(rows) for c in range(height)]


ZERO3 = (0, 0, 0)
PLAIN_F = plain_order(ROWS, COLS)
PLAIN_C = plain_order(6, 12)
TABLES = dict(
    tok_send=send_matrix(PLAIN_F, leading(ROWS, COLS), ZERO3),
    cot_send=send_matrix(PLAIN_C, leading(6, 12), COARSE_AT),
)
TABLES["tok_main"], TABLES["tok_halo"] = take_matrices(
    PLAIN_F, window_order(), leading(ROWS, COLS), ZERO3, (3, 6), ROWS, COLS
)
TABLES["cot_main"], TABLES["cot_halo"] = take_matrices(
    PLAIN_C, PLAIN_C, leading(6, 12), COARSE_AT, (3, 6), 6, 12
)
TABLES["y_send"] = send_matrix(window_order(), leading(ROWS, COLS), ZERO3, NARROW)
TABLES["y_main"], TABLES["y_halo"] = take_matrices(
    window_order(), patch_order(), leading(ROWS, COLS), ZERO3, (3, 6), ROWS, COLS, NARROW
)
TABLES["df_send"] = send_matrix(patch_order(), trailing(ROWS, COLS), ZERO3)
TABLES["df_main"], TABLES["df_halo"] = take_matrices(
    patch_order(), window_order(), trailing(ROWS, COLS), ZERO3, (-3, -6), ROWS, COLS
)
TABLES["out_send"] = send_matrix(PLAIN_C, trailing(6, 12), COARSE_AT)
TABLES["out_main"], TABLES["out_halo"] = take_matrices(
    PLAIN_C, padded_rows(6, 12, 16), trailing(6, 12), COARSE_AT, (-3, -6), 6, 12
)
TABLES["dx_send"] = send_matrix(window_order(), trailing(ROWS, COLS), ZERO3, NARROW)
TABLES["dx_main"], TABLES["dx_halo"] = take_matrices(
    window_order(), PLAIN_F, trailing(ROWS, COLS), ZERO3, (-3, -6), ROWS, COLS, NARROW
)


def table(name):
    return jnp.asarray(TABLES[name], BF16)


def mm(a, b):
    return lax.dot_general(a, b, (((1,), (0,)), ((), ())), preferred_element_type=F32)


def mm_nt(a, b):
    return lax.dot_general(a, b, (((1,), (1,)), ((), ())), preferred_element_type=F32)


def mm_tn(a, b):
    return lax.dot_general(a, b, (((0,), (0,)), ((), ())), preferred_element_type=F32)


def rounded(x):
    return x.astype(BF16).astype(F32)


def call(kernel, outs, *args, scratch=(), specs=None, limit=None):
    return pl.pallas_call(
        kernel,
        out_shape=[jax.ShapeDtypeStruct(s, d) for s, d in outs],
        in_specs=specs or [VMEM_SPEC] * len(args),
        out_specs=[VMEM_SPEC] * len(outs),
        scratch_shapes=list(scratch),
        compiler_params=pltpu.CompilerParams(vmem_limit_bytes=limit or VMEM_LIMIT),
        cost_estimate=pl.CostEstimate(flops=FLOPS, bytes_accessed=BYTES, transcendentals=0),
        interpret=INTERPRET,
    )(*args)


def scalar_call(kernel, outs, scalar, *args, scratch=()):
    return call(kernel, outs, scalar, *args, scratch=scratch, specs=[SMEM_SPEC] + [VMEM_SPEC] * len(args))


def cut(stack, *refs):
    at = 0
    for ref in refs:
        ref[...] = stack[at : at + ref.shape[0]]
        at += ref.shape[0]


def normalize(x):
    shifted = x - jnp.mean(x, axis=-1, keepdims=True)
    inverse = lax.rsqrt(jnp.mean(shifted * shifted, axis=-1, keepdims=True) + EPSILON)
    return shifted * inverse, inverse


def normalize_back(d, xhat, inverse):
    return inverse * (
        d - jnp.mean(d, axis=-1, keepdims=True) - xhat * jnp.mean(d * xhat, axis=-1, keepdims=True)
    )


def lane_half():
    lane = lax.broadcasted_iota(jnp.int32, (1, 128), 1)
    low = (lane < 64).astype(F32)
    return low, 1.0 - low


def stacked(x):
    low, high = lane_half()
    pad = jnp.zeros((128 - CELLS, 128), F32)
    return jnp.concatenate([x * low, pad, x * high, pad], axis=0).astype(BF16)


def unstacked(x):
    low, high = lane_half()
    return x[:CELLS] * low + x[128 : 128 + CELLS] * high


def key_lanes():
    lane = lax.broadcasted_iota(jnp.int32, (CELLS, 256), 1)
    return jnp.where(lane >= 128, lane - 128, lane)


def apart(split):
    row = lax.broadcasted_iota(jnp.int32, (CELLS, 256), 0)
    key = key_lanes()
    differ = (row >= CELLS // 2) != (key >= CELLS // 2)
    return jnp.logical_and(differ, split)


def halves(fn, x):
    return jnp.concatenate(
        [jnp.broadcast_to(fn(x[:, :128]), (CELLS, 128)), jnp.broadcast_to(fn(x[:, 128:]), (CELLS, 128))],
        axis=1,
    )


def attend(q, k2, v2, differ):
    scores = mm_nt(q.astype(BF16), k2) * 0.125
    scores = jnp.where(differ, NEGATIVE, scores)
    scores = jnp.where(key_lanes() < CELLS, scores, LOWEST)
    exponent = jnp.exp(scores - halves(lambda s: jnp.max(s, axis=1, keepdims=True), scores))
    weights = exponent / halves(lambda s: jnp.sum(s, axis=1, keepdims=True), exponent)
    return weights, mm(weights.astype(BF16), v2)


def attend_back(q, k2, v2, weights, differ, d):
    d = d.astype(BF16)
    dv = unstacked(mm_tn(weights.astype(BF16), d))
    dw = rounded(mm_nt(d, v2))
    ds = weights * (dw - halves(lambda s: jnp.sum(s, axis=1, keepdims=True), dw * weights))
    ds = jnp.where(differ, 0.0, ds * 0.125).astype(BF16)
    dq = mm(ds, k2)
    dk = unstacked(mm_tn(ds, q.astype(BF16)))
    return dq, dk, dv


def first_kernel(
    place, tok_in, cot_in, tok_send_in, cot_send_in, tok2d, side, edge, corner, cot2d,
    tok, cot, tok_send, cot_send, arrived,
):
    loads = [
        pltpu.make_async_copy(source, target, arrived.at[i])
        for i, (source, target) in enumerate(
            ((tok_in, tok), (cot_in, cot), (tok_send_in, tok_send), (cot_send_in, cot_send))
        )
    ]
    for load in loads:
        load.start()
    for load in loads:
        load.wait()
    x = tok[...].astype(F32).reshape(ROWS * COLS, D).astype(BF16)
    tok2d[...] = x
    for r in range(6):
        cot2d[pl.ds(12 * r, 12), :] = cot[r].astype(F32)
    y = cot2d[...].astype(BF16)
    stack = (mm(tok_send[...], x) + mm(cot_send[...], y)).astype(BF16)
    cut(stack, side, edge, corner)


def fine_forward_kernel(
    place, x_in, side, edge, corner, gain, wqkv, wproj, t_main, t_halo, y_send,
    x_out, nm_out, p_out, w_out, y_out, side_out, edge_out, corner_out, mixed,
):
    halo = jnp.concatenate([side[...], edge[...], corner[...]], axis=0)
    x = mm(t_main[...], x_in[...]) + mm(t_halo[...], halo)
    x_out[...] = x.astype(BF16)
    xhat, _ = normalize(x)
    n = (xhat * gain[...]).astype(BF16)
    nm_out[:, pl.ds(0, D)] = n
    p_out[...] = rounded(mm(n, wqkv[...]))
    for w in range(WINDOWS):
        differ = apart(decode(place)[3] == 1 if w >= 2 else False)
        for p in range(HF // 2):
            rows = pl.ds(CELLS * w, CELLS)
            q, k, v = (p_out[rows, pl.ds(256 * part + 128 * p, 128)] for part in range(3))
            weights, out = attend(q, stacked(k), stacked(v), differ)
            w_out[2 * w + p] = weights
            mixed[rows, pl.ds(128 * p, 128)] = out
    m = mixed[...].astype(BF16)
    nm_out[:, pl.ds(D, 256)] = m
    y = (x + mm(m, wproj[...])).astype(BF16)
    y_out[...] = y
    stack = mm(y_send[...], y).astype(BF16)
    cut(stack, side_out, edge_out, corner_out)


def coarse_kernel(
    place, y_in, side, edge, corner, cot_in, cside, cedge, ccorner,
    mgain, mweight, gain, wqkv, wproj, y_main, y_halo, c_main, c_halo, df_send, out_send,
    y2_out, df_out, side_out, edge_out, corner_out, fac_out, packed, mixed, dpacked, wsave,
):
    halo = jnp.concatenate([side[...], edge[...], corner[...]], axis=0)
    patches = mm(y_main[...], y_in[...]) + mm(y_halo[...], halo)
    g = jnp.concatenate([patches[CELLS * i : CELLS * (i + 1)] for i in range(4)], axis=1)
    ghat, ginv = normalize(g)
    mn = (ghat * mgain[...]).astype(BF16)
    z = rounded(mm(mn, mweight[...]))
    zhat, zinv = normalize(z)
    n = (zhat * gain[...]).astype(BF16)
    packed[...] = rounded(mm(n, wqkv[...]))
    differ = apart(decode(place)[3] == 1)
    for p in range(HC // 2):
        lanes = pl.ds(128 * p, 128)
        q, k, v = (packed[:, pl.ds(512 * part + 128 * p, 128)] for part in range(3))
        weights, out = attend(q, stacked(k), stacked(v), differ)
        wsave[p] = weights
        mixed[:, lanes] = out
    m = mixed[...].astype(BF16)
    y2 = (z + mm(m, wproj[...])).astype(BF16)
    y2_out[...] = y2

    chalo = jnp.concatenate([cside[...], cedge[...], ccorner[...]], axis=0)
    dy = mm(c_main[...], cot_in[...].astype(BF16)) + mm(c_halo[...], chalo)
    mixed[...] = rounded(mm_nt(dy.astype(BF16), wproj[...]))
    for p in range(HC // 2):
        q, k, v = (packed[:, pl.ds(512 * part + 128 * p, 128)] for part in range(3))
        grads = attend_back(q, stacked(k), stacked(v), wsave[p], differ, mixed[:, pl.ds(128 * p, 128)])
        for part in range(3):
            dpacked[:, pl.ds(512 * part + 128 * p, 128)] = grads[part]
    dp = dpacked[...].astype(BF16)
    dn = rounded(mm_nt(dp, wqkv[...]))
    dz = (dy + normalize_back(dn * gain[...], zhat, zinv)).astype(BF16)
    dmn = rounded(mm_nt(dz, mweight[...]))
    dg = normalize_back(dmn * mgain[...], ghat, ginv)
    df = jnp.concatenate([dg[:, D * i : D * (i + 1)] for i in range(4)], axis=0).astype(BF16)
    df_out[...] = df
    stack = (mm(df_send[...], df) + mm(out_send[...], y2)).astype(BF16)
    cut(stack, side_out, edge_out, corner_out)
    at = 0
    for piece in (mn, n, m, dz, dp, dy.astype(BF16)):
        fac_out[pl.ds(0, CELLS), pl.ds(at, piece.shape[1])] = piece
        at += piece.shape[1]
    fac_out[pl.ds(CELLS, TALL - CELLS), :] = jnp.zeros((TALL - CELLS, at), BF16)


def fine_backward_kernel(
    place, df_in, side, edge, corner, x_in, p_in, w_in, gain, wqkv, wproj, d_main, d_halo, dx_send,
    dx_out, side_out, edge_out, corner_out, fac_out, dmixed, dpacked,
):
    halo = jnp.concatenate([side[...], edge[...], corner[...]], axis=0)
    dy = mm(d_main[...], df_in[...]) + mm(d_halo[...], halo)
    dmixed[...] = rounded(mm_nt(dy.astype(BF16), wproj[...]))
    for w in range(WINDOWS):
        differ = apart(decode(place)[3] == 1 if w >= 2 else False)
        for p in range(HF // 2):
            rows = pl.ds(CELLS * w, CELLS)
            q, k, v = (p_in[rows, pl.ds(256 * part + 128 * p, 128)] for part in range(3))
            d = dmixed[rows, pl.ds(128 * p, 128)]
            grads = attend_back(q, stacked(k), stacked(v), w_in[2 * w + p], differ, d)
            for part in range(3):
                dpacked[rows, pl.ds(256 * part + 128 * p, 128)] = grads[part]
    dp = dpacked[...].astype(BF16)
    dn = rounded(mm_nt(dp, wqkv[...]))
    xhat, inverse = normalize(x_in[...].astype(F32))
    dx = (dy + normalize_back(dn * gain[...], xhat, inverse)).astype(BF16)
    dx_out[...] = dx
    stack = mm(dx_send[...], dx).astype(BF16)
    cut(stack, side_out, edge_out, corner_out)
    fac_out[:, pl.ds(0, 768)] = dp
    fac_out[:, pl.ds(768, D)] = dy.astype(BF16)


def decode(place):
    code = place[0]
    bits = tuple(lax.bitwise_and(lax.shift_right_logical(code, i), 1) for i in range(4))
    return bits + (lax.shift_right_logical(code, 4),)


def one_hot(want, width):
    lane = lax.broadcasted_iota(jnp.int32, (want.shape[0], width), 1)
    return jnp.where(lane == want, 1.0, 0.0).astype(BF16)


def row_index(count):
    return lax.broadcasted_iota(jnp.int32, (count, 1), 0)


def field(x, low, bits):
    return lax.bitwise_and(lax.shift_right_logical(x, low), (1 << bits) - 1)


def coarse_weights_kernel(place, own, other, mk, ms, ck, cs, lines):
    core, zp, yp, _, _ = decode(place)

    def at(start, size):
        return jnp.concatenate([own[:, pl.ds(start, size)], other[:, pl.ds(start, size)]], axis=0)

    dz = at(2048 + 1024, D)
    row = row_index(256)
    group = field(row, 4, 3) * 2 + lax.bitwise_xor(field(row, 7, 1), yp)
    select = one_hot((2 * group + core) * 16 + field(row, 0, 4), D)
    for zh in range(2):
        pair = [at(D * (2 * zh + k), D) for k in range(2)]
        plain = jnp.full(pair[0].shape, zp, jnp.int32) == 0
        ordered = (
            jnp.where(plain, pair[0].astype(F32), pair[1].astype(F32)).astype(BF16),
            jnp.where(plain, pair[1].astype(F32), pair[0].astype(F32)).astype(BF16),
        )
        for zd in range(2):
            left = mm_nt(select, ordered[zd]).astype(BF16)
            part = mm(left, dz).reshape(16, 16, D).astype(BF16)
            for yd in range(2):
                for h in range(4):
                    piece = part[8 * yd : 8 * yd + 8, :, 128 * h : 128 * h + 128]
                    (ms if zd else mk)[pl.ds(16 * yd + 8 * zh, 8), pl.ds(16 * h, 16), :] = piece
    row = row_index(256)
    z = field(row, 3, 1) * 2 + lax.bitwise_xor(field(row, 5, 1), zp)
    group = z * 16 + field(row, 0, 3) * 2 + lax.bitwise_xor(field(row, 4, 1), yp)
    select = one_hot((2 * group + core) * 4 + field(row, 6, 2), D)
    n = mm_nt(select, at(2048, D)).astype(BF16)
    m = mm_nt(select, at(2048 + D, D)).astype(BF16)
    for j in range(4):
        part = mm(n if j < 3 else m, at(2048 + 1536 + D * j, D))
        for i in range(4):
            line = part[64 * i : 64 * (i + 1)]
            for h in range(4):
                lines[pl.ds(1024 * h + 4 * j + i, 64, 16), :] = line[:, 128 * h : 128 * h + 128]
    for h in range(4):
        chunk = lines[pl.ds(1024 * h, 1024), :].reshape(64, 16, 128).astype(BF16)
        cs[:, pl.ds(16 * h, 16), :] = chunk[:32]
        ck[:, pl.ds(16 * h, 16), :] = chunk[32:]


def middle_kernel(mk, mc, ck, cc, m_keep, m_send, c_keep, c_send):
    for keep, came, stay, send, first in ((mk, mc, m_keep, m_send, 0), (ck, cc, c_keep, c_send, 1)):
        total = keep[...].astype(F32) + came[...].astype(F32)
        for part in range(2):
            same = total[16 * (part ^ first) : 16 * (part ^ first) + 16]
            other = total[16 * (1 - (part ^ first)) : 16 * (1 - (part ^ first)) + 16]
            for h in range(4):
                rows = slice(16 * h + 8 * part, 16 * h + 8 * part + 8)
                stay[pl.ds(16 * part, 16), pl.ds(8 * h, 8), :] = same[:, rows].astype(BF16)
                send[pl.ds(16 * part, 16), pl.ds(8 * h, 8), :] = other[:, rows].astype(BF16)


def fine_weights_kernel(place, nm_own, nm_other, own, other, out, lines):
    core = decode(place)[0]
    row = row_index(256)
    select = one_hot((2 * field(row, 0, 6) + core) * 4 + field(row, 6, 2), D)
    dp = lambda ref: ref[:, pl.ds(0, 768)]
    dy = lambda ref: ref[:, pl.ds(768, D)]
    n = [mm_nt(select, ref[:, pl.ds(0, D)]).astype(BF16) for ref in (nm_own, nm_other)]
    part = mm(n[0], dp(own)) + mm(n[1], dp(other))
    for i in range(4):
        line = part[64 * i : 64 * (i + 1)]
        for h in range(4):
            lines[pl.ds(512 * h + i, 64, 8), :] = line[:, 128 * h : 128 * h + 128]
        for h in range(2):
            lines[pl.ds(512 * (2 * (i // 2) + h) + 4 + i % 2, 64, 8), :] = line[:, 512 + 128 * h : 640 + 128 * h]
    row = row_index(128)
    select = one_hot((2 * field(row, 0, 6) + core) * 2 + field(row, 6, 1), 256)
    m = [mm_nt(select, ref[:, pl.ds(D, 256)]).astype(BF16) for ref in (nm_own, nm_other)]
    part = mm(m[0], dy(own)) + mm(m[1], dy(other))
    for i in range(2):
        line = part[64 * i : 64 * (i + 1)]
        for h in range(4):
            lines[pl.ds(512 * h + 6 + i, 64, 8), :] = line[:, 128 * h : 128 * h + 128]
    for h in range(4):
        out[:, pl.ds(8 * h, 8), :] = lines[pl.ds(512 * h, 512), :].reshape(64, 8, 128).astype(BF16)


def join_kernel(place, m, mc, c, cc, fine, out):
    _, zp, yp, _, _ = decode(place)
    for keep, came, zd in ((m, mc, 0), (c, cc, 1)):
        total = (keep[...].astype(F32) + came[...].astype(F32)).astype(BF16)
        for part in range(2):
            yd = part ^ zd
            for zh in range(2):
                at = 16 * part + 8 * zh
                out[zh, lax.bitwise_xor(zp, zd), :, lax.bitwise_xor(yp, yd), pl.ds(0, 32), :] = total[at : at + 8]
    out[:, :, :, :, pl.ds(32, 32), :] = fine[...].reshape(2, 2, 8, 2, 32, 128)


def gain_rows(weight, gain, device, share):
    count = max(8, share)
    pick_rows = one_hot(device * share + row_index(count), gain.shape[1])
    over = jnp.sum(pick_rows.astype(F32) * gain, axis=1, keepdims=True)
    return mm(pick_rows, weight)[:share] / over[:share]


def coefficients_kernel(place, fgain, fqkv, mgain, mweight, cgain, cqkv, fcoef, mcoef, ccoef):
    device = decode(place)[4]
    fcoef[...] = gain_rows(fqkv[...], fgain[...], device, 4)
    mcoef[...] = gain_rows(mweight[...], mgain[...], device, 16)
    ccoef[...] = gain_rows(cqkv[...], cgain[...], device, 4)


def output_kernel(y2, side, edge, corner, out_main, out_halo, out):
    halo = jnp.concatenate([side[...], edge[...], corner[...]], axis=0)
    y = mm(out_main[...], y2[...]) + mm(out_halo[...], halo)
    for r in range(6):
        out[r] = y[16 * r : 16 * r + 12].astype(BF16)


def tokens_kernel(dx, side, edge, corner, dx_main, dx_halo, grad):
    halo = jnp.concatenate([side[...], edge[...], corner[...]], axis=0)
    d = mm(dx_main[...], dx[...]) + mm(dx_halo[...], halo)
    grad[...] = d.reshape(ROWS, COLS, D).astype(BF16)


def as_row(column):
    size = column.shape[0]
    row = lax.broadcasted_iota(jnp.int32, (size, size), 0)
    lane = lax.broadcasted_iota(jnp.int32, (size, size), 1)
    return jnp.sum(jnp.where(row == lane, column, 0.0), axis=0, keepdims=True)


def sum_kernel(place, parts, fcoef, mcoef, ccoef, fgain, fqkv, fproj, mgain, merge, cgain, cqkv, cproj):
    _, zp, yp, _, _ = decode(place)
    factor = (ROWS * COLS * 128 // 4) ** (-0.5)
    sums = []
    for z in range(2):
        for y in range(2):
            total = None
            for zh in range(2):
                for k in range(8):
                    term = parts[zh, z, k, y].astype(F32)
                    total = term if total is None else total + term
            sums.append(total * factor)
    fine = (sums[0] + sums[1] + sums[2] + sums[3])[32:]
    tops = [v[:32] for v in sums]
    z_same = jnp.full((32, 128), zp, jnp.int32) == 0
    y_same = jnp.full((32, 128), yp, jnp.int32) == 0

    def related(zd, yd):
        low = [jnp.where(z_same, tops[2 * zd + y], tops[2 * (1 - zd) + y]) for y in range(2)]
        return jnp.where(y_same, low[yd], low[1 - yd])

    m0, m1, c0, c1 = (related(0, 0), related(0, 1), related(1, 1), related(1, 0))
    for h in range(4):
        lanes = pl.ds(128 * h, 128)
        rows = slice(8 * h, 8 * h + 8)
        merge[pl.ds(0, 8), lanes] = m0[rows]
        merge[pl.ds(8, 8), lanes] = m1[rows]
        cqkv[:, lanes] = c0[8 * h : 8 * h + 4]
        cqkv[:, pl.ds(D + 128 * h, 128)] = c0[8 * h + 4 : 8 * h + 8]
        cqkv[:, pl.ds(2 * D + 128 * h, 128)] = c1[8 * h : 8 * h + 4]
        cproj[:, lanes] = c1[8 * h + 4 : 8 * h + 8]
        fqkv[:, lanes] = fine[8 * h : 8 * h + 4]
        fqkv[pl.ds(2 * (h // 2), 2), pl.ds(D + 128 * (h % 2), 128)] = fine[8 * h + 4 : 8 * h + 6]
        fproj[:, lanes] = fine[8 * h + 6 : 8 * h + 8]
    for ref, coef, grad in ((fgain, fcoef, fqkv), (mgain, mcoef, merge), (cgain, ccoef, cqkv)):
        ref[...] = as_row(jnp.sum(coef[...] * grad[...], axis=1, keepdims=True))


def exchange(pieces, step):
    lat = lax.axis_size("lat")
    pair = lax.axis_size("pair")
    lon = 2 * pair
    arrived = []
    for piece, (dr, dc) in zip(pieces, ((0, 1), (1, 0), (1, 1))):
        pairs = []
        for r in range(lat):
            for c in range(lon):
                to = ((r + step * dr) % lat) * lon + (c + step * dc) % lon
                pairs.append((r * lon + c, to))
        arrived.append(lax.ppermute(piece, ("lat", "pair", "core"), pairs))
    return arrived


def partner(value):
    return lax.ppermute(value, "core", [(0, 1), (1, 0)])


def fold(value, axis, second):
    lat, pair = (lax.axis_size("lat"), lax.axis_size("pair"))
    pairs = []
    for r in range(lat):
        for p in range(pair):
            z, y = (r // 2, (r % 2) * 2 + p % 2)
            at = z if axis == "z" else y
            at = (at + (1 if at % 2 == (1 if second else 0) else -1)) % 4
            z, y = (at, y) if axis == "z" else (z, at)
            pairs.append((r * pair + p, (2 * z + y // 2) * pair + (p // 2) * 2 + y % 2))
    return lax.ppermute(value, ("lat", "pair"), pairs)


def deal(value):
    return lax.all_to_all(value, ("lat", "pair"), 0, 0)


def local(
    tokens, fine_gain, fine_qkv, fine_proj, merge_gain, merge_weight, coarse_gain, coarse_qkv, coarse_proj, cotangent
):
    lat_count = lax.axis_size("lat")
    lat, core = (lax.axis_index("lat"), lax.axis_index("core"))
    device = (lat * lax.axis_size("pair") + lax.axis_index("pair")) * 2 + core
    parity = lax.bitwise_and(lax.shift_right_logical(lat, 1), 1)
    seam = (lat == lat_count - 1).astype(jnp.int32)
    flip = lax.bitwise_and(lax.axis_index("pair"), 1)
    place = (device * 16 + seam * 8 + flip * 4 + parity * 2 + core).astype(jnp.int32).reshape(1)
    fgain, mgain, cgain = (v.reshape(1, -1) for v in (fine_gain, merge_gain, coarse_gain))
    cells = WINDOWS * CELLS

    pieces = [((size, D), BF16) for size in SLOTS]
    narrow = [((size, D), BF16) for size in NARROW]
    tok, *sent, cot = call(
        first_kernel,
        [((cells, D), BF16)] + pieces + [((CELLS, D), F32)],
        place,
        *(
            pltpu.with_memory_space_constraint(v, pltpu.HBM)
            for v in (tokens, cotangent, table("tok_send"), table("cot_send"))
        ),
        specs=[SMEM_SPEC] + [pl.BlockSpec(memory_space=pltpu.HBM)] * 4,
        scratch=[
            pltpu.VMEM((ROWS, COLS, D), BF16), pltpu.VMEM((6, 12, D), BF16), pltpu.VMEM((sum(SLOTS), cells), BF16),
            pltpu.VMEM((sum(SLOTS), CELLS), BF16), pltpu.SemaphoreType.DMA((4,)),
        ],
    )
    ahead = exchange(sent, -1)
    x, nm, p, w, y, *sent = scalar_call(
        fine_forward_kernel,
        [
            ((cells, D), BF16), ((cells, 768), BF16), ((cells, 768), F32), ((8, CELLS, 256), F32),
            ((cells, D), BF16),
        ]
        + narrow,
        place, tok, *ahead, fgain, fine_qkv, fine_proj, table("tok_main"), table("tok_halo"), table("y_send"),
        scratch=[pltpu.VMEM((cells, 256), F32)],
    )
    merged = exchange(sent, -1)
    nm_other = partner(nm)
    y2, df, *sent, fac = scalar_call(
        coarse_kernel,
        [((CELLS, D), BF16), ((cells, D), BF16)] + pieces + [((TALL, 5632), BF16)],
        place, y, *merged, cot, *ahead, mgain, merge_weight, cgain, coarse_qkv, coarse_proj,
        table("y_main"), table("y_halo"), table("cot_main"), table("cot_halo"), table("df_send"), table("out_send"),
        scratch=[
            pltpu.VMEM((CELLS, 1536), F32), pltpu.VMEM((CELLS, D), F32), pltpu.VMEM((CELLS, 1536), F32),
            pltpu.VMEM((4, CELLS, 256), F32),
        ],
    )
    back = exchange(sent, 1)
    mk, ms, ck, cs = scalar_call(
        coarse_weights_kernel,
        [((32, 64, 128), BF16)] * 4,
        place, fac, partner(fac),
        scratch=[pltpu.VMEM((4096, 128), F32)],
    )
    mc, cc = (fold(ms, "z", False), fold(cs, "z", True))
    dx, *sent, fac = scalar_call(
        fine_backward_kernel,
        [((cells, D), BF16)] + narrow + [((cells, 1280), BF16)],
        place, df, *back, x, p, w, fgain, fine_qkv, fine_proj, table("df_main"), table("df_halo"), table("dx_send"),
        scratch=[pltpu.VMEM((cells, 256), F32), pltpu.VMEM((cells, 768), F32)],
    )
    ended = exchange(sent, 1)
    m, ms, c, cs = call(middle_kernel, [((32, 32, 128), BF16)] * 4, mk, mc, ck, cc)
    mc, cc = (fold(ms, "y", False), fold(cs, "y", True))
    (fine_part,) = scalar_call(
        fine_weights_kernel,
        [((64, 32, 128), BF16)],
        place, nm, nm_other, fac, partner(fac),
        scratch=[pltpu.VMEM((2048, 128), F32)],
    )
    (joined,) = scalar_call(
        join_kernel,
        [((2, 2, 8, 2, 64, 128), BF16)],
        place, m, mc, c, cc, fine_part,
    )
    parts = deal(joined.reshape(64, 64, 128)).reshape(2, 2, 8, 2, 64, 128)
    (output,) = call(output_kernel, [((6, 12, D), BF16)], y2, *back, table("out_main"), table("out_halo"))
    (grad,) = call(tokens_kernel, [((ROWS, COLS, D), BF16)], dx, *ended, table("dx_main"), table("dx_halo"))
    fcoef, mcoef, ccoef = scalar_call(
        coefficients_kernel,
        [((4, 768), F32), ((16, D), F32), ((4, 1536), F32)],
        place, fgain, fine_qkv, mgain, merge_weight, cgain, coarse_qkv,
    )
    fg, fqkv, fproj, mg, merge, cg, cqkv, cproj = scalar_call(
        sum_kernel,
        [
            ((1, 4), F32), ((4, 768), F32), ((2, D), F32), ((1, 16), F32), ((16, D), F32), ((1, 4), F32),
            ((4, 1536), F32), ((4, D), F32),
        ],
        place, parts, fcoef, mcoef, ccoef,
    )
    fg, mg, cg = (v.reshape(-1) for v in (fg, mg, cg))
    return (output, grad, fg, fqkv, fproj, mg, merge, cg, cqkv, cproj)


def solution(mesh):
    lat, lon = (mesh.shape["lat"], mesh.shape["lon"])
    split = Mesh(mesh.devices.reshape(lat, lon // 2, 2), ("lat", "pair", "core"))
    lon = ("pair", "core")
    grid = P("lat", lon, None)
    whole = ("lat", "pair", "core")
    return jax.shard_map(
        local,
        mesh=split,
        in_specs=(grid, P(), P(), P(), P(), P(), P(), P(), P(), grid),
        out_specs=(
            grid, grid, P(whole), P(whole, None), P(whole, None), P(whole), P(whole, None), P(whole),
            P(whole, None), P(whole, None),
        ),
        check_vma=False,
    )
```

```python
import jax
import jax.numpy as jnp
import numpy as np
from jax import lax
from jax.experimental import pallas as pl
from jax.experimental.pallas import tpu as pltpu
from jax.sharding import Mesh, PartitionSpec as P

D = 512
HF = 4
HC = 8
CELLS = 72
TALL = 80
WINDOWS = 4
ROWS = 12
COLS = 24
EPSILON = 1e-05
NEGATIVE = -1000000000.0
LOWEST = -3.0e38
INTERPRET = False
VMEM_SPEC = pl.BlockSpec(memory_space=pltpu.VMEM)
SMEM_SPEC = pl.BlockSpec(memory_space=pltpu.SMEM)
VMEM_LIMIT = 12 * 1024 * 1024
FLOPS = 5_000_000_000
BYTES = 4_000_000


F32 = jnp.float32
BF16 = jnp.bfloat16


def window_order():
    return [
        (6 * a + r, 12 * b + c) for a in range(2) for b in range(2) for r in range(6) for c in range(12)
    ]


def patch_order():
    return [
        (2 * r + dr, 2 * c + dc) for dc in range(2) for dr in range(2) for r in range(6) for c in range(12)
    ]


def plain_order(rows, cols):
    return [(r, c) for r in range(rows) for c in range(cols)]


def leading(rows, cols):
    half_r, half_c = (3, 6)
    side = [(r, c) for r in range(half_r, rows) for c in range(half_c)]
    edge = [(r, c) for r in range(half_r) for c in range(half_c, cols)]
    corner = [(r, c) for r in range(half_r) for c in range(half_c)]
    return (side, edge, corner)


def trailing(rows, cols):
    half_r, half_c = (3, 6)
    side = [(r, c) for r in range(rows - half_r) for c in range(cols - half_c, cols)]
    edge = [(r, c) for r in range(rows - half_r, rows) for c in range(cols - half_c)]
    corner = [(r, c) for r in range(rows - half_r, rows) for c in range(cols - half_c, cols)]
    return (side, edge, corner)


SLOTS = (80, 80, 48)
NARROW = (64, 64, 32)
COARSE_AT = (56, 56, 24)


def pick(order, cells, places, total):
    where = {cell: i for i, cell in enumerate(order)}
    matrix = np.zeros((total, len(order)), np.float32)
    for place, cell in zip(places, cells):
        matrix[place, where[cell]] = 1.0
    return matrix


def send_matrix(order, pieces, starts, slots=SLOTS):
    cells, places, at = [], [], 0
    for piece, start, slot in zip(pieces, starts, slots):
        cells += piece
        places += [at + start + i for i in range(len(piece))]
        at += slot
    return pick(order, cells, places, at)


def take_matrices(own_order, out_cells, pieces, starts, shift, rows, cols, slots=SLOTS):
    own = {cell: i for i, cell in enumerate(own_order)}
    stack, at = {}, 0
    for piece, start, slot in zip(pieces, starts, slots):
        for i, cell in enumerate(piece):
            stack[cell] = at + start + i
        at += slot
    main = np.zeros((len(out_cells), len(own_order)), np.float32)
    halo = np.zeros((len(out_cells), at), np.float32)
    for i, cell in enumerate(out_cells):
        if cell is None:
            continue
        r, c = (cell[0] + shift[0], cell[1] + shift[1])
        if 0 <= r < rows and 0 <= c < cols:
            main[i, own[r, c]] = 1.0
        else:
            halo[i, stack[r % rows, c % cols]] = 1.0
    return main, halo


def padded_rows(rows, cols, height):
    return [(r, c) if c < cols else None for r in range(rows) for c in range(height)]


ZERO3 = (0, 0, 0)
PLAIN_F = plain_order(ROWS, COLS)
PLAIN_C = plain_order(6, 12)
TABLES = dict(
    tok_send=send_matrix(PLAIN_F, leading(ROWS, COLS), ZERO3),
    cot_send=send_matrix(PLAIN_C, leading(6, 12), COARSE_AT),
)
TABLES["tok_main"], TABLES["tok_halo"] = take_matrices(
    PLAIN_F, window_order(), leading(ROWS, COLS), ZERO3, (3, 6), ROWS, COLS
)
TABLES["cot_main"], TABLES["cot_halo"] = take_matrices(
    PLAIN_C, PLAIN_C, leading(6, 12), COARSE_AT, (3, 6), 6, 12
)
TABLES["y_send"] = send_matrix(window_order(), leading(ROWS, COLS), ZERO3, NARROW)
TABLES["y_main"], TABLES["y_halo"] = take_matrices(
    window_order(), patch_order(), leading(ROWS, COLS), ZERO3, (3, 6), ROWS, COLS, NARROW
)
TABLES["df_send"] = send_matrix(patch_order(), trailing(ROWS, COLS), ZERO3)
TABLES["df_main"], TABLES["df_halo"] = take_matrices(
    patch_order(), window_order(), trailing(ROWS, COLS), ZERO3, (-3, -6), ROWS, COLS
)
TABLES["out_send"] = send_matrix(PLAIN_C, trailing(6, 12), COARSE_AT)
TABLES["out_main"], TABLES["out_halo"] = take_matrices(
    PLAIN_C, padded_rows(6, 12, 16), trailing(6, 12), COARSE_AT, (-3, -6), 6, 12
)
TABLES["dx_send"] = send_matrix(window_order(), trailing(ROWS, COLS), ZERO3, NARROW)
TABLES["dx_main"], TABLES["dx_halo"] = take_matrices(
    window_order(), PLAIN_F, trailing(ROWS, COLS), ZERO3, (-3, -6), ROWS, COLS, NARROW
)


def table(name):
    return jnp.asarray(TABLES[name], BF16)


def mm(a, b):
    return lax.dot_general(a, b, (((1,), (0,)), ((), ())), preferred_element_type=F32)


def mm_nt(a, b):
    return lax.dot_general(a, b, (((1,), (1,)), ((), ())), preferred_element_type=F32)


def mm_tn(a, b):
    return lax.dot_general(a, b, (((0,), (0,)), ((), ())), preferred_element_type=F32)


def rounded(x):
    return x.astype(BF16).astype(F32)


def call(kernel, outs, *args, scratch=(), specs=None, limit=None):
    return pl.pallas_call(
        kernel,
        out_shape=[jax.ShapeDtypeStruct(s, d) for s, d in outs],
        in_specs=specs or [VMEM_SPEC] * len(args),
        out_specs=[VMEM_SPEC] * len(outs),
        scratch_shapes=list(scratch),
        compiler_params=pltpu.CompilerParams(vmem_limit_bytes=limit or VMEM_LIMIT),
        cost_estimate=pl.CostEstimate(flops=FLOPS, bytes_accessed=BYTES, transcendentals=0),
        interpret=INTERPRET,
    )(*args)


def scalar_call(kernel, outs, scalar, *args, scratch=()):
    return call(kernel, outs, scalar, *args, scratch=scratch, specs=[SMEM_SPEC] + [VMEM_SPEC] * len(args))


def cut(stack, *refs):
    at = 0
    for ref in refs:
        ref[...] = stack[at : at + ref.shape[0]]
        at += ref.shape[0]


def normalize(x):
    shifted = x - jnp.mean(x, axis=-1, keepdims=True)
    inverse = lax.rsqrt(jnp.mean(shifted * shifted, axis=-1, keepdims=True) + EPSILON)
    return shifted * inverse, inverse


def normalize_back(d, xhat, inverse):
    return inverse * (
        d - jnp.mean(d, axis=-1, keepdims=True) - xhat * jnp.mean(d * xhat, axis=-1, keepdims=True)
    )


def lane_half():
    lane = lax.broadcasted_iota(jnp.int32, (1, 128), 1)
    low = (lane < 64).astype(F32)
    return low, 1.0 - low


def stacked(x):
    low, high = lane_half()
    pad = jnp.zeros((128 - CELLS, 128), F32)
    return jnp.concatenate([x * low, pad, x * high, pad], axis=0).astype(BF16)


def unstacked(x):
    low, high = lane_half()
    return x[:CELLS] * low + x[128 : 128 + CELLS] * high


def key_lanes():
    lane = lax.broadcasted_iota(jnp.int32, (CELLS, 256), 1)
    return jnp.where(lane >= 128, lane - 128, lane)


def apart(split):
    row = lax.broadcasted_iota(jnp.int32, (CELLS, 256), 0)
    key = key_lanes()
    differ = (row >= CELLS // 2) != (key >= CELLS // 2)
    return jnp.logical_and(differ, split)


def halves(fn, x):
    return jnp.concatenate(
        [jnp.broadcast_to(fn(x[:, :128]), (CELLS, 128)), jnp.broadcast_to(fn(x[:, 128:]), (CELLS, 128))],
        axis=1,
    )


def attend(q, k2, v2, differ):
    scores = mm_nt(q.astype(BF16), k2) * 0.125
    scores = jnp.where(differ, NEGATIVE, scores)
    scores = jnp.where(key_lanes() < CELLS, scores, LOWEST)
    exponent = jnp.exp(scores - halves(lambda s: jnp.max(s, axis=1, keepdims=True), scores))
    weights = exponent / halves(lambda s: jnp.sum(s, axis=1, keepdims=True), exponent)
    return weights, mm(weights.astype(BF16), v2)


def attend_back(q, k2, v2, weights, differ, d):
    d = d.astype(BF16)
    dv = unstacked(mm_tn(weights.astype(BF16), d))
    dw = rounded(mm_nt(d, v2))
    ds = weights * (dw - halves(lambda s: jnp.sum(s, axis=1, keepdims=True), dw * weights))
    ds = jnp.where(differ, 0.0, ds * 0.125).astype(BF16)
    dq = mm(ds, k2)
    dk = unstacked(mm_tn(ds, q.astype(BF16)))
    return dq, dk, dv


def first_kernel(
    place, tok_in, cot_in, tok_send_in, cot_send_in, tok2d, side, edge, corner, cot2d,
    tok, cot, tok_send, cot_send, arrived,
):
    loads = [
        pltpu.make_async_copy(source, target, arrived.at[i])
        for i, (source, target) in enumerate(
            ((tok_in, tok), (cot_in, cot), (tok_send_in, tok_send), (cot_send_in, cot_send))
        )
    ]
    for load in loads:
        load.start()
    for load in loads:
        load.wait()
    x = tok[...].astype(F32).reshape(ROWS * COLS, D).astype(BF16)
    tok2d[...] = x
    for r in range(6):
        cot2d[pl.ds(12 * r, 12), :] = cot[r].astype(F32)
    y = cot2d[...].astype(BF16)
    stack = (mm(tok_send[...], x) + mm(cot_send[...], y)).astype(BF16)
    cut(stack, side, edge, corner)


def fine_forward_kernel(
    place, x_in, side, edge, corner, gain, wqkv, wproj, t_main, t_halo, y_send,
    x_out, nm_out, p_out, w_out, y_out, side_out, edge_out, corner_out, mixed,
):
    halo = jnp.concatenate([side[...], edge[...], corner[...]], axis=0)
    x = mm(t_main[...], x_in[...]) + mm(t_halo[...], halo)
    x_out[...] = x.astype(BF16)
    xhat, _ = normalize(x)
    n = (xhat * gain[...]).astype(BF16)
    nm_out[:, pl.ds(0, D)] = n
    p_out[...] = rounded(mm(n, wqkv[...]))
    for w in range(WINDOWS):
        differ = apart(decode(place)[3] == 1 if w >= 2 else False)
        for p in range(HF // 2):
            rows = pl.ds(CELLS * w, CELLS)
            q, k, v = (p_out[rows, pl.ds(256 * part + 128 * p, 128)] for part in range(3))
            weights, out = attend(q, stacked(k), stacked(v), differ)
            w_out[2 * w + p] = weights
            mixed[rows, pl.ds(128 * p, 128)] = out
    m = mixed[...].astype(BF16)
    nm_out[:, pl.ds(D, 256)] = m
    y = (x + mm(m, wproj[...])).astype(BF16)
    y_out[...] = y
    stack = mm(y_send[...], y).astype(BF16)
    cut(stack, side_out, edge_out, corner_out)


def coarse_kernel(
    place, y_in, side, edge, corner, cot_in, cside, cedge, ccorner,
    mgain, mweight, gain, wqkv, wproj, y_main, y_halo, c_main, c_halo, df_send, out_send,
    y2_out, df_out, side_out, edge_out, corner_out, fac_out, packed, mixed, dpacked, wsave,
):
    halo = jnp.concatenate([side[...], edge[...], corner[...]], axis=0)
    patches = mm(y_main[...], y_in[...]) + mm(y_halo[...], halo)
    g = jnp.concatenate([patches[CELLS * i : CELLS * (i + 1)] for i in range(4)], axis=1)
    ghat, ginv = normalize(g)
    mn = (ghat * mgain[...]).astype(BF16)
    z = rounded(mm(mn, mweight[...]))
    zhat, zinv = normalize(z)
    n = (zhat * gain[...]).astype(BF16)
    packed[...] = rounded(mm(n, wqkv[...]))
    differ = apart(decode(place)[3] == 1)
    for p in range(HC // 2):
        lanes = pl.ds(128 * p, 128)
        q, k, v = (packed[:, pl.ds(512 * part + 128 * p, 128)] for part in range(3))
        weights, out = attend(q, stacked(k), stacked(v), differ)
        wsave[p] = weights
        mixed[:, lanes] = out
    m = mixed[...].astype(BF16)
    y2 = (z + mm(m, wproj[...])).astype(BF16)
    y2_out[...] = y2

    chalo = jnp.concatenate([cside[...], cedge[...], ccorner[...]], axis=0)
    dy = mm(c_main[...], cot_in[...].astype(BF16)) + mm(c_halo[...], chalo)
    mixed[...] = rounded(mm_nt(dy.astype(BF16), wproj[...]))
    for p in range(HC // 2):
        q, k, v = (packed[:, pl.ds(512 * part + 128 * p, 128)] for part in range(3))
        grads = attend_back(q, stacked(k), stacked(v), wsave[p], differ, mixed[:, pl.ds(128 * p, 128)])
        for part in range(3):
            dpacked[:, pl.ds(512 * part + 128 * p, 128)] = grads[part]
    dp = dpacked[...].astype(BF16)
    dn = rounded(mm_nt(dp, wqkv[...]))
    dz = (dy + normalize_back(dn * gain[...], zhat, zinv)).astype(BF16)
    dmn = rounded(mm_nt(dz, mweight[...]))
    dg = normalize_back(dmn * mgain[...], ghat, ginv)
    df = jnp.concatenate([dg[:, D * i : D * (i + 1)] for i in range(4)], axis=0).astype(BF16)
    df_out[...] = df
    stack = (mm(df_send[...], df) + mm(out_send[...], y2)).astype(BF16)
    cut(stack, side_out, edge_out, corner_out)
    at = 0
    for piece in (mn, n, m, dz, dp, dy.astype(BF16)):
        fac_out[pl.ds(0, CELLS), pl.ds(at, piece.shape[1])] = piece
        at += piece.shape[1]
    fac_out[pl.ds(CELLS, TALL - CELLS), :] = jnp.zeros((TALL - CELLS, at), BF16)


def fine_backward_kernel(
    place, df_in, side, edge, corner, x_in, p_in, w_in, gain, wqkv, wproj, d_main, d_halo, dx_send,
    dx_out, side_out, edge_out, corner_out, fac_out, dmixed, dpacked,
):
    halo = jnp.concatenate([side[...], edge[...], corner[...]], axis=0)
    dy = mm(d_main[...], df_in[...]) + mm(d_halo[...], halo)
    dmixed[...] = rounded(mm_nt(dy.astype(BF16), wproj[...]))
    for w in range(WINDOWS):
        differ = apart(decode(place)[3] == 1 if w >= 2 else False)
        for p in range(HF // 2):
            rows = pl.ds(CELLS * w, CELLS)
            q, k, v = (p_in[rows, pl.ds(256 * part + 128 * p, 128)] for part in range(3))
            d = dmixed[rows, pl.ds(128 * p, 128)]
            grads = attend_back(q, stacked(k), stacked(v), w_in[2 * w + p], differ, d)
            for part in range(3):
                dpacked[rows, pl.ds(256 * part + 128 * p, 128)] = grads[part]
    dp = dpacked[...].astype(BF16)
    dn = rounded(mm_nt(dp, wqkv[...]))
    xhat, inverse = normalize(x_in[...].astype(F32))
    dx = (dy + normalize_back(dn * gain[...], xhat, inverse)).astype(BF16)
    dx_out[...] = dx
    stack = mm(dx_send[...], dx).astype(BF16)
    cut(stack, side_out, edge_out, corner_out)
    fac_out[:, pl.ds(0, 768)] = dp
    fac_out[:, pl.ds(768, D)] = dy.astype(BF16)


def decode(place):
    code = place[0]
    bits = tuple(lax.bitwise_and(lax.shift_right_logical(code, i), 1) for i in range(4))
    return bits + (lax.shift_right_logical(code, 4),)


def one_hot(want, width):
    lane = lax.broadcasted_iota(jnp.int32, (want.shape[0], width), 1)
    return jnp.where(lane == want, 1.0, 0.0).astype(BF16)


def row_index(count):
    return lax.broadcasted_iota(jnp.int32, (count, 1), 0)


def field(x, low, bits):
    return lax.bitwise_and(lax.shift_right_logical(x, low), (1 << bits) - 1)


def coarse_weights_kernel(
    place, own, other, m0k, m0s, m1k, m1s, c0k, c0s, c1k, c1s, lines
):
    core, zp, yp, _, _ = decode(place)

    def at(start, size):
        return jnp.concatenate([own[:, pl.ds(start, size)], other[:, pl.ds(start, size)]], axis=0)

    dz = at(2048 + 1024, D)
    row = row_index(256)
    group = field(row, 4, 3) * 2 + lax.bitwise_xor(field(row, 7, 1), yp)
    select = one_hot((2 * group + core) * 16 + field(row, 0, 4), D)
    for zh in range(2):
        pair = [at(D * (2 * zh + k), D) for k in range(2)]
        plain = jnp.full(pair[0].shape, zp, jnp.int32) == 0
        ordered = (
            jnp.where(plain, pair[0].astype(F32), pair[1].astype(F32)).astype(BF16),
            jnp.where(plain, pair[1].astype(F32), pair[0].astype(F32)).astype(BF16),
        )
        for zd in range(2):
            left = mm_nt(select, ordered[zd]).astype(BF16)
            part = mm(left, dz).reshape(16, 16, D)
            for yd in range(2):
                for h in range(4):
                    piece = part[8 * yd : 8 * yd + 8, :, 128 * h : 128 * h + 128]
                    (m0s if zd else m0k)[pl.ds(16 * yd + 8 * zh, 8), pl.ds(8 * h, 8), :] = piece[:, :8].astype(BF16)
                    (m1s if yd else m1k)[pl.ds(16 * zd + 8 * zh, 8), pl.ds(8 * h, 8), :] = piece[:, 8:].astype(BF16)
    row = row_index(256)
    z = field(row, 3, 1) * 2 + lax.bitwise_xor(field(row, 5, 1), zp)
    group = z * 16 + field(row, 0, 3) * 2 + lax.bitwise_xor(field(row, 4, 1), yp)
    select = one_hot((2 * group + core) * 4 + field(row, 6, 2), D)
    n = mm_nt(select, at(2048, D)).astype(BF16)
    m = mm_nt(select, at(2048 + D, D)).astype(BF16)
    for j in range(4):
        part = mm(n if j < 3 else m, at(2048 + 1536 + D * j, D))
        for i in range(4):
            line = part[64 * i : 64 * (i + 1)]
            for h in range(4):
                lines[pl.ds(512 * (4 * (j // 2) + h) + 4 * (j % 2) + i, 64, 8), :] = line[:, 128 * h : 128 * h + 128]
    for h in range(4):
        first = lines[pl.ds(512 * h, 512), :].reshape(64, 8, 128).astype(BF16)
        c0s[:, pl.ds(8 * h, 8), :] = first[:32]
        c0k[:, pl.ds(8 * h, 8), :] = first[32:]
        second = lines[pl.ds(512 * (4 + h), 512), :].reshape(64, 8, 128).astype(BF16)
        for zd in range(2):
            c1s[pl.ds(16 * zd, 16), pl.ds(8 * h, 8), :] = second[32 * zd : 32 * zd + 16]
            c1k[pl.ds(16 * zd, 16), pl.ds(8 * h, 8), :] = second[32 * zd + 16 : 32 * zd + 32]


def middle_kernel(m0k, m0c, m1k, m1c, c0k, c0c, c1k, c1c, y_keep, y_send, z_keep, z_send):
    for keep, came, at, first, second in (
        (m0k, m0c, 0, y_keep, y_send), (c0k, c0c, 16, y_send, y_keep),
        (m1k, m1c, 0, z_send, z_keep), (c1k, c1c, 16, z_keep, z_send),
    ):
        total = (keep[...].astype(F32) + came[...].astype(F32)).astype(BF16)
        first[pl.ds(at, 16)] = total[:16]
        second[pl.ds(at, 16)] = total[16:]


def fine_weights_kernel(place, nm_own, nm_other, own, other, out, lines):
    core = decode(place)[0]
    row = row_index(256)
    select = one_hot((2 * field(row, 0, 6) + core) * 4 + field(row, 6, 2), D)
    dp = lambda ref: ref[:, pl.ds(0, 768)]
    dy = lambda ref: ref[:, pl.ds(768, D)]
    n = [mm_nt(select, ref[:, pl.ds(0, D)]).astype(BF16) for ref in (nm_own, nm_other)]
    part = mm(n[0], dp(own)) + mm(n[1], dp(other))
    for i in range(4):
        line = part[64 * i : 64 * (i + 1)]
        for h in range(4):
            lines[pl.ds(512 * h + i, 64, 8), :] = line[:, 128 * h : 128 * h + 128]
        for h in range(2):
            lines[pl.ds(512 * (2 * (i // 2) + h) + 4 + i % 2, 64, 8), :] = line[:, 512 + 128 * h : 640 + 128 * h]
    row = row_index(128)
    select = one_hot((2 * field(row, 0, 6) + core) * 2 + field(row, 6, 1), 256)
    m = [mm_nt(select, ref[:, pl.ds(D, 256)]).astype(BF16) for ref in (nm_own, nm_other)]
    part = mm(m[0], dy(own)) + mm(m[1], dy(other))
    for i in range(2):
        line = part[64 * i : 64 * (i + 1)]
        for h in range(4):
            lines[pl.ds(512 * h + 6 + i, 64, 8), :] = line[:, 128 * h : 128 * h + 128]
    for h in range(4):
        out[:, pl.ds(8 * h, 8), :] = lines[pl.ds(512 * h, 512), :].reshape(64, 8, 128).astype(BF16)


def join_kernel(place, yk, yc, zk, zc, fine, out):
    _, zp, yp, _, _ = decode(place)
    for keep, came, relations in ((yk, yc, ((0, 0), (1, 1))), (zk, zc, ((1, 0), (0, 1)))):
        total = (keep[...].astype(F32) + came[...].astype(F32)).astype(BF16)
        for part, (zd, yd) in enumerate(relations):
            for zh in range(2):
                at = 16 * part + 8 * zh
                out[zh, lax.bitwise_xor(zp, zd), :, lax.bitwise_xor(yp, yd), pl.ds(0, 32), :] = total[at : at + 8]
    out[:, :, :, :, pl.ds(32, 32), :] = fine[...].reshape(2, 2, 8, 2, 32, 128)


def gain_rows(weight, gain, device, share):
    count = max(8, share)
    pick_rows = one_hot(device * share + row_index(count), gain.shape[1])
    over = jnp.sum(pick_rows.astype(F32) * gain, axis=1, keepdims=True)
    return mm(pick_rows, weight)[:share] / over[:share]


def coefficients_kernel(place, fgain, fqkv, mgain, mweight, cgain, cqkv, fcoef, mcoef, ccoef):
    device = decode(place)[4]
    fcoef[...] = gain_rows(fqkv[...], fgain[...], device, 4)
    mcoef[...] = gain_rows(mweight[...], mgain[...], device, 16)
    ccoef[...] = gain_rows(cqkv[...], cgain[...], device, 4)


def output_kernel(y2, side, edge, corner, out_main, out_halo, out):
    halo = jnp.concatenate([side[...], edge[...], corner[...]], axis=0)
    y = mm(out_main[...], y2[...]) + mm(out_halo[...], halo)
    for r in range(6):
        out[r] = y[16 * r : 16 * r + 12].astype(BF16)


def tokens_kernel(dx, side, edge, corner, dx_main, dx_halo, grad):
    halo = jnp.concatenate([side[...], edge[...], corner[...]], axis=0)
    d = mm(dx_main[...], dx[...]) + mm(dx_halo[...], halo)
    grad[...] = d.reshape(ROWS, COLS, D).astype(BF16)


def as_row(column):
    size = column.shape[0]
    row = lax.broadcasted_iota(jnp.int32, (size, size), 0)
    lane = lax.broadcasted_iota(jnp.int32, (size, size), 1)
    return jnp.sum(jnp.where(row == lane, column, 0.0), axis=0, keepdims=True)


def sum_kernel(place, parts, fcoef, mcoef, ccoef, fgain, fqkv, fproj, mgain, merge, cgain, cqkv, cproj):
    _, zp, yp, _, _ = decode(place)
    factor = (ROWS * COLS * 128 // 4) ** (-0.5)
    sums = []
    for z in range(2):
        for y in range(2):
            total = None
            for zh in range(2):
                for k in range(8):
                    term = parts[zh, z, k, y].astype(F32)
                    total = term if total is None else total + term
            sums.append(total * factor)
    fine = (sums[0] + sums[1] + sums[2] + sums[3])[32:]
    tops = [v[:32] for v in sums]
    z_same = jnp.full((32, 128), zp, jnp.int32) == 0
    y_same = jnp.full((32, 128), yp, jnp.int32) == 0

    def related(zd, yd):
        low = [jnp.where(z_same, tops[2 * zd + y], tops[2 * (1 - zd) + y]) for y in range(2)]
        return jnp.where(y_same, low[yd], low[1 - yd])

    m0, m1, c0, c1 = (related(0, 0), related(1, 0), related(1, 1), related(0, 1))
    for h in range(4):
        lanes = pl.ds(128 * h, 128)
        rows = slice(8 * h, 8 * h + 8)
        merge[pl.ds(0, 8), lanes] = m0[rows]
        merge[pl.ds(8, 8), lanes] = m1[rows]
        cqkv[:, lanes] = c0[8 * h : 8 * h + 4]
        cqkv[:, pl.ds(D + 128 * h, 128)] = c0[8 * h + 4 : 8 * h + 8]
        cqkv[:, pl.ds(2 * D + 128 * h, 128)] = c1[8 * h : 8 * h + 4]
        cproj[:, lanes] = c1[8 * h + 4 : 8 * h + 8]
        fqkv[:, lanes] = fine[8 * h : 8 * h + 4]
        fqkv[pl.ds(2 * (h // 2), 2), pl.ds(D + 128 * (h % 2), 128)] = fine[8 * h + 4 : 8 * h + 6]
        fproj[:, lanes] = fine[8 * h + 6 : 8 * h + 8]
    for ref, coef, grad in ((fgain, fcoef, fqkv), (mgain, mcoef, merge), (cgain, ccoef, cqkv)):
        ref[...] = as_row(jnp.sum(coef[...] * grad[...], axis=1, keepdims=True))


def exchange(pieces, step):
    lat = lax.axis_size("lat")
    pair = lax.axis_size("pair")
    lon = 2 * pair
    arrived = []
    for piece, (dr, dc) in zip(pieces, ((0, 1), (1, 0), (1, 1))):
        pairs = []
        for r in range(lat):
            for c in range(lon):
                to = ((r + step * dr) % lat) * lon + (c + step * dc) % lon
                pairs.append((r * lon + c, to))
        arrived.append(lax.ppermute(piece, ("lat", "pair", "core"), pairs))
    return arrived


def partner(value):
    return lax.ppermute(value, "core", [(0, 1), (1, 0)])


def fold(value, axis, second):
    lat, pair = (lax.axis_size("lat"), lax.axis_size("pair"))
    pairs = []
    for r in range(lat):
        for p in range(pair):
            z, y = (r // 2, (r % 2) * 2 + p % 2)
            at = z if axis == "z" else y
            at = (at + (1 if at % 2 == (1 if second else 0) else -1)) % 4
            z, y = (at, y) if axis == "z" else (z, at)
            pairs.append((r * pair + p, (2 * z + y // 2) * pair + (p // 2) * 2 + y % 2))
    return lax.ppermute(value, ("lat", "pair"), pairs)


def deal(value):
    return lax.all_to_all(value, ("lat", "pair"), 0, 0)


def local(
    tokens, fine_gain, fine_qkv, fine_proj, merge_gain, merge_weight, coarse_gain, coarse_qkv, coarse_proj, cotangent
):
    lat_count = lax.axis_size("lat")
    lat, core = (lax.axis_index("lat"), lax.axis_index("core"))
    device = (lat * lax.axis_size("pair") + lax.axis_index("pair")) * 2 + core
    parity = lax.bitwise_and(lax.shift_right_logical(lat, 1), 1)
    seam = (lat == lat_count - 1).astype(jnp.int32)
    flip = lax.bitwise_and(lax.axis_index("pair"), 1)
    place = (device * 16 + seam * 8 + flip * 4 + parity * 2 + core).astype(jnp.int32).reshape(1)
    fgain, mgain, cgain = (v.reshape(1, -1) for v in (fine_gain, merge_gain, coarse_gain))
    cells = WINDOWS * CELLS

    pieces = [((size, D), BF16) for size in SLOTS]
    narrow = [((size, D), BF16) for size in NARROW]
    tok, *sent, cot = call(
        first_kernel,
        [((cells, D), BF16)] + pieces + [((CELLS, D), F32)],
        place,
        *(
            pltpu.with_memory_space_constraint(v, pltpu.HBM)
            for v in (tokens, cotangent, table("tok_send"), table("cot_send"))
        ),
        specs=[SMEM_SPEC] + [pl.BlockSpec(memory_space=pltpu.HBM)] * 4,
        scratch=[
            pltpu.VMEM((ROWS, COLS, D), BF16), pltpu.VMEM((6, 12, D), BF16), pltpu.VMEM((sum(SLOTS), cells), BF16),
            pltpu.VMEM((sum(SLOTS), CELLS), BF16), pltpu.SemaphoreType.DMA((4,)),
        ],
    )
    ahead = exchange(sent, -1)
    x, nm, p, w, y, *sent = scalar_call(
        fine_forward_kernel,
        [
            ((cells, D), BF16), ((cells, 768), BF16), ((cells, 768), F32), ((8, CELLS, 256), F32),
            ((cells, D), BF16),
        ]
        + narrow,
        place, tok, *ahead, fgain, fine_qkv, fine_proj, table("tok_main"), table("tok_halo"), table("y_send"),
        scratch=[pltpu.VMEM((cells, 256), F32)],
    )
    merged = exchange(sent, -1)
    nm_other = partner(nm)
    y2, df, *sent, fac = scalar_call(
        coarse_kernel,
        [((CELLS, D), BF16), ((cells, D), BF16)] + pieces + [((TALL, 5632), BF16)],
        place, y, *merged, cot, *ahead, mgain, merge_weight, cgain, coarse_qkv, coarse_proj,
        table("y_main"), table("y_halo"), table("cot_main"), table("cot_halo"), table("df_send"), table("out_send"),
        scratch=[
            pltpu.VMEM((CELLS, 1536), F32), pltpu.VMEM((CELLS, D), F32), pltpu.VMEM((CELLS, 1536), F32),
            pltpu.VMEM((4, CELLS, 256), F32),
        ],
    )
    back = exchange(sent, 1)
    m0k, m0s, m1k, m1s, c0k, c0s, c1k, c1s = scalar_call(
        coarse_weights_kernel,
        [((32, 32, 128), BF16)] * 8,
        place, fac, partner(fac),
        scratch=[pltpu.VMEM((4096, 128), F32)],
    )
    first = [
        fold(v, axis, second)
        for v, axis, second in ((m0s, "z", False), (m1s, "y", False), (c0s, "z", True), (c1s, "y", True))
    ]
    dx, *sent, fac = scalar_call(
        fine_backward_kernel,
        [((cells, D), BF16)] + narrow + [((cells, 1280), BF16)],
        place, df, *back, x, p, w, fgain, fine_qkv, fine_proj, table("df_main"), table("df_halo"), table("dx_send"),
        scratch=[pltpu.VMEM((cells, 256), F32), pltpu.VMEM((cells, 768), F32)],
    )
    ended = exchange(sent, 1)
    y_keep, y_send, z_keep, z_send = call(
        middle_kernel,
        [((32, 32, 128), BF16)] * 4,
        m0k, first[0], m1k, first[1], c0k, first[2], c1k, first[3],
    )
    y_came, z_came = (fold(y_send, "y", False), fold(z_send, "z", False))
    (fine_part,) = scalar_call(
        fine_weights_kernel,
        [((64, 32, 128), BF16)],
        place, nm, nm_other, fac, partner(fac),
        scratch=[pltpu.VMEM((2048, 128), F32)],
    )
    (joined,) = scalar_call(
        join_kernel,
        [((2, 2, 8, 2, 64, 128), BF16)],
        place, y_keep, y_came, z_keep, z_came, fine_part,
    )
    parts = deal(joined.reshape(64, 64, 128)).reshape(2, 2, 8, 2, 64, 128)
    (output,) = call(output_kernel, [((6, 12, D), BF16)], y2, *back, table("out_main"), table("out_halo"))
    (grad,) = call(tokens_kernel, [((ROWS, COLS, D), BF16)], dx, *ended, table("dx_main"), table("dx_halo"))
    fcoef, mcoef, ccoef = scalar_call(
        coefficients_kernel,
        [((4, 768), F32), ((16, D), F32), ((4, 1536), F32)],
        place, fgain, fine_qkv, mgain, merge_weight, cgain, coarse_qkv,
    )
    fg, fqkv, fproj, mg, merge, cg, cqkv, cproj = scalar_call(
        sum_kernel,
        [
            ((1, 4), F32), ((4, 768), F32), ((2, D), F32), ((1, 16), F32), ((16, D), F32), ((1, 4), F32),
            ((4, 1536), F32), ((4, D), F32),
        ],
        place, parts, fcoef, mcoef, ccoef,
    )
    fg, mg, cg = (v.reshape(-1) for v in (fg, mg, cg))
    return (output, grad, fg, fqkv, fproj, mg, merge, cg, cqkv, cproj)


def solution(mesh):
    lat, lon = (mesh.shape["lat"], mesh.shape["lon"])
    split = Mesh(mesh.devices.reshape(lat, lon // 2, 2), ("lat", "pair", "core"))
    lon = ("pair", "core")
    grid = P("lat", lon, None)
    whole = ("lat", "pair", "core")
    return jax.shard_map(
        local,
        mesh=split,
        in_specs=(grid, P(), P(), P(), P(), P(), P(), P(), P(), grid),
        out_specs=(
            grid, grid, P(whole), P(whole, None), P(whole, None), P(whole), P(whole, None), P(whole),
            P(whole, None), P(whole, None),
        ),
        check_vma=False,
    )
```

```python
import jax
import jax.numpy as jnp
import numpy as np
from jax import lax
from jax.experimental import pallas as pl
from jax.experimental.pallas import tpu as pltpu
from jax.sharding import Mesh, PartitionSpec as P

D = 512
HF = 4
HC = 8
CELLS = 72
TALL = 80
WINDOWS = 4
ROWS = 12
COLS = 24
EPSILON = 1e-05
NEGATIVE = -1000000000.0
LOWEST = -3.0e38
INTERPRET = False
VMEM_SPEC = pl.BlockSpec(memory_space=pltpu.VMEM)
SMEM_SPEC = pl.BlockSpec(memory_space=pltpu.SMEM)
VMEM_LIMIT = 12 * 1024 * 1024
FLOPS = 5_000_000_000
BYTES = 4_000_000


F32 = jnp.float32
BF16 = jnp.bfloat16


def window_order():
    return [
        (6 * a + r, 12 * b + c) for a in range(2) for b in range(2) for r in range(6) for c in range(12)
    ]


def patch_order():
    return [
        (2 * r + dr, 2 * c + dc) for dc in range(2) for dr in range(2) for r in range(6) for c in range(12)
    ]


def plain_order(rows, cols):
    return [(r, c) for r in range(rows) for c in range(cols)]


def leading(rows, cols):
    half_r, half_c = (3, 6)
    side = [(r, c) for r in range(half_r, rows) for c in range(half_c)]
    edge = [(r, c) for r in range(half_r) for c in range(half_c, cols)]
    corner = [(r, c) for r in range(half_r) for c in range(half_c)]
    return (side, edge, corner)


def trailing(rows, cols):
    half_r, half_c = (3, 6)
    side = [(r, c) for r in range(rows - half_r) for c in range(cols - half_c, cols)]
    edge = [(r, c) for r in range(rows - half_r, rows) for c in range(cols - half_c)]
    corner = [(r, c) for r in range(rows - half_r, rows) for c in range(cols - half_c, cols)]
    return (side, edge, corner)


SLOTS = (80, 80, 48)
NARROW = (64, 64, 32)
COARSE_AT = (56, 56, 24)


def pick(order, cells, places, total):
    where = {cell: i for i, cell in enumerate(order)}
    matrix = np.zeros((total, len(order)), np.float32)
    for place, cell in zip(places, cells):
        matrix[place, where[cell]] = 1.0
    return matrix


def send_matrix(order, pieces, starts, slots=SLOTS):
    cells, places, at = [], [], 0
    for piece, start, slot in zip(pieces, starts, slots):
        cells += piece
        places += [at + start + i for i in range(len(piece))]
        at += slot
    return pick(order, cells, places, at)


def take_matrices(own_order, out_cells, pieces, starts, shift, rows, cols, slots=SLOTS):
    own = {cell: i for i, cell in enumerate(own_order)}
    stack, at = {}, 0
    for piece, start, slot in zip(pieces, starts, slots):
        for i, cell in enumerate(piece):
            stack[cell] = at + start + i
        at += slot
    main = np.zeros((len(out_cells), len(own_order)), np.float32)
    halo = np.zeros((len(out_cells), at), np.float32)
    for i, cell in enumerate(out_cells):
        if cell is None:
            continue
        r, c = (cell[0] + shift[0], cell[1] + shift[1])
        if 0 <= r < rows and 0 <= c < cols:
            main[i, own[r, c]] = 1.0
        else:
            halo[i, stack[r % rows, c % cols]] = 1.0
    return main, halo


def padded_rows(rows, cols, height):
    return [(r, c) if c < cols else None for r in range(rows) for c in range(height)]


ZERO3 = (0, 0, 0)
PLAIN_F = plain_order(ROWS, COLS)
PLAIN_C = plain_order(6, 12)
TABLES = dict(
    tok_send=send_matrix(PLAIN_F, leading(ROWS, COLS), ZERO3),
    cot_send=send_matrix(PLAIN_C, leading(6, 12), COARSE_AT),
)
TABLES["tok_main"], TABLES["tok_halo"] = take_matrices(
    PLAIN_F, window_order(), leading(ROWS, COLS), ZERO3, (3, 6), ROWS, COLS
)
TABLES["cot_main"], TABLES["cot_halo"] = take_matrices(
    PLAIN_C, PLAIN_C, leading(6, 12), COARSE_AT, (3, 6), 6, 12
)
TABLES["y_send"] = send_matrix(window_order(), leading(ROWS, COLS), ZERO3, NARROW)
TABLES["y_main"], TABLES["y_halo"] = take_matrices(
    window_order(), patch_order(), leading(ROWS, COLS), ZERO3, (3, 6), ROWS, COLS, NARROW
)
TABLES["df_send"] = send_matrix(patch_order(), trailing(ROWS, COLS), ZERO3)
TABLES["df_main"], TABLES["df_halo"] = take_matrices(
    patch_order(), window_order(), trailing(ROWS, COLS), ZERO3, (-3, -6), ROWS, COLS
)
TABLES["out_send"] = send_matrix(PLAIN_C, trailing(6, 12), COARSE_AT)
TABLES["out_main"], TABLES["out_halo"] = take_matrices(
    PLAIN_C, padded_rows(6, 12, 16), trailing(6, 12), COARSE_AT, (-3, -6), 6, 12
)
TABLES["dx_send"] = send_matrix(window_order(), trailing(ROWS, COLS), ZERO3, NARROW)
TABLES["dx_main"], TABLES["dx_halo"] = take_matrices(
    window_order(), PLAIN_F, trailing(ROWS, COLS), ZERO3, (-3, -6), ROWS, COLS, NARROW
)


def table(name):
    return jnp.asarray(TABLES[name], BF16)


def mm(a, b):
    return lax.dot_general(a, b, (((1,), (0,)), ((), ())), preferred_element_type=F32)


def mm_nt(a, b):
    return lax.dot_general(a, b, (((1,), (1,)), ((), ())), preferred_element_type=F32)


def mm_tn(a, b):
    return lax.dot_general(a, b, (((0,), (0,)), ((), ())), preferred_element_type=F32)


def rounded(x):
    return x.astype(BF16).astype(F32)


def call(kernel, outs, *args, scratch=(), specs=None, limit=None):
    return pl.pallas_call(
        kernel,
        out_shape=[jax.ShapeDtypeStruct(s, d) for s, d in outs],
        in_specs=specs or [VMEM_SPEC] * len(args),
        out_specs=[VMEM_SPEC] * len(outs),
        scratch_shapes=list(scratch),
        compiler_params=pltpu.CompilerParams(vmem_limit_bytes=limit or VMEM_LIMIT),
        cost_estimate=pl.CostEstimate(flops=FLOPS, bytes_accessed=BYTES, transcendentals=0),
        interpret=INTERPRET,
    )(*args)


def scalar_call(kernel, outs, scalar, *args, scratch=()):
    return call(kernel, outs, scalar, *args, scratch=scratch, specs=[SMEM_SPEC] + [VMEM_SPEC] * len(args))


def cut(stack, *refs):
    at = 0
    for ref in refs:
        ref[...] = stack[at : at + ref.shape[0]]
        at += ref.shape[0]


def normalize(x):
    shifted = x - jnp.mean(x, axis=-1, keepdims=True)
    inverse = lax.rsqrt(jnp.mean(shifted * shifted, axis=-1, keepdims=True) + EPSILON)
    return shifted * inverse, inverse


def normalize_back(d, xhat, inverse):
    return inverse * (
        d - jnp.mean(d, axis=-1, keepdims=True) - xhat * jnp.mean(d * xhat, axis=-1, keepdims=True)
    )


def lane_half():
    lane = lax.broadcasted_iota(jnp.int32, (1, 128), 1)
    low = (lane < 64).astype(F32)
    return low, 1.0 - low


def stacked(x):
    low, high = lane_half()
    pad = jnp.zeros((128 - CELLS, 128), F32)
    return jnp.concatenate([x * low, pad, x * high, pad], axis=0).astype(BF16)


def unstacked(x):
    low, high = lane_half()
    return x[:CELLS] * low + x[128 : 128 + CELLS] * high


def key_lanes():
    lane = lax.broadcasted_iota(jnp.int32, (CELLS, 256), 1)
    return jnp.where(lane >= 128, lane - 128, lane)


def apart(split):
    row = lax.broadcasted_iota(jnp.int32, (CELLS, 256), 0)
    key = key_lanes()
    differ = (row >= CELLS // 2) != (key >= CELLS // 2)
    return jnp.logical_and(differ, split)


def halves(fn, x):
    return jnp.concatenate(
        [jnp.broadcast_to(fn(x[:, :128]), (CELLS, 128)), jnp.broadcast_to(fn(x[:, 128:]), (CELLS, 128))],
        axis=1,
    )


def attend(q, k2, v2, differ):
    scores = mm_nt(q.astype(BF16), k2) * 0.125
    scores = jnp.where(differ, NEGATIVE, scores)
    scores = jnp.where(key_lanes() < CELLS, scores, LOWEST)
    exponent = jnp.exp(scores - halves(lambda s: jnp.max(s, axis=1, keepdims=True), scores))
    weights = exponent / halves(lambda s: jnp.sum(s, axis=1, keepdims=True), exponent)
    return weights, mm(weights.astype(BF16), v2)


def attend_back(q, k2, v2, weights, differ, d):
    d = d.astype(BF16)
    dv = unstacked(mm_tn(weights.astype(BF16), d))
    dw = rounded(mm_nt(d, v2))
    ds = weights * (dw - halves(lambda s: jnp.sum(s, axis=1, keepdims=True), dw * weights))
    ds = jnp.where(differ, 0.0, ds * 0.125).astype(BF16)
    dq = mm(ds, k2)
    dk = unstacked(mm_tn(ds, q.astype(BF16)))
    return dq, dk, dv


def first_kernel(
    place, tok_in, cot_in, tok_send_in, cot_send_in, tok2d, side, edge, corner, cot2d,
    tok, cot, tok_send, cot_send, arrived,
):
    loads = [
        pltpu.make_async_copy(source, target, arrived.at[i])
        for i, (source, target) in enumerate(
            ((tok_in, tok), (cot_in, cot), (tok_send_in, tok_send), (cot_send_in, cot_send))
        )
    ]
    for load in loads:
        load.start()
    for load in loads:
        load.wait()
    x = tok[...].astype(F32).reshape(ROWS * COLS, D).astype(BF16)
    tok2d[...] = x
    for r in range(6):
        cot2d[pl.ds(12 * r, 12), :] = cot[r].astype(F32)
    y = cot2d[...].astype(BF16)
    stack = (mm(tok_send[...], x) + mm(cot_send[...], y)).astype(BF16)
    cut(stack, side, edge, corner)


def fine_forward_kernel(
    place, x_in, side, edge, corner, gain, wqkv, wproj, t_halo, y_send,
    x_out, nm_out, p_out, w_out, y_out, side_out, edge_out, corner_out, mixed,
):
    halo = jnp.concatenate([side[...], edge[...], corner[...]], axis=0)
    x = x_in[...].astype(F32) + mm(t_halo[...], halo)
    x_out[...] = x.astype(BF16)
    xhat, _ = normalize(x)
    n = (xhat * gain[...]).astype(BF16)
    nm_out[:, pl.ds(0, D)] = n
    p_out[...] = rounded(mm(n, wqkv[...]))
    for w in range(WINDOWS):
        differ = apart(decode(place)[3] == 1 if w >= 2 else False)
        for p in range(HF // 2):
            rows = pl.ds(CELLS * w, CELLS)
            q, k, v = (p_out[rows, pl.ds(256 * part + 128 * p, 128)] for part in range(3))
            weights, out = attend(q, stacked(k), stacked(v), differ)
            w_out[2 * w + p] = weights
            mixed[rows, pl.ds(128 * p, 128)] = out
    m = mixed[...].astype(BF16)
    nm_out[:, pl.ds(D, 256)] = m
    y = (x + mm(m, wproj[...])).astype(BF16)
    y_out[...] = y
    stack = mm(y_send[...], y).astype(BF16)
    cut(stack, side_out, edge_out, corner_out)


def coarse_kernel(
    place, y_in, side, edge, corner, dy_in, dmixed,
    mgain, mweight, gain, wqkv, wproj, y_halo, df_send, out_send,
    y2_out, df_out, side_out, edge_out, corner_out, fac_out, packed, mixed, dpacked, wsave,
):
    halo = jnp.concatenate([side[...], edge[...], corner[...]], axis=0)
    patches = y_in[...].astype(F32) + mm(y_halo[...], halo)
    g = jnp.concatenate([patches[CELLS * i : CELLS * (i + 1)] for i in range(4)], axis=1)
    ghat, ginv = normalize(g)
    mn = (ghat * mgain[...]).astype(BF16)
    z = rounded(mm(mn, mweight[...]))
    zhat, zinv = normalize(z)
    n = (zhat * gain[...]).astype(BF16)
    packed[...] = rounded(mm(n, wqkv[...]))
    differ = apart(decode(place)[3] == 1)
    for p in range(HC // 2):
        lanes = pl.ds(128 * p, 128)
        q, k, v = (packed[:, pl.ds(512 * part + 128 * p, 128)] for part in range(3))
        weights, out = attend(q, stacked(k), stacked(v), differ)
        wsave[p] = weights
        mixed[:, lanes] = out
    m = mixed[...].astype(BF16)
    y2 = (z + mm(m, wproj[...])).astype(BF16)
    y2_out[...] = y2

    dy = dy_in[...].astype(F32)
    for p in range(HC // 2):
        q, k, v = (packed[:, pl.ds(512 * part + 128 * p, 128)] for part in range(3))
        grads = attend_back(q, stacked(k), stacked(v), wsave[p], differ, dmixed[:, pl.ds(128 * p, 128)])
        for part in range(3):
            dpacked[:, pl.ds(512 * part + 128 * p, 128)] = grads[part]
    dp = dpacked[...].astype(BF16)
    dn = rounded(mm_nt(dp, wqkv[...]))
    dz = (dy + normalize_back(dn * gain[...], zhat, zinv)).astype(BF16)
    dmn = rounded(mm_nt(dz, mweight[...]))
    dg = normalize_back(dmn * mgain[...], ghat, ginv)
    df = jnp.concatenate([dg[:, D * i : D * (i + 1)] for i in range(4)], axis=0).astype(BF16)
    df_out[...] = df
    stack = (mm(df_send[...], df) + mm(out_send[...], y2)).astype(BF16)
    cut(stack, side_out, edge_out, corner_out)
    at = 0
    for piece in (mn, n, m, dz, dp, dy.astype(BF16)):
        fac_out[pl.ds(0, CELLS), pl.ds(at, piece.shape[1])] = piece
        at += piece.shape[1]
    fac_out[pl.ds(CELLS, TALL - CELLS), :] = jnp.zeros((TALL - CELLS, at), BF16)


def own_rows_kernel(rows, main, out):
    out[...] = mm(main[...], rows[...]).astype(BF16)


def before_coarse_kernel(y_in, y_main, cot_in, side, edge, corner, c_main, c_halo, wproj, y_out, dy_out, dmixed):
    y_out[...] = mm(y_main[...], y_in[...]).astype(BF16)
    halo = jnp.concatenate([side[...], edge[...], corner[...]], axis=0)
    dy = (mm(c_main[...], cot_in[...].astype(BF16)) + mm(c_halo[...], halo)).astype(BF16)
    dy_out[...] = dy
    dmixed[...] = rounded(mm_nt(dy, wproj[...]))


def fine_backward_kernel(
    place, df_in, side, edge, corner, x_in, p_in, w_in, gain, wqkv, wproj, d_main, d_halo, dx_send,
    dx_out, side_out, edge_out, corner_out, fac_out, dmixed, dpacked,
):
    halo = jnp.concatenate([side[...], edge[...], corner[...]], axis=0)
    dy = mm(d_main[...], df_in[...]) + mm(d_halo[...], halo)
    dmixed[...] = rounded(mm_nt(dy.astype(BF16), wproj[...]))
    for w in range(WINDOWS):
        differ = apart(decode(place)[3] == 1 if w >= 2 else False)
        for p in range(HF // 2):
            rows = pl.ds(CELLS * w, CELLS)
            q, k, v = (p_in[rows, pl.ds(256 * part + 128 * p, 128)] for part in range(3))
            d = dmixed[rows, pl.ds(128 * p, 128)]
            grads = attend_back(q, stacked(k), stacked(v), w_in[2 * w + p], differ, d)
            for part in range(3):
                dpacked[rows, pl.ds(256 * part + 128 * p, 128)] = grads[part]
    dp = dpacked[...].astype(BF16)
    dn = rounded(mm_nt(dp, wqkv[...]))
    xhat, inverse = normalize(x_in[...].astype(F32))
    dx = (dy + normalize_back(dn * gain[...], xhat, inverse)).astype(BF16)
    dx_out[...] = dx
    stack = mm(dx_send[...], dx).astype(BF16)
    cut(stack, side_out, edge_out, corner_out)
    fac_out[:, pl.ds(0, 768)] = dp
    fac_out[:, pl.ds(768, D)] = dy.astype(BF16)


def decode(place):
    code = place[0]
    bits = tuple(lax.bitwise_and(lax.shift_right_logical(code, i), 1) for i in range(4))
    return bits + (lax.shift_right_logical(code, 4),)


def one_hot(want, width):
    lane = lax.broadcasted_iota(jnp.int32, (want.shape[0], width), 1)
    return jnp.where(lane == want, 1.0, 0.0).astype(BF16)


def row_index(count):
    return lax.broadcasted_iota(jnp.int32, (count, 1), 0)


def field(x, low, bits):
    return lax.bitwise_and(lax.shift_right_logical(x, low), (1 << bits) - 1)


def coarse_weights_kernel(
    place, own, other, m0k, m0s, m1k, m1s, c0k, c0s, c1k, c1s, lines
):
    core, zp, yp, _, _ = decode(place)

    def at(start, size):
        return jnp.concatenate([own[:, pl.ds(start, size)], other[:, pl.ds(start, size)]], axis=0)

    dz = at(2048 + 1024, D)
    row = row_index(256)
    group = field(row, 4, 3) * 2 + lax.bitwise_xor(field(row, 7, 1), yp)
    select = one_hot((2 * group + core) * 16 + field(row, 0, 4), D)
    for zh in range(2):
        pair = [at(D * (2 * zh + k), D) for k in range(2)]
        plain = jnp.full(pair[0].shape, zp, jnp.int32) == 0
        ordered = (
            jnp.where(plain, pair[0].astype(F32), pair[1].astype(F32)).astype(BF16),
            jnp.where(plain, pair[1].astype(F32), pair[0].astype(F32)).astype(BF16),
        )
        for zd in range(2):
            left = mm_nt(select, ordered[zd]).astype(BF16)
            part = mm(left, dz).reshape(16, 16, D)
            for yd in range(2):
                for h in range(4):
                    piece = part[8 * yd : 8 * yd + 8, :, 128 * h : 128 * h + 128]
                    (m0s if zd else m0k)[pl.ds(16 * yd + 8 * zh, 8), pl.ds(8 * h, 8), :] = piece[:, :8].astype(BF16)
                    (m1s if yd else m1k)[pl.ds(16 * zd + 8 * zh, 8), pl.ds(8 * h, 8), :] = piece[:, 8:].astype(BF16)
    row = row_index(256)
    z = field(row, 3, 1) * 2 + lax.bitwise_xor(field(row, 5, 1), zp)
    group = z * 16 + field(row, 0, 3) * 2 + lax.bitwise_xor(field(row, 4, 1), yp)
    select = one_hot((2 * group + core) * 4 + field(row, 6, 2), D)
    n = mm_nt(select, at(2048, D)).astype(BF16)
    m = mm_nt(select, at(2048 + D, D)).astype(BF16)
    for j in range(4):
        part = mm(n if j < 3 else m, at(2048 + 1536 + D * j, D))
        for i in range(4):
            line = part[64 * i : 64 * (i + 1)]
            for h in range(4):
                lines[pl.ds(512 * (4 * (j // 2) + h) + 4 * (j % 2) + i, 64, 8), :] = line[:, 128 * h : 128 * h + 128]
    for h in range(4):
        first = lines[pl.ds(512 * h, 512), :].reshape(64, 8, 128).astype(BF16)
        c0s[:, pl.ds(8 * h, 8), :] = first[:32]
        c0k[:, pl.ds(8 * h, 8), :] = first[32:]
        second = lines[pl.ds(512 * (4 + h), 512), :].reshape(64, 8, 128).astype(BF16)
        for zd in range(2):
            c1s[pl.ds(16 * zd, 16), pl.ds(8 * h, 8), :] = second[32 * zd : 32 * zd + 16]
            c1k[pl.ds(16 * zd, 16), pl.ds(8 * h, 8), :] = second[32 * zd + 16 : 32 * zd + 32]


def middle_kernel(m0k, m0c, m1k, m1c, c0k, c0c, c1k, c1c, y_keep, y_send, z_keep, z_send):
    for keep, came, at, first, second in (
        (m0k, m0c, 0, y_keep, y_send), (c0k, c0c, 16, y_send, y_keep),
        (m1k, m1c, 0, z_send, z_keep), (c1k, c1c, 16, z_keep, z_send),
    ):
        total = (keep[...].astype(F32) + came[...].astype(F32)).astype(BF16)
        first[pl.ds(at, 16)] = total[:16]
        second[pl.ds(at, 16)] = total[16:]


def fine_weights_kernel(place, nm_own, nm_other, own, other, out, lines):
    core = decode(place)[0]
    row = row_index(256)
    select = one_hot((2 * field(row, 0, 6) + core) * 4 + field(row, 6, 2), D)
    dp = lambda ref: ref[:, pl.ds(0, 768)]
    dy = lambda ref: ref[:, pl.ds(768, D)]
    n = [mm_nt(select, ref[:, pl.ds(0, D)]).astype(BF16) for ref in (nm_own, nm_other)]
    part = mm(n[0], dp(own)) + mm(n[1], dp(other))
    for i in range(4):
        line = part[64 * i : 64 * (i + 1)]
        for h in range(4):
            lines[pl.ds(512 * h + i, 64, 8), :] = line[:, 128 * h : 128 * h + 128]
        for h in range(2):
            lines[pl.ds(512 * (2 * (i // 2) + h) + 4 + i % 2, 64, 8), :] = line[:, 512 + 128 * h : 640 + 128 * h]
    row = row_index(128)
    select = one_hot((2 * field(row, 0, 6) + core) * 2 + field(row, 6, 1), 256)
    m = [mm_nt(select, ref[:, pl.ds(D, 256)]).astype(BF16) for ref in (nm_own, nm_other)]
    part = mm(m[0], dy(own)) + mm(m[1], dy(other))
    for i in range(2):
        line = part[64 * i : 64 * (i + 1)]
        for h in range(4):
            lines[pl.ds(512 * h + 6 + i, 64, 8), :] = line[:, 128 * h : 128 * h + 128]
    for h in range(4):
        out[:, pl.ds(8 * h, 8), :] = lines[pl.ds(512 * h, 512), :].reshape(64, 8, 128).astype(BF16)


def join_kernel(place, yk, yc, zk, zc, fine, out):
    _, zp, yp, _, _ = decode(place)
    for keep, came, relations in ((yk, yc, ((0, 0), (1, 1))), (zk, zc, ((1, 0), (0, 1)))):
        total = (keep[...].astype(F32) + came[...].astype(F32)).astype(BF16)
        for part, (zd, yd) in enumerate(relations):
            for zh in range(2):
                at = 16 * part + 8 * zh
                out[zh, lax.bitwise_xor(zp, zd), :, lax.bitwise_xor(yp, yd), pl.ds(0, 32), :] = total[at : at + 8]
    out[:, :, :, :, pl.ds(32, 32), :] = fine[...].reshape(2, 2, 8, 2, 32, 128)


def gain_rows(weight, gain, device, share):
    count = max(8, share)
    pick_rows = one_hot(device * share + row_index(count), gain.shape[1])
    over = jnp.sum(pick_rows.astype(F32) * gain, axis=1, keepdims=True)
    return mm(pick_rows, weight)[:share] / over[:share]


def coefficients_kernel(place, fgain, fqkv, mgain, mweight, cgain, cqkv, fcoef, mcoef, ccoef):
    device = decode(place)[4]
    fcoef[...] = gain_rows(fqkv[...], fgain[...], device, 4)
    mcoef[...] = gain_rows(mweight[...], mgain[...], device, 16)
    ccoef[...] = gain_rows(cqkv[...], cgain[...], device, 4)


def output_kernel(y2, side, edge, corner, out_main, out_halo, out):
    halo = jnp.concatenate([side[...], edge[...], corner[...]], axis=0)
    y = mm(out_main[...], y2[...]) + mm(out_halo[...], halo)
    for r in range(6):
        out[r] = y[16 * r : 16 * r + 12].astype(BF16)


def tokens_kernel(dx, side, edge, corner, dx_halo, grad):
    halo = jnp.concatenate([side[...], edge[...], corner[...]], axis=0)
    d = dx[...].astype(F32) + mm(dx_halo[...], halo)
    grad[...] = d.reshape(ROWS, COLS, D).astype(BF16)


def as_row(column):
    size = column.shape[0]
    row = lax.broadcasted_iota(jnp.int32, (size, size), 0)
    lane = lax.broadcasted_iota(jnp.int32, (size, size), 1)
    return jnp.sum(jnp.where(row == lane, column, 0.0), axis=0, keepdims=True)


def sum_kernel(place, parts, fcoef, mcoef, ccoef, fgain, fqkv, fproj, mgain, merge, cgain, cqkv, cproj):
    _, zp, yp, _, _ = decode(place)
    factor = (ROWS * COLS * 128 // 4) ** (-0.5)
    sums = []
    for z in range(2):
        for y in range(2):
            total = None
            for zh in range(2):
                for k in range(8):
                    term = parts[zh, z, k, y].astype(F32)
                    total = term if total is None else total + term
            sums.append(total * factor)
    fine = (sums[0] + sums[1] + sums[2] + sums[3])[32:]
    tops = [v[:32] for v in sums]
    z_same = jnp.full((32, 128), zp, jnp.int32) == 0
    y_same = jnp.full((32, 128), yp, jnp.int32) == 0

    def related(zd, yd):
        low = [jnp.where(z_same, tops[2 * zd + y], tops[2 * (1 - zd) + y]) for y in range(2)]
        return jnp.where(y_same, low[yd], low[1 - yd])

    m0, m1, c0, c1 = (related(0, 0), related(1, 0), related(1, 1), related(0, 1))
    for h in range(4):
        lanes = pl.ds(128 * h, 128)
        rows = slice(8 * h, 8 * h + 8)
        merge[pl.ds(0, 8), lanes] = m0[rows]
        merge[pl.ds(8, 8), lanes] = m1[rows]
        cqkv[:, lanes] = c0[8 * h : 8 * h + 4]
        cqkv[:, pl.ds(D + 128 * h, 128)] = c0[8 * h + 4 : 8 * h + 8]
        cqkv[:, pl.ds(2 * D + 128 * h, 128)] = c1[8 * h : 8 * h + 4]
        cproj[:, lanes] = c1[8 * h + 4 : 8 * h + 8]
        fqkv[:, lanes] = fine[8 * h : 8 * h + 4]
        fqkv[pl.ds(2 * (h // 2), 2), pl.ds(D + 128 * (h % 2), 128)] = fine[8 * h + 4 : 8 * h + 6]
        fproj[:, lanes] = fine[8 * h + 6 : 8 * h + 8]
    for ref, coef, grad in ((fgain, fcoef, fqkv), (mgain, mcoef, merge), (cgain, ccoef, cqkv)):
        ref[...] = as_row(jnp.sum(coef[...] * grad[...], axis=1, keepdims=True))


def exchange(pieces, step):
    lat = lax.axis_size("lat")
    pair = lax.axis_size("pair")
    lon = 2 * pair
    arrived = []
    for piece, (dr, dc) in zip(pieces, ((0, 1), (1, 0), (1, 1))):
        pairs = []
        for r in range(lat):
            for c in range(lon):
                to = ((r + step * dr) % lat) * lon + (c + step * dc) % lon
                pairs.append((r * lon + c, to))
        arrived.append(lax.ppermute(piece, ("lat", "pair", "core"), pairs))
    return arrived


def partner(value):
    return lax.ppermute(value, "core", [(0, 1), (1, 0)])


def fold(value, axis, second):
    lat, pair = (lax.axis_size("lat"), lax.axis_size("pair"))
    pairs = []
    for r in range(lat):
        for p in range(pair):
            z, y = (r // 2, (r % 2) * 2 + p % 2)
            at = z if axis == "z" else y
            at = (at + (1 if at % 2 == (1 if second else 0) else -1)) % 4
            z, y = (at, y) if axis == "z" else (z, at)
            pairs.append((r * pair + p, (2 * z + y // 2) * pair + (p // 2) * 2 + y % 2))
    return lax.ppermute(value, ("lat", "pair"), pairs)


def deal(value):
    return lax.all_to_all(value, ("lat", "pair"), 0, 0)


def local(
    tokens, fine_gain, fine_qkv, fine_proj, merge_gain, merge_weight, coarse_gain, coarse_qkv, coarse_proj, cotangent
):
    lat_count = lax.axis_size("lat")
    lat, core = (lax.axis_index("lat"), lax.axis_index("core"))
    device = (lat * lax.axis_size("pair") + lax.axis_index("pair")) * 2 + core
    parity = lax.bitwise_and(lax.shift_right_logical(lat, 1), 1)
    seam = (lat == lat_count - 1).astype(jnp.int32)
    flip = lax.bitwise_and(lax.axis_index("pair"), 1)
    place = (device * 16 + seam * 8 + flip * 4 + parity * 2 + core).astype(jnp.int32).reshape(1)
    fgain, mgain, cgain = (v.reshape(1, -1) for v in (fine_gain, merge_gain, coarse_gain))
    cells = WINDOWS * CELLS

    pieces = [((size, D), BF16) for size in SLOTS]
    narrow = [((size, D), BF16) for size in NARROW]
    tok, *sent, cot = call(
        first_kernel,
        [((cells, D), BF16)] + pieces + [((CELLS, D), F32)],
        place,
        *(
            pltpu.with_memory_space_constraint(v, pltpu.HBM)
            for v in (tokens, cotangent, table("tok_send"), table("cot_send"))
        ),
        specs=[SMEM_SPEC] + [pl.BlockSpec(memory_space=pltpu.HBM)] * 4,
        scratch=[
            pltpu.VMEM((ROWS, COLS, D), BF16), pltpu.VMEM((6, 12, D), BF16), pltpu.VMEM((sum(SLOTS), cells), BF16),
            pltpu.VMEM((sum(SLOTS), CELLS), BF16), pltpu.SemaphoreType.DMA((4,)),
        ],
    )
    ahead = exchange(sent, -1)
    (tok,) = call(own_rows_kernel, [((cells, D), BF16)], tok, table("tok_main"))
    x, nm, p, w, y, *sent = scalar_call(
        fine_forward_kernel,
        [
            ((cells, D), BF16), ((cells, 768), BF16), ((cells, 768), F32), ((8, CELLS, 256), F32),
            ((cells, D), BF16),
        ]
        + narrow,
        place, tok, *ahead, fgain, fine_qkv, fine_proj, table("tok_halo"), table("y_send"),
        scratch=[pltpu.VMEM((cells, 256), F32)],
    )
    merged = exchange(sent, -1)
    y, dy, dmixed = call(
        before_coarse_kernel,
        [((cells, D), BF16), ((CELLS, D), BF16), ((CELLS, D), F32)],
        y, table("y_main"), cot, *ahead, table("cot_main"), table("cot_halo"), coarse_proj,
    )
    nm_other = partner(nm)
    y2, df, *sent, fac = scalar_call(
        coarse_kernel,
        [((CELLS, D), BF16), ((cells, D), BF16)] + pieces + [((TALL, 5632), BF16)],
        place, y, *merged, dy, dmixed, mgain, merge_weight, cgain, coarse_qkv, coarse_proj,
        table("y_halo"), table("df_send"), table("out_send"),
        scratch=[
            pltpu.VMEM((CELLS, 1536), F32), pltpu.VMEM((CELLS, D), F32), pltpu.VMEM((CELLS, 1536), F32),
            pltpu.VMEM((4, CELLS, 256), F32),
        ],
    )
    back = exchange(sent, 1)
    m0k, m0s, m1k, m1s, c0k, c0s, c1k, c1s = scalar_call(
        coarse_weights_kernel,
        [((32, 32, 128), BF16)] * 8,
        place, fac, partner(fac),
        scratch=[pltpu.VMEM((4104, 128), F32)],
    )
    first = [
        fold(v, axis, second)
        for v, axis, second in ((m0s, "z", False), (m1s, "y", False), (c0s, "z", True), (c1s, "y", True))
    ]
    dx, *sent, fac = scalar_call(
        fine_backward_kernel,
        [((cells, D), BF16)] + narrow + [((cells, 1280), BF16)],
        place, df, *back, x, p, w, fgain, fine_qkv, fine_proj, table("df_main"), table("df_halo"), table("dx_send"),
        scratch=[pltpu.VMEM((cells, 256), F32), pltpu.VMEM((cells, 768), F32)],
    )
    ended = exchange(sent, 1)
    y_keep, y_send, z_keep, z_send = call(
        middle_kernel,
        [((32, 32, 128), BF16)] * 4,
        m0k, first[0], m1k, first[1], c0k, first[2], c1k, first[3],
    )
    y_came, z_came = (fold(y_send, "y", False), fold(z_send, "z", False))
    (fine_part,) = scalar_call(
        fine_weights_kernel,
        [((64, 32, 128), BF16)],
        place, nm, nm_other, fac, partner(fac),
        scratch=[pltpu.VMEM((2056, 128), F32)],
    )
    (joined,) = scalar_call(
        join_kernel,
        [((2, 2, 8, 2, 64, 128), BF16)],
        place, y_keep, y_came, z_keep, z_came, fine_part,
    )
    parts = deal(joined.reshape(64, 64, 128)).reshape(2, 2, 8, 2, 64, 128)
    (output,) = call(output_kernel, [((6, 12, D), BF16)], y2, *back, table("out_main"), table("out_halo"))
    (dx,) = call(own_rows_kernel, [((cells, D), BF16)], dx, table("dx_main"))
    (grad,) = call(tokens_kernel, [((ROWS, COLS, D), BF16)], dx, *ended, table("dx_halo"))
    fcoef, mcoef, ccoef = scalar_call(
        coefficients_kernel,
        [((4, 768), F32), ((16, D), F32), ((4, 1536), F32)],
        place, fgain, fine_qkv, mgain, merge_weight, cgain, coarse_qkv,
    )
    fg, fqkv, fproj, mg, merge, cg, cqkv, cproj = scalar_call(
        sum_kernel,
        [
            ((1, 4), F32), ((4, 768), F32), ((2, D), F32), ((1, 16), F32), ((16, D), F32), ((1, 4), F32),
            ((4, 1536), F32), ((4, D), F32),
        ],
        place, parts, fcoef, mcoef, ccoef,
    )
    fg, mg, cg = (v.reshape(-1) for v in (fg, mg, cg))
    return (output, grad, fg, fqkv, fproj, mg, merge, cg, cqkv, cproj)


def solution(mesh):
    lat, lon = (mesh.shape["lat"], mesh.shape["lon"])
    split = Mesh(mesh.devices.reshape(lat, lon // 2, 2), ("lat", "pair", "core"))
    lon = ("pair", "core")
    grid = P("lat", lon, None)
    whole = ("lat", "pair", "core")
    return jax.shard_map(
        local,
        mesh=split,
        in_specs=(grid, P(), P(), P(), P(), P(), P(), P(), P(), grid),
        out_specs=(
            grid, grid, P(whole), P(whole, None), P(whole, None), P(whole), P(whole, None), P(whole),
            P(whole, None), P(whole, None),
        ),
        check_vma=False,
    )
```
